128 devices in a mesh: ga: 16 (over x, y), band: 8 (over z, core).
Axes of the slice: x: 4, y: 4, z: 4, core: 2. Of those that a mesh axis runs over, the one named last changes fastest.
Arguments:
- psi: bfloat16 [2, 16, 96, 2048], P(None, 'band', None, 'ga'), may hold values from -6 to 6
- vloc: float32 [96, 9216], P('ga'), may hold values from 0.5 to 1.5
- dv: float32 [96, 9216], P('ga'), may hold values from -6 to 6
- beta: float32 [2, 128, 96, 2048], P(None, None, None, 'ga'), may hold values from -0.02734375 to 0.02734375
- dij: float32 [2, 4, 4], replicated, may hold values from -1 to 1.5, as said below
- atom_type: int32 [32], replicated, may hold values from 0 to 1
- stick_xy: int32 [2048], replicated, may hold values from 0 to 9215, as said below
- band_shift: float32 [16], P('band'), may hold values from 0.3 to 3
Outputs:
- response: float32 [2, 16, 96, 2048], P(None, 'band', None, 'ga')
- density: float32 [96, 9216], P('ga', 'band')
The draws below stay inside these ranges and needn't reach their ends.
Inputs may be any that keep to these rules, and one draw needn't show every extreme that they name: `stick_xy`: 2048 distinct columns, each with both frequencies f(y) and f(x) in -(32) to 31. `dij`: each of the 2 matrices is symmetric positive definite with diagonal at least 0.5.
All inputs are finite; a program needn't handle non-finite values.
Results may differ from the reference program's by a relative error of at most 0.0003.
Values may be sent and summed in bfloat16 or wider, within the bound.
A program may use at most 128 MiB of HBM per device.

```python
import math
import jax
import jax.numpy as jnp
from jax import lax

GRID = 96
STICKS = 2048
NATOM = 32
NBETA = 4
NTYPE = 2
ITERS = 2
NPROJ = 128
BANDS = 16


def draw_stick_xy(key, part):
    radius_cells = GRID // 3
    square_side = 2 * radius_cells
    chosen = jax.random.permutation(key, square_side * square_side)[:STICKS]
    freq_y = chosen // square_side - radius_cells
    freq_x = chosen % square_side - radius_cells
    return (freq_y % GRID * GRID + freq_x % GRID).astype(jnp.int32)


def draw_dij(key, part):
    factor = jax.random.uniform(key, (NTYPE, NBETA, NBETA), jnp.float32, -1.0, 1.0)
    product = jnp.einsum('tij,tkj->tik', factor, factor) / NBETA
    return product + 0.5 * jnp.eye(NBETA, dtype=jnp.float32)[None]


def with_ends(values, key, least, largest):
    dims = values.shape
    spot = [jax.random.randint(jax.random.fold_in(key, axis), (), 0, dims[axis]) for axis in range(len(dims))]
    values = values.at[tuple(spot)].set(least)
    longest = dims.index(max(dims))
    spot[longest] = (spot[longest] + 1) % dims[longest]
    return values.at[tuple(spot)].set(largest)


def level_of(key, dims, cuts, low, high):
    gain = 1.0
    for dim, parts in cuts:
        draws = jax.random.uniform(jax.random.fold_in(jax.random.fold_in(key, 6), dim), (parts,), jnp.float32, low / len(cuts), high / len(cuts))
        gain = gain * jnp.repeat(jnp.exp(draws), dims[dim] // parts).reshape((-1,) + (1,) * (len(dims) - 1 - dim))
    return gain


def noise(rng, dims, width, reach, shards=(), kind=jnp.bfloat16):
    entries = jax.random.normal(rng, dims, jnp.float32) * width
    if len(shards) > 0:
        entries = level_of(rng, dims, shards, -0.22, 0.18) * entries
    return jnp.clip(entries, min=-reach, max=reach).astype(kind)


def setup_inputs(seed: int = 0) -> dict:
    streams_of = jax.random.split(jax.random.key(seed), 9)
    return {
        "psi": noise(streams_of[0], (2, BANDS, GRID, STICKS), 1.0, 6.0, ((1, 8), (3, 16))),
        "vloc": jnp.clip(0.5 + 1.0 * jax.random.uniform(streams_of[1], (GRID, GRID * GRID), jnp.float32) ** level_of(streams_of[1], (GRID, GRID * GRID), ((0, 16),), -0.2, 0.2), 0.5, 1.5),
        "dv": noise(streams_of[2], (GRID, GRID * GRID), 1.0, 6.0, ((0, 16),), jnp.float32),
        "beta": noise(streams_of[3], (2, NPROJ, GRID, STICKS), (GRID * STICKS // 4) ** -0.5, 0.02734375, ((3, 16),), jnp.float32),
        "dij": draw_dij(jax.random.fold_in(streams_of[8], 71), 0),
        "atom_type": with_ends(jax.random.randint(streams_of[5], (NATOM,), 0, NTYPE), jax.random.fold_in(streams_of[5], 1), 0, NTYPE - 1).astype(jnp.int32),
        "stick_xy": draw_stick_xy(jax.random.fold_in(streams_of[8], 71), 0),
        "band_shift": jnp.clip(jnp.exp(math.log(3.0) - 2.3025851 * jax.random.uniform(streams_of[7], (BANDS,), jnp.float32) ** level_of(streams_of[7], (BANDS,), ((0, 8),), -0.2, 0.2)), 0.3, 3.0),
    }


highest = lax.Precision.HIGHEST


def frequency(index):
    return (index + GRID // 2) % GRID - GRID // 2


def kinetic_table(stick_xy):
    freq_z = frequency(jnp.arange(GRID, dtype=jnp.int32))
    freq_y = frequency(stick_xy // GRID)
    freq_x = frequency(stick_xy % GRID)
    summed = freq_z[:, None] ** 2 + (freq_y ** 2 + freq_x ** 2)[None, :]
    return summed.astype(jnp.float32) * (4.0 / (GRID * GRID))


def to_real(coef, stick_xy):
    values = coef[0] + 1j * coef[1]
    grid = jnp.zeros((GRID, GRID * GRID), values.dtype).at[:, stick_xy].set(values)
    field = jnp.fft.ifftn(grid.reshape(GRID, GRID, GRID)) * (GRID ** 1.5)
    field = field.reshape(GRID, GRID * GRID)
    return jnp.stack([jnp.real(field), jnp.imag(field)])


def to_recip(field, stick_xy):
    values = (field[0] + 1j * field[1]).reshape(GRID, GRID, GRID)
    spectrum = jnp.fft.fftn(values).reshape(GRID, GRID * GRID) / (GRID ** 1.5)
    picked = spectrum[:, stick_xy]
    return jnp.stack([jnp.real(picked), jnp.imag(picked)])


def reference(psi, vloc, dv, beta, dij, atom_type, stick_xy, band_shift):
    occupied = jnp.moveaxis(psi.astype(jnp.float32), 1, 0)
    kinetic = kinetic_table(stick_xy)
    inv_norm = 1.0 / (2.0 * GRID * STICKS)

    def dv_image(coef):
        return to_recip(dv[None] * to_real(coef, stick_xy), stick_xy)

    image = lax.map(dv_image, occupied)
    intersect_re = jnp.einsum('mczs,nczs->mn', occupied, image, precision=highest) * inv_norm
    intersect_im = (jnp.einsum('mzs,nzs->mn', occupied[:, 0], image[:, 1], precision=highest) - jnp.einsum('mzs,nzs->mn', occupied[:, 1], image[:, 0], precision=highest)) * inv_norm
    corr_re = jnp.einsum('mn,mzs->nzs', intersect_re, occupied[:, 0], precision=highest) - jnp.einsum('mn,mzs->nzs', intersect_im, occupied[:, 1], precision=highest)
    corr_im = jnp.einsum('mn,mzs->nzs', intersect_im, occupied[:, 0], precision=highest) + jnp.einsum('mn,mzs->nzs', intersect_re, occupied[:, 1], precision=highest)
    rhs = jnp.stack([corr_re, corr_im], axis=1) - image
    selected = dij[atom_type]
    diagonal = kinetic[None] + band_shift[:, None, None]

    def local_image(coef):
        return to_recip(vloc[None] * to_real(coef, stick_xy), stick_xy)

    def apply_operator(vector):
        local = lax.map(local_image, vector)
        proj_re = jnp.einsum('jzs,bzs->bj', beta[0], vector[:, 0], precision=highest) + jnp.einsum('jzs,bzs->bj', beta[1], vector[:, 1], precision=highest)
        proj_im = jnp.einsum('jzs,bzs->bj', beta[0], vector[:, 1], precision=highest) - jnp.einsum('jzs,bzs->bj', beta[1], vector[:, 0], precision=highest)
        shaped_re = proj_re.reshape(BANDS, NATOM, NBETA)
        shaped_im = proj_im.reshape(BANDS, NATOM, NBETA)
        coup_re = jnp.einsum('aij,baj->bai', selected, shaped_re, precision=highest).reshape(BANDS, NPROJ)
        coup_im = jnp.einsum('aij,baj->bai', selected, shaped_im, precision=highest).reshape(BANDS, NPROJ)
        back_re = jnp.einsum('jzs,bj->bzs', beta[0], coup_re, precision=highest) - jnp.einsum('jzs,bj->bzs', beta[1], coup_im, precision=highest)
        back_im = jnp.einsum('jzs,bj->bzs', beta[0], coup_im, precision=highest) + jnp.einsum('jzs,bj->bzs', beta[1], coup_re, precision=highest)
        return diagonal[:, None] * vector + local + jnp.stack([back_re, back_im], axis=1)

    def band_sum(first, second):
        return jnp.sum(first * second, axis=(1, 2, 3))

    solution = jnp.zeros_like(rhs)
    residual = rhs
    direction = rhs
    norm_now = band_sum(rhs, rhs)
    for iteration in range(ITERS):
        image_now = apply_operator(direction)
        alpha = (norm_now / band_sum(direction, image_now))[:, None, None, None]
        solution = solution + alpha * direction
        residual = residual - alpha * image_now
        if iteration + 1 < ITERS:
            norm_next = band_sum(residual, residual)
            direction = residual + (norm_next / norm_now)[:, None, None, None] * direction
            norm_now = norm_next

    def accumulate(carry, pair):
        psi_field = to_real(pair[0], stick_xy)
        resp_field = to_real(pair[1], stick_xy)
        return carry + 4.0 * jnp.sum(psi_field * resp_field, axis=0), None

    density, unused = lax.scan(accumulate, jnp.zeros((GRID, GRID * GRID), jnp.float32), (occupied, solution))
    return jnp.moveaxis(solution, 0, 1), density
```

```python
import functools
import math

import jax
import jax.numpy as jnp
import numpy as np
from jax import lax
from jax.experimental import pallas as pl
from jax.experimental.pallas import tpu as pltpu
from jax.sharding import PartitionSpec as P

GRID = 96
SIDE = 64
GROUPS = 16
PLANES = 6
ROWS = 24
MESH = pl.DeviceIdType.MESH
f32 = jnp.float32
bf16 = jnp.bfloat16


def complex_table(angle):
    cos, sin = np.cos(angle), np.sin(angle)
    return np.array([[cos, -sin], [sin, cos]]) / math.sqrt(GRID)


def halves(table):
    high = np.asarray(table, np.float32).astype(jnp.bfloat16)
    low = (table - high.astype(np.float64)).astype(jnp.bfloat16)
    return high, low


def tables(bands):
    unit = 2.0 * math.pi / GRID
    cells = np.arange(GRID)
    freqs = np.arange(SIDE) - SIDE // 2
    along_z = complex_table(unit * (cells[:, None] * cells[None, :] % GRID))
    along_z = along_z.reshape(2, 2, GROUPS, PLANES, GRID)
    z_table = np.einsum("oidpk,be->dopbiek", along_z, np.eye(bands))
    z_table = z_table.reshape(GROUPS * 2 * PLANES * bands, 2 * bands * GRID)
    along_x = np.zeros((2, 2, SIDE, 128))
    along_x[..., :GRID] = complex_table(unit * (freqs[:, None] * cells[None, :] % GRID))
    x_table = np.einsum("oikx,be->ibkoex", along_x, np.eye(2)).reshape(256, 512)
    along_y = complex_table(unit * (cells[:, None] * freqs[None, :] % GRID))
    along_y = along_y.reshape(2, 2, GRID, 16, 4)
    y_table = np.einsum("oiygl->oyilg", along_y).reshape(192, 128)
    out = []
    for table in (z_table, z_table.T, x_table, x_table.T, y_table):
        out.extend(halves(np.ascontiguousarray(table)))
    high, low = halves(np.ascontiguousarray(y_table.T))
    out.append(np.concatenate([high, high, low], axis=1))
    return [jnp.asarray(t) for t in out]


def dot(a, b):
    return lax.dot_general(a, b, (((1,), (0,)), ((), ())), preferred_element_type=f32)


def dot_nt(a, b):
    return lax.dot_general(a, b, (((1,), (1,)), ((), ())), preferred_element_type=f32)


def split(x):
    high = x.astype(bf16)
    return high, (x - high.astype(f32)).astype(bf16)


def left(high, low, x):
    xh, xl = split(x)
    return dot(
        jnp.concatenate([high, high, low], axis=1), jnp.concatenate([xh, xl, xh], axis=0)
    )


def right(ah, al, high, low):
    return dot(
        jnp.concatenate([ah, al, ah], axis=1), jnp.concatenate([high, high, low], axis=0)
    )


def row_sum(x):
    return jnp.sum(jnp.sum(x.reshape(-1, 8, 128), axis=0), axis=0, keepdims=True)


def lane_total(row):
    return jnp.sum(row, axis=1, keepdims=True)


def kernel(
    shift, dij, psi, vloc, dv, beta_hbm, kind, sticks,
    zh, zl, zth, ztl, xh, xl, xth, xtl, yh, yl, yt3,
    response, density,
    beta, occupied, onehot, mask, send, recv, small_send, small_recv,
    part_send, part_recv, lhs, grid, eh, el, dh, dl, psi_field, field0, field1,
    q, proj, coef, couple, vec, image, kin, own, dens,
    beta_sem, psi_ssem, psi_rsem, ssem, rsem, tssem, trsem, dssem, drsem,
):
    me = lax.axis_index("ga")
    mb = lax.axis_index("band")
    nb = 8

    barrier = pltpu.get_barrier_semaphore()

    def greet_ga(k, c):
        pl.semaphore_signal(
            barrier, inc=1, device_id=(lax.rem(me + k, GROUPS), mb), device_id_type=MESH
        )
        return c

    def greet_band(k, c):
        pl.semaphore_signal(
            barrier, inc=1, device_id=(me, lax.rem(mb + k, nb)), device_id_type=MESH
        )
        return c

    lax.fori_loop(1, GROUPS, greet_ga, 0)
    lax.fori_loop(1, nb, greet_band, 0)
    beta_copy = pltpu.make_async_copy(beta_hbm, beta, beta_sem)
    beta_copy.start()

    def ga_copy(rnd, k):
        other = lax.rem(me + k, GROUPS)
        return pltpu.make_async_remote_copy(
            src_ref=send.at[rnd, other],
            dst_ref=recv.at[rnd, me],
            send_sem=ssem.at[rnd, other],
            recv_sem=rsem.at[rnd, me],
            device_id=(other, mb),
            device_id_type=MESH,
        )

    def ga_landed(rnd, k):
        other = lax.rem(me + k, GROUPS)
        return pltpu.make_async_remote_copy(
            src_ref=send.at[rnd, other],
            dst_ref=recv.at[rnd, other],
            send_sem=ssem.at[rnd, other],
            recv_sem=rsem.at[rnd, other],
            device_id=(other, mb),
            device_id_type=MESH,
        )

    def exchange(rnd):
        def body(k, c):
            ga_copy(rnd, k).start()
            return c

        lax.fori_loop(1, GROUPS, body, 0)
        recv[rnd, me] = send[rnd, me]

    def arrived(rnd):
        def body(k, c):
            ga_landed(rnd, k).wait_recv()
            return c

        lax.fori_loop(1, GROUPS, body, 0)

    def small_copy(rnd, k, slot):
        other = lax.rem(me + k, GROUPS)
        return pltpu.make_async_remote_copy(
            src_ref=small_send.at[rnd],
            dst_ref=small_recv.at[rnd, me if slot is None else other],
            send_sem=tssem.at[rnd, other],
            recv_sem=trsem.at[rnd, me if slot is None else other],
            device_id=(other, mb),
            device_id_type=MESH,
        )

    def small_exchange(rnd):
        def body(k, c):
            small_copy(rnd, k, None).start()
            return c

        lax.fori_loop(1, GROUPS, body, 0)
        small_recv[rnd, me] = small_send[rnd]

    def small_total(rnd):
        def body(k, c):
            small_copy(rnd, k, 0).wait_recv()
            return c

        lax.fori_loop(1, GROUPS, body, 0)
        return jnp.sum(small_recv[rnd], axis=0)

    def psi_copy(k, slot):
        other = lax.rem(mb + k, nb)
        return pltpu.make_async_remote_copy(
            src_ref=psi,
            dst_ref=occupied.at[mb if slot is None else other],
            send_sem=psi_ssem.at[other],
            recv_sem=psi_rsem.at[mb if slot is None else other],
            device_id=(me, other),
            device_id_type=MESH,
        )

    def part_copy(k, slot):
        other = lax.rem(mb + k, nb)
        return pltpu.make_async_remote_copy(
            src_ref=part_send.at[other],
            dst_ref=part_recv.at[mb if slot is None else other],
            send_sem=dssem.at[other],
            recv_sem=drsem.at[mb if slot is None else other],
            device_id=(me, other),
            device_id_type=MESH,
        )

    wide = psi[...].reshape(384, 128)
    send[0] = dot(
        jnp.concatenate([zh[...], zl[...]], axis=1), jnp.concatenate([wide, wide], axis=0)
    ).reshape(GROUPS, ROWS, 128)
    pl.semaphore_wait(barrier, GROUPS - 1 + nb - 1)
    exchange(0)

    def psi_out(k, c):
        psi_copy(k, None).start()
        return c

    lax.fori_loop(1, nb, psi_out, 0)
    occupied[mb] = psi[...]

    def places(xy):
        flat = xy.astype(f32)
        y = jnp.floor((flat + 0.5) * (1.0 / GRID))
        x = flat - GRID * y
        fy = jnp.where(y >= GRID // 2, y - GRID, y)
        fx = jnp.where(x >= GRID // 2, x - GRID, x)
        return fy, fx

    fy, fx = places(sticks[...])
    ky = fy + SIDE // 2
    kx = fx + SIDE // 2
    high = jnp.floor(ky * 0.25)
    low = (ky - 4.0 * high) * SIDE + kx
    own[0:1, :] = low
    own[1:2, :] = high
    mask[...] = (
        lax.broadcasted_iota(jnp.int32, (16, 2048), 0).astype(f32) == own[1:2, :]
    ).astype(f32)

    def fill(k, c):
        lanes = pl.ds(pl.multiple_of(k * 256, 256), 256)
        ids = lax.broadcasted_iota(jnp.int32, (256, 256), 0).astype(f32)
        onehot[:, lanes] = (ids == own[0:1, lanes]).astype(f32).astype(bf16)
        return c

    lax.fori_loop(0, 8, fill, 0)
    mine = sticks[:, pl.ds(pl.multiple_of(me * 128, 128), 128)]
    oy, ox = places(mine)
    kz = lax.broadcasted_iota(jnp.int32, (GRID, 128), 0).astype(f32)
    fz = jnp.where(kz >= GRID // 2, kz - GRID, kz)
    kin[...] = (fz * fz + (oy * oy + ox * ox)) * (4.0 / (GRID * GRID))

    row = lax.broadcasted_iota(jnp.int32, (128, 128), 0)
    lane = lax.broadcasted_iota(jnp.int32, (128, 128), 1)
    same = (row // 4) == (lane // 4)
    first = kind[...] == 0
    total = jnp.zeros((128, 128), f32)
    for i in range(4):
        for k in range(4):
            value = jnp.where(first, dij[i * 4 + k], dij[16 + i * 4 + k])
            here = same & ((row % 4) == i) & ((lane % 4) == k)
            total = total + jnp.where(here, value, 0.0)
    couple[...] = total
    ones = jnp.ones((256, 128), bf16)

    def fill_planes(rnd, out):

        def body(src, c):
            piece = recv[rnd, src]
            upper = piece.astype(bf16).astype(f32)
            lower = piece - upper
            cols = pl.ds(pl.multiple_of(src * 128, 128), 128)
            keep = mask[:, cols]
            for r in range(ROWS):
                lhs[16 * r : 16 * r + 16, cols] = (
                    jnp.broadcast_to(upper[r : r + 1], (16, 128)) * keep
                ).astype(bf16)
                lhs[384 + 16 * r : 400 + 16 * r, cols] = (
                    jnp.broadcast_to(lower[r : r + 1], (16, 128)) * keep
                ).astype(bf16)
            return c

        lax.fori_loop(0, GROUPS, body, 0)
        both = dot_nt(lhs[...], onehot[...])
        grid[...] = both[0:384] + both[384:768]
        for t in range(2):
            lanes = slice(128 * t, 128 * t + 128)
            data = jnp.concatenate([grid[0:192, lanes], grid[192:384, lanes]], axis=1)
            ah, al = split(data)
            along = right(ah, al, xh[...], xl[...])
            uh, ul = split(along)
            eh[...] = uh
            el[...] = ul
            for c in range(2):
                for j in range(2):
                    rows = slice(16 * (4 * c + 2 * t + j), 16 * (4 * c + 2 * t + j) + 16)
                    cols = slice(128 * (2 * c + j), 128 * (2 * c + j) + 128)
                    for i in range(12):
                        dh[rows, 128 * i : 128 * i + 128] = eh[16 * i : 16 * i + 16, cols]
                        dl[rows, 128 * i : 128 * i + 128] = el[16 * i : 16 * i + 16, cols]
        for part in range(6):
            lanes = slice(256 * part, 256 * part + 256)
            out[:, lanes] = dot(
                jnp.concatenate([yh[...], yh[...], yl[...]], axis=1),
                jnp.concatenate([dh[:, lanes], dl[:, lanes], dh[:, lanes]], axis=0),
            )

    def to_sticks(rnd, potential, source):
        for p in range(PLANES):
            lanes = slice(256 * p, 256 * p + 256)
            pot = potential[:, 128 * p : 128 * p + 128]
            pot = jnp.concatenate([pot, pot], axis=1)
            pot = jnp.concatenate([pot, pot], axis=0)
            ah, al = split(source[:, lanes] * pot)
            along = dot(yt3[...], jnp.concatenate([ah, al, ah], axis=0))
            uh, ul = split(along)
            dh[:, lanes] = uh
            dl[:, lanes] = ul
        for t in range(2):
            for c in range(2):
                for j in range(2):
                    rows = slice(16 * (4 * c + 2 * t + j), 16 * (4 * c + 2 * t + j) + 16)
                    cols = slice(128 * (2 * c + j), 128 * (2 * c + j) + 128)
                    for i in range(12):
                        eh[16 * i : 16 * i + 16, cols] = dh[rows, 128 * i : 128 * i + 128]
                        el[16 * i : 16 * i + 16, cols] = dl[rows, 128 * i : 128 * i + 128]
            along = right(eh[...], el[...], xth[...], xtl[...])
            uh, ul = split(along)
            lanes = slice(128 * t, 128 * t + 128)
            for c in range(2):
                q[192 * c : 192 * c + 192, lanes] = uh[:, 128 * c : 128 * c + 128]
                q[384 + 192 * c : 576 + 192 * c, lanes] = ul[:, 128 * c : 128 * c + 128]

        def body(k, carry):
            lanes = pl.ds(pl.multiple_of(k * 256, 256), 256)
            place = onehot[:, lanes]
            keep = mask[:, lanes]
            both = dot(q[...], place)
            found = both[0:384] + both[384:768]
            picked = jnp.sum(found.reshape(ROWS, 16, 256) * keep[None], axis=1)
            send[rnd, 2 * k] = picked[:, 0:128]
            send[rnd, 2 * k + 1] = picked[:, 128:256]
            return carry

        lax.fori_loop(0, 8, body, 0)

    def z_forward(rnd):
        return left(zth[...], ztl[...], recv[rnd].reshape(384, 128))

    def project(load, count, source):
        def body(j, c):
            p0, p1 = load(j)
            for b in range(2):
                v0 = source[96 * b : 96 * b + 96, :]
                v1 = source[192 + 96 * b : 288 + 96 * b, :]
                proj[b, pl.ds(j, 1), :] = row_sum(p0 * v0 + p1 * v1)
                proj[2 + b, pl.ds(j, 1), :] = row_sum(p0 * v1 - p1 * v0)
            return c

        lax.fori_loop(0, count, body, 0)

    def projections(o, count):
        ph, pl_ = split(proj[o, 0:count, :])
        one = jnp.ones((8, 128), bf16)
        return dot_nt(
            jnp.concatenate([one, one], axis=1), jnp.concatenate([ph, pl_], axis=1)
        )[0:1, :]

    def spread(matrix, values):
        count = matrix.shape[0]
        for o in range(4):
            mh, ml = split(matrix * values[o : o + 1, :])
            coef[o, 0:count, :] = dot(jnp.concatenate([mh, ml], axis=1), ones)

    def apply(load, count, base):
        rows = 24
        for z in range(GRID // rows):

            def body(j, acc):
                p0, p1 = load(j, z * rows, rows)
                out = []
                for b in range(2):
                    cr = coef[b, pl.ds(j, 1), :]
                    ci = coef[2 + b, pl.ds(j, 1), :]
                    out.append(acc[2 * b] + (p0 * cr - p1 * ci))
                    out.append(acc[2 * b + 1] + (p0 * ci + p1 * cr))
                return tuple(out)

            init = tuple(
                base[192 * c + 96 * b + z * rows : 192 * c + 96 * b + z * rows + rows, :]
                for b in range(2)
                for c in range(2)
            )
            done = lax.fori_loop(0, count, body, init)
            for b in range(2):
                for c in range(2):
                    at = 192 * c + 96 * b + z * rows
                    image[at : at + rows, :] = done[2 * b + c]

    def beta_rows(j, at=0, rows=GRID):
        return beta[0, j, at : at + rows, :], beta[1, j, at : at + rows, :]

    def psi_rows(m, at=0, rows=GRID):
        owner, b = m // 2, m % 2
        return (
            occupied[owner, 0, b, at : at + rows, :].astype(f32),
            occupied[owner, 1, b, at : at + rows, :].astype(f32),
        )

    arrived(0)
    fill_planes(0, psi_field)
    to_sticks(1, dv, psi_field)
    exchange(1)

    def psi_in(k, c):
        psi_copy(k, 0).wait_recv()
        return c

    arrived(1)
    vec[1] = z_forward(1)
    lax.fori_loop(1, nb, psi_in, 0)

    project(psi_rows, 16, vec.at[1])
    small_send[0] = jnp.zeros((16, 128), f32)
    for o in range(4):
        small_send[0, o : o + 1, 0:16] = projections(o, 16)
    small_exchange(0)
    found = small_total(0) * (1.0 / (2.0 * GRID * 2048))
    eye = (row[0:16] == lane[0:16]).astype(f32)
    spread(eye, found)
    vec[1] = -vec[1]
    apply(psi_rows, 16, vec.at[1])
    vec[0] = image[...]

    def transform_out(rnd, source):
        send[rnd] = left(zh[...], zl[...], source[...]).reshape(GROUPS, ROWS, 128)
        exchange(rnd)

    def stick_sum(a, b, weight=None):
        out = []
        for n in range(2):
            s0 = slice(96 * n, 96 * n + 96)
            s1 = slice(192 + 96 * n, 288 + 96 * n)
            both = a[s0, :] * b[s0, :] + a[s1, :] * b[s1, :]
            if weight is not None:
                both = both * (kin[...] + shift[n])
            out.append(row_sum(both))
        return out

    def grid_sum(a, b):
        out = []
        for n in range(2):
            total = jnp.zeros((1, 128), f32)
            for p in range(PLANES):
                lanes = slice(128 * (2 * p + n), 128 * (2 * p + n) + 128)
                pot = vloc[:, 128 * p : 128 * p + 128]
                both = a[0:96, lanes] * b[0:96, lanes] + a[96:192, lanes] * b[96:192, lanes]
                total = total + row_sum(both * pot)
            out.append(total)
        return out

    def band_dots(values, coupled):
        both = values * coupled
        return [lane_total(both[b : b + 1] + both[2 + b : 3 + b]) for b in range(2)]

    ch, cl = split(couple[...])

    def coupled_rows(values):
        vh, vl = split(values)
        return dot_nt(
            jnp.concatenate([vh, vl, vh], axis=1), jnp.concatenate([ch, ch, cl], axis=1)
        )

    direction = vec.at[0]
    transform_out(2, direction)
    beta_copy.wait()
    project(beta_rows, 128, direction)
    small_send[1] = jnp.zeros((16, 128), f32)
    for o in range(4):
        small_send[1, o : o + 1, :] = projections(o, 128)
    norms = stick_sum(direction, direction)
    curves = stick_sum(direction, direction, True)
    arrived(2)
    fill_planes(2, field0)
    local = grid_sum(field0, field0)
    for b in range(2):
        small_send[1, 4 + b : 5 + b, :] = norms[b]
        small_send[1, 6 + b : 7 + b, :] = curves[b] + local[b]
    small_exchange(1)
    to_sticks(3, vloc, field0)
    exchange(3)
    sums = small_total(1)
    values0 = sums[0:4]
    coupled0 = coupled_rows(sums[0:8])[0:4]
    nonlocal0 = band_dots(values0, coupled0)
    norm0 = [lane_total(sums[4 + b : 5 + b]) for b in range(2)]
    curve0 = [lane_total(sums[6 + b : 7 + b]) + nonlocal0[b] for b in range(2)]
    alpha0 = [norm0[b] / curve0[b] for b in range(2)]
    spread(couple[...], values0)
    for c in range(2):
        for b in range(2):
            at = slice(192 * c + 96 * b, 192 * c + 96 * b + 96)
            vec[1, at, :] = direction[at, :] * (kin[...] + shift[b])
    apply(beta_rows, 128, vec.at[1])
    arrived(3)
    image[...] += z_forward(3)
    residual = vec.at[1]
    for c in range(2):
        for b in range(2):
            at = slice(192 * c + 96 * b, 192 * c + 96 * b + 96)
            residual[at, :] = direction[at, :] - alpha0[b] * image[at, :]

    transform_out(4, residual)
    project(beta_rows, 128, residual)
    small_send[2] = jnp.zeros((16, 128), f32)
    for o in range(4):
        small_send[2, o : o + 1, :] = projections(o, 128)
    norms = stick_sum(residual, residual)
    selfs = stick_sum(residual, residual, True)
    crosses = stick_sum(residual, direction, True)
    arrived(4)
    fill_planes(4, field1)
    self_local = grid_sum(field1, field1)
    cross_local = grid_sum(field1, field0)
    for b in range(2):
        small_send[2, 4 + b : 5 + b, :] = norms[b]
        small_send[2, 6 + b : 7 + b, :] = selfs[b] + self_local[b]
        small_send[2, 8 + b : 9 + b, :] = crosses[b] + cross_local[b]
    small_exchange(2)
    sums = small_total(2)
    values1 = sums[0:4]
    coupled1 = coupled_rows(sums[0:8])[0:4]
    self_dots = band_dots(values1, coupled1)
    cross_dots = band_dots(values1, coupled0)
    weight0, weight1 = [], []
    for b in range(2):
        ratio = lane_total(sums[4 + b : 5 + b]) / norm0[b]
        self_curve = lane_total(sums[6 + b : 7 + b]) + self_dots[b]
        cross_curve = lane_total(sums[8 + b : 9 + b]) + cross_dots[b]
        curve = self_curve + ratio * (2.0 * cross_curve + ratio * curve0[b])
        alpha = lane_total(sums[4 + b : 5 + b]) / curve
        weight0.append(alpha0[b] + alpha * ratio)
        weight1.append(alpha)

    for p in range(PLANES):
        total = jnp.zeros((GRID, 128), f32)
        for b in range(2):
            lanes = slice(128 * (2 * p + b), 128 * (2 * p + b) + 128)
            for c in range(2):
                at = slice(96 * c, 96 * c + 96)
                change = weight0[b] * field0[at, lanes] + weight1[b] * field1[at, lanes]
                total = total + psi_field[at, lanes] * change
        dens[:, 128 * p : 128 * p + 128] = 4.0 * total
    for i in range(nb):
        part_send[i, 0:12, :] = dens[12 * i : 12 * i + 12, :]
        part_send[i, 12:16, :] = jnp.zeros((4, 768), f32)

    def part_out(k, c):
        part_copy(k, None).start()
        return c

    lax.fori_loop(1, nb, part_out, 0)
    part_recv[mb] = part_send[mb]
    for c in range(2):
        for b in range(2):
            at = slice(192 * c + 96 * b, 192 * c + 96 * b + 96)
            response[c, b] = weight0[b] * direction[at, :] + weight1[b] * residual[at, :]

    def part_in(k, c):
        part_copy(k, 0).wait_recv()
        return c

    lax.fori_loop(1, nb, part_in, 0)
    density[...] = jnp.sum(part_recv[...], axis=0)[0:12, :]

    def sent(k, c):
        for rnd in range(5):
            ga_copy(rnd, k).wait_send()
        for rnd in range(3):
            small_copy(rnd, k, None).wait_send()
        return c

    lax.fori_loop(1, GROUPS, sent, 0)

    def band_sent(k, c):
        psi_copy(k, None).wait_send()
        part_copy(k, None).wait_send()
        return c

    lax.fori_loop(1, nb, band_sent, 0)


def per_device(psi, vloc, dv, beta, dij, atom_type, stick_xy, band_shift):
    def padded(plane):
        cube = plane.reshape(PLANES, GRID, GRID)
        cube = jnp.pad(cube, ((0, 0), (0, 0), (0, 128 - GRID)))
        return jnp.moveaxis(cube, 0, 1).reshape(GRID, PLANES * 128)

    vmem = pl.BlockSpec(memory_space=pltpu.VMEM)
    smem = pl.BlockSpec(memory_space=pltpu.SMEM)
    dma = pltpu.SemaphoreType.DMA
    response, density = pl.pallas_call(
        kernel,
        out_shape=(
            jax.ShapeDtypeStruct((2, 2, GRID, 128), f32),
            jax.ShapeDtypeStruct((12, PLANES * 128), f32),
        ),
        in_specs=[smem, smem, vmem, vmem, vmem, pl.BlockSpec(memory_space=pl.ANY)] + [vmem] * 13,
        out_specs=(vmem, vmem),
        scratch_shapes=[
            pltpu.VMEM((2, 128, GRID, 128), f32),
            pltpu.VMEM((8, 2, 2, GRID, 128), bf16),
            pltpu.VMEM((256, 2048), bf16),
            pltpu.VMEM((16, 2048), f32),
            pltpu.VMEM((5, GROUPS, ROWS, 128), f32),
            pltpu.VMEM((5, GROUPS, ROWS, 128), f32),
            pltpu.VMEM((3, 16, 128), f32),
            pltpu.VMEM((3, GROUPS, 16, 128), f32),
            pltpu.VMEM((8, 16, 768), f32),
            pltpu.VMEM((8, 16, 768), f32),
            pltpu.VMEM((768, 2048), bf16),
            pltpu.VMEM((384, 256), f32),
            pltpu.VMEM((192, 512), bf16),
            pltpu.VMEM((192, 512), bf16),
            pltpu.VMEM((128, 1536), bf16),
            pltpu.VMEM((128, 1536), bf16),
            pltpu.VMEM((192, 1536), f32),
            pltpu.VMEM((192, 1536), f32),
            pltpu.VMEM((192, 1536), f32),
            pltpu.VMEM((768, 256), bf16),
            pltpu.VMEM((4, 128, 128), f32),
            pltpu.VMEM((4, 128, 128), f32),
            pltpu.VMEM((128, 128), f32),
            pltpu.VMEM((2, 384, 128), f32),
            pltpu.VMEM((384, 128), f32),
            pltpu.VMEM((GRID, 128), f32),
            pltpu.VMEM((8, 2048), f32),
            pltpu.VMEM((GRID, 768), f32),
            dma,
            dma((8,)),
            dma((8,)),
            dma((5, GROUPS)),
            dma((5, GROUPS)),
            dma((3, GROUPS)),
            dma((3, GROUPS)),
            dma((8,)),
            dma((8,)),
        ],
        compiler_params=pltpu.CompilerParams(
            collective_id=0, has_side_effects=True, vmem_limit_bytes=60 * 1024 * 1024
        ),
    )(
        band_shift,
        dij.reshape(32),
        psi,
        padded(vloc),
        padded(dv),
        beta,
        jnp.repeat(atom_type, 4).reshape(1, 128),
        stick_xy.reshape(1, 2048),
        *tables(2),
    )
    cells = density.reshape(12, PLANES, 128)[:, :, :GRID]
    return response, jnp.moveaxis(cells, 0, 1).reshape(PLANES, 12 * GRID)


def solution(mesh):
    return jax.shard_map(
        per_device,
        mesh=mesh,
        in_specs=(
            P(None, "band", None, "ga"),
            P("ga", None),
            P("ga", None),
            P(None, None, None, "ga"),
            P(),
            P(),
            P(),
            P("band"),
        ),
        out_specs=(P(None, "band", None, "ga"), P("ga", "band")),
        check_vma=False,
    )
```

```python
import functools
import math

import jax
import jax.numpy as jnp
import numpy as np
from jax import lax
from jax.experimental import pallas as pl
from jax.experimental.pallas import tpu as pltpu
from jax.sharding import PartitionSpec as P

GRID = 96
SIDE = 64
GROUPS = 16
PLANES = 6
ROWS = 24
MESH = pl.DeviceIdType.MESH
f32 = jnp.float32
bf16 = jnp.bfloat16


def complex_table(angle):
    cos, sin = np.cos(angle), np.sin(angle)
    return np.array([[cos, -sin], [sin, cos]]) / math.sqrt(GRID)


def halves(table):
    high = np.asarray(table, np.float32).astype(jnp.bfloat16)
    low = (table - high.astype(np.float64)).astype(jnp.bfloat16)
    return high, low


def tables(bands):
    unit = 2.0 * math.pi / GRID
    cells = np.arange(GRID)
    freqs = np.arange(SIDE) - SIDE // 2
    along_z = complex_table(unit * (cells[:, None] * cells[None, :] % GRID))
    along_z = along_z.reshape(2, 2, GROUPS, PLANES, GRID)
    z_table = np.einsum("oidpk,be->dopbiek", along_z, np.eye(bands))
    z_table = z_table.reshape(GROUPS * 2 * PLANES * bands, 2 * bands * GRID)
    along_x = np.zeros((2, 2, SIDE, 128))
    along_x[..., :GRID] = complex_table(unit * (freqs[:, None] * cells[None, :] % GRID))
    x_table = np.einsum("oikx,be->ibkoex", along_x, np.eye(2)).reshape(256, 512)
    along_y = complex_table(unit * (cells[:, None] * freqs[None, :] % GRID))
    along_y = along_y.reshape(2, 2, GRID, 16, 4)
    y_table = np.einsum("oiygl->oyilg", along_y).reshape(192, 128)
    out = []
    for table in (z_table, z_table.T, x_table, x_table.T, y_table):
        out.extend(halves(np.ascontiguousarray(table)))
    high, low = halves(np.ascontiguousarray(y_table.T))
    out.append(np.concatenate([high, high, low], axis=1))
    return [jnp.asarray(t) for t in out]


def dot(a, b):
    return lax.dot_general(a, b, (((1,), (0,)), ((), ())), preferred_element_type=f32)


def dot_nt(a, b):
    return lax.dot_general(a, b, (((1,), (1,)), ((), ())), preferred_element_type=f32)


def split(x):
    high = x.astype(bf16)
    return high, (x - high.astype(f32)).astype(bf16)


def left(high, low, x):
    xh, xl = split(x)
    return dot(
        jnp.concatenate([high, high, low], axis=1), jnp.concatenate([xh, xl, xh], axis=0)
    )


def right(ah, al, high, low):
    return dot(
        jnp.concatenate([ah, al, ah], axis=1), jnp.concatenate([high, high, low], axis=0)
    )


def row_sum(x):
    return jnp.sum(jnp.sum(x.reshape(-1, 8, 128), axis=0), axis=0, keepdims=True)


def lane_total(row):
    return jnp.sum(row, axis=1, keepdims=True)


def kernel(
    shift, dij, kind, psi, sticks, zh, zl,
    vloc_hbm, dv_hbm, zth_hbm, ztl_hbm, xh_hbm, xl_hbm, xth_hbm, xtl_hbm,
    yh_hbm, yl_hbm, yt3_hbm, beta_hbm,
    response, density,
    vloc_flat, dv_flat, zth, ztl, xh, xl, xth, xtl, yh, yl, yt3,
    beta, vloc, dv, cells, occupied, onehot, mask, send, recv, small_send, small_recv,
    part_send, part_recv, lhs, grid, eh, el, dh, dl, psi_field, field0, field1,
    q, proj, coef, couple, vec, image, kin, own, dens,
    load_sem, psi_ssem, psi_rsem, ssem, rsem, tssem, trsem, dssem, drsem,
):
    me = lax.axis_index("ga")
    mb = lax.axis_index("band")
    nb = 8

    barrier = pltpu.get_barrier_semaphore()

    def greet_ga(k, c):
        pl.semaphore_signal(
            barrier, inc=1, device_id=(lax.rem(me + k, GROUPS), mb), device_id_type=MESH
        )
        return c

    def greet_band(k, c):
        pl.semaphore_signal(
            barrier, inc=1, device_id=(me, lax.rem(mb + k, nb)), device_id_type=MESH
        )
        return c

    lax.fori_loop(1, GROUPS, greet_ga, 0)
    lax.fori_loop(1, nb, greet_band, 0)
    loads = {}
    pairs = dict(
        dv=(dv_hbm, dv_flat), xh=(xh_hbm, xh), xl=(xl_hbm, xl), yh=(yh_hbm, yh),
        yl=(yl_hbm, yl), yt3=(yt3_hbm, yt3), xth=(xth_hbm, xth), xtl=(xtl_hbm, xtl),
        zth=(zth_hbm, zth), ztl=(ztl_hbm, ztl), vloc=(vloc_hbm, vloc_flat),
        beta=(beta_hbm, beta),
    )
    for at, (name, (source, target)) in enumerate(pairs.items()):
        loads[name] = pltpu.make_async_copy(source, target, load_sem.at[at])
        loads[name].start()

    def ga_copy(rnd, k):
        other = lax.rem(me + k, GROUPS)
        return pltpu.make_async_remote_copy(
            src_ref=send.at[rnd, other],
            dst_ref=recv.at[rnd, me],
            send_sem=ssem.at[rnd, other],
            recv_sem=rsem.at[rnd, me],
            device_id=(other, mb),
            device_id_type=MESH,
        )

    def ga_landed(rnd, k):
        other = lax.rem(me + k, GROUPS)
        return pltpu.make_async_remote_copy(
            src_ref=send.at[rnd, other],
            dst_ref=recv.at[rnd, other],
            send_sem=ssem.at[rnd, other],
            recv_sem=rsem.at[rnd, other],
            device_id=(other, mb),
            device_id_type=MESH,
        )

    def exchange(rnd):
        def body(k, c):
            ga_copy(rnd, k).start()
            return c

        lax.fori_loop(1, GROUPS, body, 0)
        recv[rnd, me] = send[rnd, me]

    @jax.named_scope("arrived")
    def arrived(rnd):
        def body(k, c):
            ga_landed(rnd, k).wait_recv()
            return c

        lax.fori_loop(1, GROUPS, body, 0)

    def small_copy(rnd, k, slot):
        other = lax.rem(me + k, GROUPS)
        return pltpu.make_async_remote_copy(
            src_ref=small_send.at[rnd],
            dst_ref=small_recv.at[rnd, me if slot is None else other],
            send_sem=tssem.at[rnd, other],
            recv_sem=trsem.at[rnd, me if slot is None else other],
            device_id=(other, mb),
            device_id_type=MESH,
        )

    def small_exchange(rnd):
        def body(k, c):
            small_copy(rnd, k, None).start()
            return c

        lax.fori_loop(1, GROUPS, body, 0)
        small_recv[rnd, me] = small_send[rnd]

    def small_total(rnd):
        def body(k, c):
            small_copy(rnd, k, 0).wait_recv()
            return c

        with jax.named_scope("small_wait"):
            lax.fori_loop(1, GROUPS, body, 0)
        return jnp.sum(small_recv[rnd], axis=0)

    def psi_copy(k, slot):
        other = lax.rem(mb + k, nb)
        return pltpu.make_async_remote_copy(
            src_ref=psi,
            dst_ref=occupied.at[mb if slot is None else other],
            send_sem=psi_ssem.at[other],
            recv_sem=psi_rsem.at[mb if slot is None else other],
            device_id=(me, other),
            device_id_type=MESH,
        )

    def part_copy(k, slot):
        other = lax.rem(mb + k, nb)
        return pltpu.make_async_remote_copy(
            src_ref=part_send.at[other],
            dst_ref=part_recv.at[mb if slot is None else other],
            send_sem=dssem.at[other],
            recv_sem=drsem.at[mb if slot is None else other],
            device_id=(me, other),
            device_id_type=MESH,
        )

    with jax.named_scope("z_psi"):
        wide = psi[...].reshape(384, 128)
        send[0] = dot(
            jnp.concatenate([zh[...], zl[...]], axis=1),
            jnp.concatenate([wide, wide], axis=0),
        ).reshape(GROUPS, ROWS, 128)
    with jax.named_scope("barrier"):
        pl.semaphore_wait(barrier, GROUPS - 1 + nb - 1)
    exchange(0)

    def psi_out(k, c):
        psi_copy(k, None).start()
        return c

    lax.fori_loop(1, nb, psi_out, 0)
    occupied[mb] = psi[...]

    def places(xy):
        flat = xy.astype(f32)
        y = jnp.floor((flat + 0.5) * (1.0 / GRID))
        x = flat - GRID * y
        fy = jnp.where(y >= GRID // 2, y - GRID, y)
        fx = jnp.where(x >= GRID // 2, x - GRID, x)
        return fy, fx

    with jax.named_scope("tables"):
        fy, fx = places(sticks[...])
        ky = fy + SIDE // 2
        kx = fx + SIDE // 2
        high = jnp.floor(ky * 0.25)
        low = (ky - 4.0 * high) * SIDE + kx
        for k in range(GROUPS):
            own[0:1, 128 * k : 128 * k + 128] = low[k : k + 1, :]
            own[1:2, 128 * k : 128 * k + 128] = high[k : k + 1, :]
        mask[...] = (
            lax.broadcasted_iota(jnp.int32, (16, 2048), 0).astype(f32) == own[1:2, :]
        ).astype(f32)

        def fill(k, c):
            lanes = pl.ds(pl.multiple_of(k * 256, 256), 256)
            ids = lax.broadcasted_iota(jnp.int32, (256, 256), 0).astype(f32)
            onehot[:, lanes] = (ids == own[0:1, lanes]).astype(f32).astype(bf16)
            return c

        lax.fori_loop(0, 8, fill, 0)
        oy, ox = places(sticks[pl.ds(me, 1), :])
        kz = lax.broadcasted_iota(jnp.int32, (GRID, 128), 0).astype(f32)
        fz = jnp.where(kz >= GRID // 2, kz - GRID, kz)
        kin[...] = (fz * fz + (oy * oy + ox * ox)) * (4.0 / (GRID * GRID))

    row = lax.broadcasted_iota(jnp.int32, (128, 128), 0)
    lane = lax.broadcasted_iota(jnp.int32, (128, 128), 1)

    def couple_all():
        atom = lax.broadcasted_iota(jnp.int32, (1, 128), 1) // 4
        kinds = jnp.zeros((1, 128), jnp.int32)
        for a in range(32):
            kinds = jnp.where(atom == a, kind[a], kinds)
        same = (row // 4) == (lane // 4)
        first = kinds == 0
        total = jnp.zeros((128, 128), f32)
        for i in range(4):
            for k in range(4):
                value = jnp.where(first, dij[0, i, k], dij[1, i, k])
                here = same & ((row % 4) == i) & ((lane % 4) == k)
                total = total + jnp.where(here, value, 0.0)
        couple[...] = total

    def unpack(flat, out):
        def body(g, c):
            piece = flat[:, pl.ds(pl.multiple_of(g * 384, 384), 384)]
            tail = jnp.zeros((PLANES, 32), f32)
            for r in range(4):
                if r < 3:
                    cut = piece[:, 96 * r : 96 * r + 128]
                else:
                    cut = jnp.concatenate([piece[:, 288:384], tail], axis=1)
                cells[pl.ds(pl.multiple_of(g * 32, 32) + 8 * r, PLANES), :] = cut
            return c

        lax.fori_loop(0, 24, body, 0)
        for p in range(PLANES):
            out[:, 128 * p : 128 * p + 128] = cells[pl.ds(p, GRID, stride=8), :]

    with jax.named_scope("couple"):
        couple_all()
    with jax.named_scope("unpack"):
        loads["dv"].wait()
        unpack(dv_flat, dv)
        loads["vloc"].wait()
        unpack(vloc_flat, vloc)
    for name in ("xh", "xl", "yh", "yl", "yt3", "xth", "xtl", "zth", "ztl"):
        loads[name].wait()
    ones = jnp.ones((256, 128), bf16)

    def fill_planes(rnd, out):

        def body(k, c):
            src = lax.rem(me + k, GROUPS)

            @pl.when(k > 0)
            def _():
                ga_landed(rnd, k).wait_recv()

            piece = recv[rnd, src]
            upper = piece.astype(bf16).astype(f32)
            lower = piece - upper
            cols = pl.ds(pl.multiple_of(src * 128, 128), 128)
            keep = mask[:, cols]
            for r in range(ROWS):
                lhs[16 * r : 16 * r + 16, cols] = (
                    jnp.broadcast_to(upper[r : r + 1], (16, 128)) * keep
                ).astype(bf16)
                lhs[384 + 16 * r : 400 + 16 * r, cols] = (
                    jnp.broadcast_to(lower[r : r + 1], (16, 128)) * keep
                ).astype(bf16)
            return c

        with jax.named_scope("fill_lhs"):
            lax.fori_loop(0, GROUPS, body, 0)
        with jax.named_scope("fill_dot"):
            both = dot_nt(lhs[...], onehot[...])
            grid[...] = both[0:384] + both[384:768]
        with jax.named_scope("fill_x"):
            for t in range(2):
                lanes = slice(128 * t, 128 * t + 128)
                data = jnp.concatenate([grid[0:192, lanes], grid[192:384, lanes]], axis=1)
                ah, al = split(data)
                along = right(ah, al, xh[...], xl[...])
                uh, ul = split(along)
                eh[...] = uh
                el[...] = ul
                for c in range(2):
                    for j in range(2):
                        rows = slice(16 * (4 * c + 2 * t + j), 16 * (4 * c + 2 * t + j) + 16)
                        cols = slice(128 * (2 * c + j), 128 * (2 * c + j) + 128)
                        for i in range(12):
                            dh[rows, 128 * i : 128 * i + 128] = eh[16 * i : 16 * i + 16, cols]
                            dl[rows, 128 * i : 128 * i + 128] = el[16 * i : 16 * i + 16, cols]
        with jax.named_scope("fill_y"):
            for part in range(6):
                lanes = slice(256 * part, 256 * part + 256)
                out[:, lanes] = dot(
                    jnp.concatenate([yh[...], yh[...], yl[...]], axis=1),
                    jnp.concatenate([dh[:, lanes], dl[:, lanes], dh[:, lanes]], axis=0),
                )

    def to_sticks(rnd, potential, source):
        with jax.named_scope("stick_y"):
            for p in range(PLANES):
                lanes = slice(256 * p, 256 * p + 256)
                pot = potential[:, 128 * p : 128 * p + 128]
                pot = jnp.concatenate([pot, pot], axis=1)
                pot = jnp.concatenate([pot, pot], axis=0)
                ah, al = split(source[:, lanes] * pot)
                along = dot(yt3[...], jnp.concatenate([ah, al, ah], axis=0))
                uh, ul = split(along)
                dh[:, lanes] = uh
                dl[:, lanes] = ul
        with jax.named_scope("stick_x"):
            for t in range(2):
                for c in range(2):
                    for j in range(2):
                        rows = slice(16 * (4 * c + 2 * t + j), 16 * (4 * c + 2 * t + j) + 16)
                        cols = slice(128 * (2 * c + j), 128 * (2 * c + j) + 128)
                        for i in range(12):
                            eh[16 * i : 16 * i + 16, cols] = dh[rows, 128 * i : 128 * i + 128]
                            el[16 * i : 16 * i + 16, cols] = dl[rows, 128 * i : 128 * i + 128]
                along = right(eh[...], el[...], xth[...], xtl[...])
                uh, ul = split(along)
                lanes = slice(128 * t, 128 * t + 128)
                for c in range(2):
                    q[192 * c : 192 * c + 192, lanes] = uh[:, 128 * c : 128 * c + 128]
                    q[384 + 192 * c : 576 + 192 * c, lanes] = ul[:, 128 * c : 128 * c + 128]

        def body(k, carry):
            pair = lax.rem(me // 2 + k, 8)
            lanes = pl.ds(pl.multiple_of(pair * 256, 256), 256)
            place = onehot[:, lanes]
            keep = mask[:, lanes]
            both = dot(q[...], place)
            found = both[0:384] + both[384:768]
            picked = jnp.sum(found.reshape(ROWS, 16, 256) * keep[None], axis=1)
            send[rnd, 2 * pair] = picked[:, 0:128]
            send[rnd, 2 * pair + 1] = picked[:, 128:256]

            @pl.when(k > 0)
            def _():
                post(rnd, lax.rem(me // 2 + k + 7, 8))

            return carry

        with jax.named_scope("stick_pick"):
            lax.fori_loop(0, 8, body, 0)
            post(rnd, lax.rem(me // 2 + 7, 8))
            recv[rnd, me] = send[rnd, me]

    def post(rnd, pair):
        for half in range(2):
            owner = 2 * pair + half

            @pl.when(owner != me)
            def _():
                ga_copy(rnd, owner - me + GROUPS).start()

    def z_forward(rnd):
        return left(zth[...], ztl[...], recv[rnd].reshape(384, 128))

    def project(load, count, source):
        step = 4

        def body(g, c):
            sums = [[None] * 4 for _ in range(step)]
            for z in range(GRID // 8):
                v = [source[96 * n + 8 * z : 96 * n + 8 * z + 8, :] for n in range(4)]
                for t in range(step):
                    p0, p1 = load(g * step + t, 8 * z, 8)
                    for b in range(2):
                        re = p0 * v[b] + p1 * v[2 + b]
                        im = p0 * v[2 + b] - p1 * v[b]
                        sums[t][b] = re if z == 0 else sums[t][b] + re
                        sums[t][2 + b] = im if z == 0 else sums[t][2 + b] + im
            for t in range(step):
                for o in range(4):
                    proj[o, pl.ds(g * step + t, 1), :] = jnp.sum(
                        sums[t][o], axis=0, keepdims=True
                    )
            return c

        with jax.named_scope("project"):
            lax.fori_loop(0, count // step, body, 0)

    def projections(o, count):
        ph, pl_ = split(proj[o, 0:count, :])
        one = jnp.ones((8, 128), bf16)
        return dot_nt(
            jnp.concatenate([one, one], axis=1), jnp.concatenate([ph, pl_], axis=1)
        )[0:1, :]

    def spread(matrix, values):
        count = matrix.shape[0]
        for o in range(4):
            mh, ml = split(matrix * values[o : o + 1, :])
            coef[o, 0:count, :] = dot(jnp.concatenate([mh, ml], axis=1), ones)

    def apply(load, count, base):
        rows = 24
        for z in range(GRID // rows):

            def body(g, acc):
                for t in range(4):
                    j = g * 4 + t
                    p0, p1 = load(j, z * rows, rows)
                    out = []
                    for b in range(2):
                        cr = coef[b, pl.ds(j, 1), :]
                        ci = coef[2 + b, pl.ds(j, 1), :]
                        out.append(acc[2 * b] + (p0 * cr - p1 * ci))
                        out.append(acc[2 * b + 1] + (p0 * ci + p1 * cr))
                    acc = out
                return tuple(acc)

            init = tuple(
                base[192 * c + 96 * b + z * rows : 192 * c + 96 * b + z * rows + rows, :]
                for b in range(2)
                for c in range(2)
            )
            with jax.named_scope("apply"):
                done = lax.fori_loop(0, count // 4, body, init)
            for b in range(2):
                for c in range(2):
                    at = 192 * c + 96 * b + z * rows
                    image[at : at + rows, :] = done[2 * b + c]

    def beta_rows(j, at=0, rows=GRID):
        return beta[0, j, at : at + rows, :], beta[1, j, at : at + rows, :]

    def psi_rows(m, at=0, rows=GRID):
        owner, b = m // 2, m % 2
        return (
            occupied[owner, 0, b, at : at + rows, :].astype(f32),
            occupied[owner, 1, b, at : at + rows, :].astype(f32),
        )

    fill_planes(0, psi_field)
    to_sticks(1, dv, psi_field)

    def psi_in(k, c):
        psi_copy(k, 0).wait_recv()
        return c

    arrived(1)
    vec[1] = z_forward(1)
    lax.fori_loop(1, nb, psi_in, 0)

    project(psi_rows, 16, vec.at[1])
    small_send[0] = jnp.zeros((8, 128), f32)
    for o in range(4):
        small_send[0, o : o + 1, 0:16] = projections(o, 16)
    small_exchange(0)
    found = small_total(0) * (1.0 / (2.0 * GRID * 2048))
    eye = (row[0:16] == lane[0:16]).astype(f32)
    spread(eye, found)
    vec[1] = -vec[1]
    apply(psi_rows, 16, vec.at[1])
    vec[0] = image[...]

    def transform_out(rnd, source):
        send[rnd] = left(zh[...], zl[...], source[...]).reshape(GROUPS, ROWS, 128)
        exchange(rnd)

    def stick_sum(a, b, weight=None):
        out = []
        for n in range(2):
            s0 = slice(96 * n, 96 * n + 96)
            s1 = slice(192 + 96 * n, 288 + 96 * n)
            both = a[s0, :] * b[s0, :] + a[s1, :] * b[s1, :]
            if weight is not None:
                both = both * (kin[...] + shift[n])
            out.append(row_sum(both))
        return out

    def grid_sum(a, b):
        out = []
        for n in range(2):
            total = jnp.zeros((1, 128), f32)
            for p in range(PLANES):
                lanes = slice(128 * (2 * p + n), 128 * (2 * p + n) + 128)
                pot = vloc[:, 128 * p : 128 * p + 128]
                both = a[0:96, lanes] * b[0:96, lanes] + a[96:192, lanes] * b[96:192, lanes]
                total = total + row_sum(both * pot)
            out.append(total)
        return out

    half = lax.broadcasted_iota(jnp.int32, (1, 128), 1) < 64

    def packed(pair):
        a, b = (r + pltpu.roll(r, 64, 1) for r in pair)
        return jnp.where(half, a, b)

    def unpacked(both):
        return [
            lane_total(jnp.where(half, both, 0.0)),
            lane_total(jnp.where(half, 0.0, both)),
        ]

    def band_dots(values, coupled):
        both = values * coupled
        return [lane_total(both[b : b + 1] + both[2 + b : 3 + b]) for b in range(2)]

    ch, cl = split(couple[...])

    def coupled_rows(values):
        vh, vl = split(values)
        return dot_nt(
            jnp.concatenate([vh, vl, vh], axis=1), jnp.concatenate([ch, ch, cl], axis=1)
        )

    direction = vec.at[0]
    transform_out(2, direction)
    loads["beta"].wait()
    project(beta_rows, 128, direction)
    small_send[1] = jnp.zeros((8, 128), f32)
    for o in range(4):
        small_send[1, o : o + 1, :] = projections(o, 128)
    norms = stick_sum(direction, direction)
    curves = stick_sum(direction, direction, True)
    fill_planes(2, field0)
    local = grid_sum(field0, field0)
    small_send[1, 4:5, :] = packed(norms)
    small_send[1, 5:6, :] = packed([curves[b] + local[b] for b in range(2)])
    small_exchange(1)
    to_sticks(3, vloc, field0)
    sums = small_total(1)
    values0 = sums[0:4]
    coupled0 = coupled_rows(sums)[0:4]
    nonlocal0 = band_dots(values0, coupled0)
    norm0 = unpacked(sums[4:5])
    curve0 = [c + n for c, n in zip(unpacked(sums[5:6]), nonlocal0)]
    alpha0 = [norm0[b] / curve0[b] for b in range(2)]
    spread(couple[...], values0)
    for c in range(2):
        for b in range(2):
            at = slice(192 * c + 96 * b, 192 * c + 96 * b + 96)
            vec[1, at, :] = direction[at, :] * (kin[...] + shift[b])
    apply(beta_rows, 128, vec.at[1])
    arrived(3)
    image[...] += z_forward(3)
    residual = vec.at[1]
    for c in range(2):
        for b in range(2):
            at = slice(192 * c + 96 * b, 192 * c + 96 * b + 96)
            residual[at, :] = direction[at, :] - alpha0[b] * image[at, :]

    transform_out(4, residual)
    project(beta_rows, 128, residual)
    small_send[2] = jnp.zeros((8, 128), f32)
    for o in range(4):
        small_send[2, o : o + 1, :] = projections(o, 128)
    norms = stick_sum(residual, residual)
    selfs = stick_sum(residual, residual, True)
    crosses = stick_sum(residual, direction, True)
    fill_planes(4, field1)
    self_local = grid_sum(field1, field1)
    cross_local = grid_sum(field1, field0)
    small_send[2, 4:5, :] = packed(norms)
    small_send[2, 5:6, :] = packed([selfs[b] + self_local[b] for b in range(2)])
    small_send[2, 6:7, :] = packed([crosses[b] + cross_local[b] for b in range(2)])
    small_exchange(2)
    with jax.named_scope("products"):
        for p in range(PLANES):
            for b in range(2):
                lanes = slice(128 * (2 * p + b), 128 * (2 * p + b) + 128)
                for n, field in enumerate((field0, field1)):
                    dens[96 * n : 96 * n + 96, lanes] = 4.0 * (
                        psi_field[0:96, lanes] * field[0:96, lanes]
                        + psi_field[96:192, lanes] * field[96:192, lanes]
                    )
    sums = small_total(2)
    values1 = sums[0:4]
    coupled1 = coupled_rows(sums)[0:4]
    self_dots = band_dots(values1, coupled1)
    cross_dots = band_dots(values1, coupled0)
    weight0, weight1 = [], []
    norm1, self1, cross1 = (unpacked(sums[n : n + 1]) for n in (4, 5, 6))
    for b in range(2):
        ratio = norm1[b] / norm0[b]
        self_curve = self1[b] + self_dots[b]
        cross_curve = cross1[b] + cross_dots[b]
        curve = self_curve + ratio * (2.0 * cross_curve + ratio * curve0[b])
        alpha = norm1[b] / curve
        weight0.append(alpha0[b] + alpha * ratio)
        weight1.append(alpha)

    with jax.named_scope("density"):
        for p in range(PLANES):
            total = jnp.zeros((GRID, 128), f32)
            for b in range(2):
                lanes = slice(128 * (2 * p + b), 128 * (2 * p + b) + 128)
                total = total + weight0[b] * dens[0:96, lanes] + weight1[b] * dens[96:192, lanes]
            for i in range(nb):
                part_send[i, 12 * p : 12 * p + 12, :] = total[12 * i : 12 * i + 12, :]

    def part_out(k, c):
        part_copy(k, None).start()
        return c

    lax.fori_loop(1, nb, part_out, 0)
    part_recv[mb] = part_send[mb]
    for c in range(2):
        for b in range(2):
            at = slice(192 * c + 96 * b, 192 * c + 96 * b + 96)
            response[c, b] = weight0[b] * direction[at, :] + weight1[b] * residual[at, :]

    def part_in(k, c):
        part_copy(k, 0).wait_recv()
        return c

    with jax.named_scope("part_wait"):
        lax.fori_loop(1, nb, part_in, 0)
    cells[0:72, :] = jnp.sum(part_recv[...], axis=0)
    for y in range(12):
        density[:, 96 * y : 96 * y + 96] = cells[pl.ds(y, PLANES, stride=12), :][:, 0:96]

    def sent(k, c):
        for rnd in range(5):
            ga_copy(rnd, k).wait_send()
        for rnd in range(3):
            small_copy(rnd, k, None).wait_send()
        return c

    lax.fori_loop(1, GROUPS, sent, 0)

    def band_sent(k, c):
        psi_copy(k, None).wait_send()
        part_copy(k, None).wait_send()
        return c

    lax.fori_loop(1, nb, band_sent, 0)


def per_device(psi, vloc, dv, beta, dij, atom_type, stick_xy, band_shift):
    vmem = pl.BlockSpec(memory_space=pltpu.VMEM)
    smem = pl.BlockSpec(memory_space=pltpu.SMEM)
    dma = pltpu.SemaphoreType.DMA
    every = tables(2)
    early, late = every[:2], every[2:]
    response, density = pl.pallas_call(
        kernel,
        out_shape=(
            jax.ShapeDtypeStruct((2, 2, GRID, 128), f32),
            jax.ShapeDtypeStruct((PLANES, 12 * GRID), f32),
        ),
        in_specs=[smem] * 3 + [vmem] * 4 + [pl.BlockSpec(memory_space=pl.ANY)] * 12,
        out_specs=(vmem, vmem),
        scratch_shapes=[
            pltpu.VMEM((PLANES, GRID * GRID), f32),
            pltpu.VMEM((PLANES, GRID * GRID), f32),
            *[pltpu.VMEM(t.shape, t.dtype) for t in late],
            pltpu.VMEM((2, 128, GRID, 128), f32),
            pltpu.VMEM((GRID, 768), f32),
            pltpu.VMEM((GRID, 768), f32),
            pltpu.VMEM((768, 128), f32),
            pltpu.VMEM((8, 2, 2, GRID, 128), bf16),
            pltpu.VMEM((256, 2048), bf16),
            pltpu.VMEM((16, 2048), f32),
            pltpu.VMEM((5, GROUPS, ROWS, 128), f32),
            pltpu.VMEM((5, GROUPS, ROWS, 128), f32),
            pltpu.VMEM((3, 8, 128), f32),
            pltpu.VMEM((3, GROUPS, 8, 128), f32),
            pltpu.VMEM((8, 72, 128), f32),
            pltpu.VMEM((8, 72, 128), f32),
            pltpu.VMEM((768, 2048), bf16),
            pltpu.VMEM((384, 256), f32),
            pltpu.VMEM((192, 512), bf16),
            pltpu.VMEM((192, 512), bf16),
            pltpu.VMEM((128, 1536), bf16),
            pltpu.VMEM((128, 1536), bf16),
            pltpu.VMEM((192, 1536), f32),
            pltpu.VMEM((192, 1536), f32),
            pltpu.VMEM((192, 1536), f32),
            pltpu.VMEM((768, 256), bf16),
            pltpu.VMEM((4, 128, 128), f32),
            pltpu.VMEM((4, 128, 128), f32),
            pltpu.VMEM((128, 128), f32),
            pltpu.VMEM((2, 384, 128), f32),
            pltpu.VMEM((384, 128), f32),
            pltpu.VMEM((GRID, 128), f32),
            pltpu.VMEM((8, 2048), f32),
            pltpu.VMEM((192, 1536), f32),
            dma((12,)),
            dma((8,)),
            dma((8,)),
            dma((5, GROUPS)),
            dma((5, GROUPS)),
            dma((3, GROUPS)),
            dma((3, GROUPS)),
            dma((8,)),
            dma((8,)),
        ],
        compiler_params=pltpu.CompilerParams(
            collective_id=0, has_side_effects=True, vmem_limit_bytes=60 * 1024 * 1024
        ),
    )(
        band_shift, dij, atom_type, psi, stick_xy.reshape(GROUPS, 128), *early,
        vloc, dv, *late, beta,
    )
    return response, density


def solution(mesh):
    return jax.shard_map(
        per_device,
        mesh=mesh,
        in_specs=(
            P(None, "band", None, "ga"),
            P("ga", None),
            P("ga", None),
            P(None, None, None, "ga"),
            P(),
            P(),
            P(),
            P("band"),
        ),
        out_specs=(P(None, "band", None, "ga"), P("ga", "band")),
        check_vma=False,
    )
```

```python
import functools
import math

import jax
import jax.numpy as jnp
import numpy as np
from jax import lax
from jax.experimental import pallas as pl
from jax.experimental.pallas import tpu as pltpu
from jax.sharding import PartitionSpec as P

GRID = 96
SIDE = 64
GROUPS = 16
PLANES = 6
ROWS = 24
MESH = pl.DeviceIdType.MESH
f32 = jnp.float32
bf16 = jnp.bfloat16


def complex_table(angle):
    cos, sin = np.cos(angle), np.sin(angle)
    return np.array([[cos, -sin], [sin, cos]]) / math.sqrt(GRID)


def halves(table):
    high = np.asarray(table, np.float32).astype(jnp.bfloat16)
    low = (table - high.astype(np.float64)).astype(jnp.bfloat16)
    return high, low


def tables(bands):
    unit = 2.0 * math.pi / GRID
    cells = np.arange(GRID)
    freqs = np.arange(SIDE) - SIDE // 2
    along_z = complex_table(unit * (cells[:, None] * cells[None, :] % GRID))
    along_z = along_z.reshape(2, 2, GROUPS, PLANES, GRID)
    z_table = np.einsum("oidpk,be->dopbiek", along_z, np.eye(bands))
    z_table = z_table.reshape(GROUPS * 2 * PLANES * bands, 2 * bands * GRID)
    along_x = np.zeros((2, 2, SIDE, 128))
    along_x[..., :GRID] = complex_table(unit * (freqs[:, None] * cells[None, :] % GRID))
    x_table = np.einsum("oikx,be->ibkoex", along_x, np.eye(2)).reshape(256, 512)
    along_y = complex_table(unit * (cells[:, None] * freqs[None, :] % GRID))
    along_y = along_y.reshape(2, 2, GRID, 8, 8)
    y_table = np.einsum("oiygl->oyilg", along_y).reshape(192, 128)
    out = []
    for table in (z_table, z_table.T, x_table, x_table.T, y_table):
        out.extend(halves(np.ascontiguousarray(table)))
    high, low = halves(np.ascontiguousarray(y_table.T))
    out.append(np.concatenate([high, high, low], axis=1))
    return [jnp.asarray(t) for t in out]


def dot(a, b):
    return lax.dot_general(a, b, (((1,), (0,)), ((), ())), preferred_element_type=f32)


def dot_nt(a, b):
    return lax.dot_general(a, b, (((1,), (1,)), ((), ())), preferred_element_type=f32)


def split(x):
    high = x.astype(bf16)
    return high, (x - high.astype(f32)).astype(bf16)


def left(high, low, x):
    xh, xl = split(x)
    return dot(
        jnp.concatenate([high, high, low], axis=1), jnp.concatenate([xh, xl, xh], axis=0)
    )


def right(ah, al, high, low):
    return dot(
        jnp.concatenate([ah, al, ah], axis=1), jnp.concatenate([high, high, low], axis=0)
    )


def row_sum(x):
    return jnp.sum(jnp.sum(x.reshape(-1, 8, 128), axis=0), axis=0, keepdims=True)


def lane_total(row):
    return jnp.sum(row, axis=1, keepdims=True)


def kernel(
    shift, dij, kind, psi_hbm, sticks_hbm, zh_hbm, zl_hbm, vloc_hbm, dv_hbm, zth_hbm, ztl_hbm, xh_hbm, xl_hbm, xth_hbm, xtl_hbm,
    yh_hbm, yl_hbm, yt3_hbm, beta_hbm,
    first_out, second_out, weights_out, cells_out,
    psi, sticks, zh, zl, vloc_flat, dv_flat, zth, ztl, xh, xl, xth, xtl, yh, yl, yt3,
    beta, vloc, dv, cells, occupied, onehot, mask, send, recv, small_send, small_recv,
    part_send, part_recv, lhs, grid, ex, eh, el, dh, dl, psi_field, field0, field1,
    q, proj, coef, couple, vec, image, kin, own, dens,
    load_sem, psi_ssem, psi_rsem, ssem, rsem, tssem, trsem, dssem, drsem,
):
    me = lax.axis_index("ga")
    mb = lax.axis_index("band")
    nb = 8

    barrier = pltpu.get_barrier_semaphore()

    def greet_ga(k, c):
        pl.semaphore_signal(
            barrier, inc=1, device_id=(lax.rem(me + k, GROUPS), mb), device_id_type=MESH
        )
        return c

    def greet_band(k, c):
        pl.semaphore_signal(
            barrier, inc=1, device_id=(me, lax.rem(mb + k, nb)), device_id_type=MESH
        )
        return c

    lax.fori_loop(1, GROUPS, greet_ga, 0)
    lax.fori_loop(1, nb, greet_band, 0)
    loads = {}
    pairs = dict(
        psi=(psi_hbm, psi), zh=(zh_hbm, zh), zl=(zl_hbm, zl), sticks=(sticks_hbm, sticks),
        dv=(dv_hbm, dv_flat), xh=(xh_hbm, xh), xl=(xl_hbm, xl), yh=(yh_hbm, yh),
        yl=(yl_hbm, yl), yt3=(yt3_hbm, yt3), xth=(xth_hbm, xth), xtl=(xtl_hbm, xtl),
        zth=(zth_hbm, zth), ztl=(ztl_hbm, ztl), vloc=(vloc_hbm, vloc_flat),
        beta=(beta_hbm, beta),
    )
    for at, (name, (source, target)) in enumerate(pairs.items()):
        loads[name] = pltpu.make_async_copy(source, target, load_sem.at[at])
        loads[name].start()

    def ga_copy(rnd, k):
        other = lax.rem(me + k, GROUPS)
        return pltpu.make_async_remote_copy(
            src_ref=send.at[rnd, other],
            dst_ref=recv.at[rnd, me],
            send_sem=ssem.at[rnd, other],
            recv_sem=rsem.at[rnd, me],
            device_id=(other, mb),
            device_id_type=MESH,
        )

    def ga_landed(rnd, k):
        other = lax.rem(me + k, GROUPS)
        return pltpu.make_async_remote_copy(
            src_ref=send.at[rnd, other],
            dst_ref=recv.at[rnd, other],
            send_sem=ssem.at[rnd, other],
            recv_sem=rsem.at[rnd, other],
            device_id=(other, mb),
            device_id_type=MESH,
        )

    def exchange(rnd):
        def body(k, c):
            ga_copy(rnd, k).start()
            return c

        lax.fori_loop(1, GROUPS, body, 0)
        recv[rnd, me] = send[rnd, me]

    @jax.named_scope("arrived")
    def arrived(rnd):
        def body(k, c):
            ga_landed(rnd, k).wait_recv()
            return c

        lax.fori_loop(1, GROUPS, body, 0)

    def small_copy(rnd, k, slot):
        other = lax.rem(me + k, GROUPS)
        return pltpu.make_async_remote_copy(
            src_ref=small_send.at[rnd],
            dst_ref=small_recv.at[rnd, me if slot is None else other],
            send_sem=tssem.at[rnd, other],
            recv_sem=trsem.at[rnd, me if slot is None else other],
            device_id=(other, mb),
            device_id_type=MESH,
        )

    def small_exchange(rnd):
        def body(k, c):
            small_copy(rnd, k, None).start()
            return c

        lax.fori_loop(1, GROUPS, body, 0)
        small_recv[rnd, me] = small_send[rnd]

    def small_total(rnd):
        def body(k, c):
            small_copy(rnd, k, 0).wait_recv()
            return c

        with jax.named_scope("small_wait"):
            lax.fori_loop(1, GROUPS, body, 0)
        return jnp.sum(small_recv[rnd], axis=0)

    def psi_copy(k, slot):
        other = lax.rem(mb + k, nb)
        return pltpu.make_async_remote_copy(
            src_ref=psi,
            dst_ref=occupied.at[mb if slot is None else other],
            send_sem=psi_ssem.at[other],
            recv_sem=psi_rsem.at[mb if slot is None else other],
            device_id=(me, other),
            device_id_type=MESH,
        )

    def part_copy(k, slot):
        other = lax.rem(mb + k, nb)
        return pltpu.make_async_remote_copy(
            src_ref=part_send.at[other],
            dst_ref=part_recv.at[mb if slot is None else other],
            send_sem=dssem.at[other],
            recv_sem=drsem.at[mb if slot is None else other],
            device_id=(me, other),
            device_id_type=MESH,
        )

    for name in ("psi", "zh", "zl"):
        loads[name].wait()
    with jax.named_scope("z_psi"):
        wide = psi[...].reshape(384, 128)
        send[0] = dot(
            jnp.concatenate([zh[...], zl[...]], axis=1),
            jnp.concatenate([wide, wide], axis=0),
        ).reshape(GROUPS, ROWS, 128)
    def places(xy):
        flat = xy.astype(f32)
        y = jnp.floor((flat + 0.5) * (1.0 / GRID))
        x = flat - GRID * y
        fy = jnp.where(y >= GRID // 2, y - GRID, y)
        fx = jnp.where(x >= GRID // 2, x - GRID, x)
        return fy, fx

    loads["sticks"].wait()
    with jax.named_scope("tables"):
        fy, fx = places(sticks[...])
        ky = fy + SIDE // 2
        kx = fx + SIDE // 2
        high = jnp.floor(ky * 0.125)
        low = (ky - 8.0 * high) * SIDE + kx
        for k in range(GROUPS):
            own[0:1, 128 * k : 128 * k + 128] = low[k : k + 1, :]
            own[1:2, 128 * k : 128 * k + 128] = high[k : k + 1, :]
        mask[...] = (
            lax.broadcasted_iota(jnp.int32, (8, 2048), 0).astype(f32) == own[1:2, :]
        ).astype(f32)

        def fill(k, c):
            lanes = pl.ds(pl.multiple_of(k * 256, 256), 256)
            ids = lax.broadcasted_iota(jnp.int32, (512, 256), 0).astype(f32)
            onehot[:, lanes] = (ids == own[0:1, lanes]).astype(f32).astype(bf16)
            return c

        lax.fori_loop(0, 8, fill, 0)
        oy, ox = places(sticks[pl.ds(me, 1), :])
        kz = lax.broadcasted_iota(jnp.int32, (GRID, 128), 0).astype(f32)
        fz = jnp.where(kz >= GRID // 2, kz - GRID, kz)
        kin[...] = (fz * fz + (oy * oy + ox * ox)) * (4.0 / (GRID * GRID))

    row = lax.broadcasted_iota(jnp.int32, (128, 128), 0)
    lane = lax.broadcasted_iota(jnp.int32, (128, 128), 1)

    def couple_all():
        atom = lax.broadcasted_iota(jnp.int32, (1, 128), 1) // 4
        kinds = jnp.zeros((1, 128), jnp.int32)
        for a in range(32):
            kinds = jnp.where(atom == a, kind[a], kinds)
        same = (row // 4) == (lane // 4)
        first = kinds == 0
        total = jnp.zeros((128, 128), f32)
        for i in range(4):
            for k in range(4):
                value = jnp.where(first, dij[0, i, k], dij[1, i, k])
                here = same & ((row % 4) == i) & ((lane % 4) == k)
                total = total + jnp.where(here, value, 0.0)
        couple[...] = total

    def unpack(flat, out):
        def body(g, c):
            piece = flat[:, pl.ds(pl.multiple_of(g * 384, 384), 384)]
            tail = jnp.zeros((PLANES, 32), f32)
            for r in range(4):
                if r < 3:
                    cut = piece[:, 96 * r : 96 * r + 128]
                else:
                    cut = jnp.concatenate([piece[:, 288:384], tail], axis=1)
                cells[pl.ds(pl.multiple_of(g * 32, 32) + 8 * r, PLANES), :] = cut
            return c

        lax.fori_loop(0, 24, body, 0)
        for p in range(PLANES):
            out[:, 128 * p : 128 * p + 128] = cells[pl.ds(p, GRID, stride=8), :]

    with jax.named_scope("couple"):
        couple_all()
    with jax.named_scope("barrier"):
        pl.semaphore_wait(barrier, GROUPS - 1 + nb - 1)
    exchange(0)

    def psi_out(k, c):
        psi_copy(k, None).start()
        return c

    lax.fori_loop(1, nb, psi_out, 0)
    occupied[mb] = psi[...]

    with jax.named_scope("unpack"):
        loads["dv"].wait()
        unpack(dv_flat, dv)
    for name in ("xh", "xl", "yh", "yl", "yt3", "xth", "xtl", "zth", "ztl"):
        loads[name].wait()
    ones = jnp.ones((256, 128), bf16)

    def fill_planes(rnd, out):

        def body(k, c):
            src = lax.rem(me + k, GROUPS)

            @pl.when(k > 0)
            def _():
                ga_landed(rnd, k).wait_recv()

            piece = recv[rnd, src]
            upper = piece.astype(bf16).astype(f32)
            lower = piece - upper
            cols = pl.ds(pl.multiple_of(src * 128, 128), 128)
            keep = mask[:, cols]
            for n, part in enumerate((upper, lower)):
                for r in range(0, ROWS, 2):
                    two = [jnp.broadcast_to(part[r + e : r + e + 1], (8, 128)) * keep for e in (0, 1)]
                    at = 192 * n + 8 * r
                    lhs[at : at + 16, cols] = jnp.concatenate(two, axis=0).astype(bf16)
            return c

        with jax.named_scope("fill_lhs"):
            lax.fori_loop(0, GROUPS, body, 0)
        with jax.named_scope("fill_dot"):
            both = dot_nt(lhs[...], onehot[...])
            grid[...] = both[0:192] + both[192:384]
        with jax.named_scope("fill_x"):
            data = [
                jnp.concatenate(
                    [grid[0:96, 128 * t : 128 * t + 128], grid[96:192, 128 * t : 128 * t + 128]],
                    axis=1,
                )
                for t in range(4)
            ]
            ah, al = split(jnp.concatenate(data, axis=0))
            ex[...] = right(ah, al, xh[...], xl[...])
            for c in range(2):
                for t in range(4):
                    rows = slice(16 * (4 * c + t), 16 * (4 * c + t) + 16)
                    for i in range(12):
                        at = 96 * t + 8 * i
                        two = [ex[at : at + 8, 128 * (2 * c + j) : 128 * (2 * c + j) + 128] for j in (0, 1)]
                        uh, ul = split(jnp.concatenate(two, axis=0))
                        dh[rows, 128 * i : 128 * i + 128] = uh
                        dl[rows, 128 * i : 128 * i + 128] = ul
        with jax.named_scope("fill_y"):
            for part in range(6):
                lanes = slice(256 * part, 256 * part + 256)
                out[:, lanes] = dot(
                    jnp.concatenate([yh[...], yh[...], yl[...]], axis=1),
                    jnp.concatenate([dh[:, lanes], dl[:, lanes], dh[:, lanes]], axis=0),
                )

    def to_sticks(rnd, potential, source):
        with jax.named_scope("stick_y"):
            for p in range(PLANES):
                lanes = slice(256 * p, 256 * p + 256)
                pot = potential[:, 128 * p : 128 * p + 128]
                pot = jnp.concatenate([pot, pot], axis=1)
                pot = jnp.concatenate([pot, pot], axis=0)
                ah, al = split(source[:, lanes] * pot)
                along = dot(yt3[...], jnp.concatenate([ah, al, ah], axis=0))
                for c in range(2):
                    for t in range(4):
                        for j in range(2):
                            rows = slice(8 * (8 * c + 2 * t + j), 8 * (8 * c + 2 * t + j) + 8)
                            two = jnp.concatenate([along[rows, 0:128], along[rows, 128:256]], axis=0)
                            uh, ul = split(two)
                            at = 96 * t + 16 * p
                            cols = slice(128 * (2 * c + j), 128 * (2 * c + j) + 128)
                            eh[at : at + 16, cols] = uh
                            el[at : at + 16, cols] = ul
        with jax.named_scope("stick_x"):
            along = right(eh[...], el[...], xth[...], xtl[...])
            uh, ul = split(along)
            for t in range(4):
                for c in range(2):
                    lanes = slice(128 * t, 128 * t + 128)
                    cols = slice(128 * c, 128 * c + 128)
                    q[96 * c : 96 * c + 96, lanes] = uh[96 * t : 96 * t + 96, cols]
                    q[192 + 96 * c : 288 + 96 * c, lanes] = ul[96 * t : 96 * t + 96, cols]

        with jax.named_scope("stick_pick"):
            for k in range(5):
                if k < 4:
                    quad = lax.rem(me // 4 + k, 4)
                    lanes = pl.ds(pl.multiple_of(quad * 512, 512), 512)
                    both = dot(q[...], onehot[:, lanes])
                    found = both[0:192] + both[192:384]
                    picked = jnp.sum(found.reshape(ROWS, 8, 512) * mask[:, lanes][None], axis=1)
                    for n in range(4):
                        send[rnd, 4 * quad + n] = picked[:, 128 * n : 128 * n + 128]
                if k > 0:
                    post(rnd, lax.rem(me // 4 + k + 3, 4))
            recv[rnd, me] = send[rnd, me]

    def post(rnd, quad):
        for n in range(4):
            owner = 4 * quad + n

            @pl.when(owner != me)
            def _():
                ga_copy(rnd, owner - me + GROUPS).start()

    def z_forward(rnd):
        return left(zth[...], ztl[...], recv[rnd].reshape(384, 128))

    def project(load, count, source):
        step = 4

        def body(g, c):
            sums = [[None] * 4 for _ in range(step)]
            for z in range(GRID // 8):
                v = [source[96 * n + 8 * z : 96 * n + 8 * z + 8, :] for n in range(4)]
                for t in range(step):
                    p0, p1 = load(g * step + t, 8 * z, 8)
                    for b in range(2):
                        re = p0 * v[b] + p1 * v[2 + b]
                        im = p0 * v[2 + b] - p1 * v[b]
                        sums[t][b] = re if z == 0 else sums[t][b] + re
                        sums[t][2 + b] = im if z == 0 else sums[t][2 + b] + im
            for t in range(step):
                for o in range(4):
                    proj[o, pl.ds(g * step + t, 1), :] = jnp.sum(
                        sums[t][o], axis=0, keepdims=True
                    )
            return c

        with jax.named_scope("project"):
            lax.fori_loop(0, count // step, body, 0)

    def projections(o, count):
        ph, pl_ = split(proj[o, 0:count, :])
        one = jnp.ones((8, 128), bf16)
        return dot_nt(
            jnp.concatenate([one, one], axis=1), jnp.concatenate([ph, pl_], axis=1)
        )[0:1, :]

    def spread(matrix, values):
        count = matrix.shape[0]
        for o in range(4):
            mh, ml = split(matrix * values[o : o + 1, :])
            coef[o, 0:count, :] = dot(jnp.concatenate([mh, ml], axis=1), ones)

    def apply(load, count, base):
        rows = 24
        for z in range(GRID // rows):

            def body(g, acc):
                for t in range(4):
                    j = g * 4 + t
                    p0, p1 = load(j, z * rows, rows)
                    out = []
                    for b in range(2):
                        cr = coef[b, pl.ds(j, 1), :]
                        ci = coef[2 + b, pl.ds(j, 1), :]
                        out.append(acc[2 * b] + (p0 * cr - p1 * ci))
                        out.append(acc[2 * b + 1] + (p0 * ci + p1 * cr))
                    acc = out
                return tuple(acc)

            init = tuple(
                base[192 * c + 96 * b + z * rows : 192 * c + 96 * b + z * rows + rows, :]
                for b in range(2)
                for c in range(2)
            )
            with jax.named_scope("apply"):
                done = lax.fori_loop(0, count // 4, body, init)
            for b in range(2):
                for c in range(2):
                    at = 192 * c + 96 * b + z * rows
                    image[at : at + rows, :] = done[2 * b + c]

    def beta_rows(j, at=0, rows=GRID):
        return beta[0, j, at : at + rows, :], beta[1, j, at : at + rows, :]

    def psi_rows(m, at=0, rows=GRID):
        owner, b = m // 2, m % 2
        return (
            occupied[owner, 0, b, at : at + rows, :].astype(f32),
            occupied[owner, 1, b, at : at + rows, :].astype(f32),
        )

    fill_planes(0, psi_field)
    to_sticks(1, dv, psi_field)

    def psi_in(k, c):
        psi_copy(k, 0).wait_recv()
        return c

    arrived(1)
    vec[1] = z_forward(1)
    lax.fori_loop(1, nb, psi_in, 0)

    project(psi_rows, 16, vec.at[1])
    small_send[0] = jnp.zeros((8, 128), f32)
    for o in range(4):
        small_send[0, o : o + 1, 0:16] = projections(o, 16)
    small_exchange(0)
    with jax.named_scope("unpack"):
        loads["vloc"].wait()
        unpack(vloc_flat, vloc)
    found = small_total(0) * (1.0 / (2.0 * GRID * 2048))
    eye = (row[0:16] == lane[0:16]).astype(f32)
    spread(eye, found)
    vec[1] = -vec[1]
    apply(psi_rows, 16, vec.at[1])
    vec[0] = image[...]

    def transform_out(rnd, source):
        send[rnd] = left(zh[...], zl[...], source[...]).reshape(GROUPS, ROWS, 128)
        exchange(rnd)

    def stick_sum(a, b, weight=None):
        out = []
        for n in range(2):
            s0 = slice(96 * n, 96 * n + 96)
            s1 = slice(192 + 96 * n, 288 + 96 * n)
            both = a[s0, :] * b[s0, :] + a[s1, :] * b[s1, :]
            if weight is not None:
                both = both * (kin[...] + shift[n])
            out.append(row_sum(both))
        return out

    def grid_sum(a, b):
        out = []
        for n in range(2):
            total = jnp.zeros((1, 128), f32)
            for p in range(PLANES):
                lanes = slice(128 * (2 * p + n), 128 * (2 * p + n) + 128)
                pot = vloc[:, 128 * p : 128 * p + 128]
                both = a[0:96, lanes] * b[0:96, lanes] + a[96:192, lanes] * b[96:192, lanes]
                total = total + row_sum(both * pot)
            out.append(total)
        return out

    half = lax.broadcasted_iota(jnp.int32, (1, 128), 1) < 64

    def packed(pair):
        a, b = (r + pltpu.roll(r, 64, 1) for r in pair)
        return jnp.where(half, a, b)

    def unpacked(both):
        return [
            lane_total(jnp.where(half, both, 0.0)),
            lane_total(jnp.where(half, 0.0, both)),
        ]

    def band_dots(values, coupled):
        both = values * coupled
        return [lane_total(both[b : b + 1] + both[2 + b : 3 + b]) for b in range(2)]

    ch, cl = split(couple[...])

    def coupled_rows(values):
        vh, vl = split(values)
        return dot_nt(
            jnp.concatenate([vh, vl, vh], axis=1), jnp.concatenate([ch, ch, cl], axis=1)
        )

    direction = vec.at[0]
    transform_out(2, direction)
    loads["beta"].wait()
    project(beta_rows, 128, direction)
    small_send[1] = jnp.zeros((8, 128), f32)
    for o in range(4):
        small_send[1, o : o + 1, :] = projections(o, 128)
    small_send[1, 4:5, :] = packed(stick_sum(direction, direction))
    small_exchange(1)
    curves = stick_sum(direction, direction, True)
    fill_planes(2, field0)
    local = grid_sum(field0, field0)
    small_send[3] = jnp.zeros((8, 128), f32)
    small_send[3, 0:1, :] = packed([curves[b] + local[b] for b in range(2)])
    small_exchange(3)
    to_sticks(3, vloc, field0)
    sums = small_total(1)
    values0 = sums[0:4]
    coupled0 = coupled_rows(sums)[0:4]
    nonlocal0 = band_dots(values0, coupled0)
    norm0 = unpacked(sums[4:5])
    spread(couple[...], values0)
    for c in range(2):
        for b in range(2):
            at = slice(192 * c + 96 * b, 192 * c + 96 * b + 96)
            vec[1, at, :] = direction[at, :] * (kin[...] + shift[b])
    apply(beta_rows, 128, vec.at[1])
    curve0 = [c + n for c, n in zip(unpacked(small_total(3)[0:1]), nonlocal0)]
    alpha0 = [norm0[b] / curve0[b] for b in range(2)]
    arrived(3)
    image[...] += z_forward(3)
    residual = vec.at[1]
    for c in range(2):
        for b in range(2):
            at = slice(192 * c + 96 * b, 192 * c + 96 * b + 96)
            residual[at, :] = direction[at, :] - alpha0[b] * image[at, :]

    transform_out(4, residual)
    project(beta_rows, 128, residual)
    small_send[2] = jnp.zeros((8, 128), f32)
    for o in range(4):
        small_send[2, o : o + 1, :] = projections(o, 128)
    small_send[2, 4:5, :] = packed(stick_sum(residual, residual))
    small_exchange(2)
    selfs = stick_sum(residual, residual, True)
    crosses = stick_sum(residual, direction, True)
    fill_planes(4, field1)
    self_local = grid_sum(field1, field1)
    cross_local = grid_sum(field1, field0)
    small_send[4] = jnp.zeros((8, 128), f32)
    small_send[4, 0:1, :] = packed([selfs[b] + self_local[b] for b in range(2)])
    small_send[4, 1:2, :] = packed([crosses[b] + cross_local[b] for b in range(2)])
    small_exchange(4)
    with jax.named_scope("products"):
        for p in range(PLANES):
            for b in range(2):
                lanes = slice(128 * (2 * p + b), 128 * (2 * p + b) + 128)
                for n, field in enumerate((field0, field1)):
                    dens[96 * n : 96 * n + 96, lanes] = 4.0 * (
                        psi_field[0:96, lanes] * field[0:96, lanes]
                        + psi_field[96:192, lanes] * field[96:192, lanes]
                    )
    sums = small_total(2)
    values1 = sums[0:4]
    coupled1 = coupled_rows(sums)[0:4]
    self_dots = band_dots(values1, coupled1)
    cross_dots = band_dots(values1, coupled0)
    weight0, weight1 = [], []
    norm1 = unpacked(sums[4:5])
    sums = small_total(4)
    self1, cross1 = (unpacked(sums[n : n + 1]) for n in range(2))
    for b in range(2):
        ratio = norm1[b] / norm0[b]
        self_curve = self1[b] + self_dots[b]
        cross_curve = cross1[b] + cross_dots[b]
        curve = self_curve + ratio * (2.0 * cross_curve + ratio * curve0[b])
        alpha = norm1[b] / curve
        weight0.append(alpha0[b] + alpha * ratio)
        weight1.append(alpha)

    with jax.named_scope("density"):
        for p in range(PLANES):
            total = jnp.zeros((GRID, 128), f32)
            for b in range(2):
                lanes = slice(128 * (2 * p + b), 128 * (2 * p + b) + 128)
                total = total + weight0[b] * dens[0:96, lanes] + weight1[b] * dens[96:192, lanes]
            for i in range(nb):
                part_send[i, 12 * p : 12 * p + 12, :] = total[12 * i : 12 * i + 12, :]

    def part_out(k, c):
        part_copy(k, None).start()
        return c

    lax.fori_loop(1, nb, part_out, 0)
    part_recv[mb] = part_send[mb]
    first_out[...] = direction[...]
    second_out[...] = residual[...]
    for b in range(2):
        weights_out[b : b + 1, :] = jnp.broadcast_to(weight0[b], (1, 128))
        weights_out[2 + b : 3 + b, :] = jnp.broadcast_to(weight1[b], (1, 128))
    weights_out[4:8, :] = jnp.zeros((4, 128), f32)

    def part_in(k, c):
        part_copy(k, 0).wait_recv()
        return c

    def sent(k, c):
        for rnd in range(5):
            ga_copy(rnd, k).wait_send()
        for rnd in range(5):
            small_copy(rnd, k, None).wait_send()
        return c

    lax.fori_loop(1, GROUPS, sent, 0)

    with jax.named_scope("part_wait"):
        lax.fori_loop(1, nb, part_in, 0)
    cells_out[...] = jnp.sum(part_recv[...], axis=0)

    def band_sent(k, c):
        psi_copy(k, None).wait_send()
        part_copy(k, None).wait_send()
        return c

    lax.fori_loop(1, nb, band_sent, 0)


OUTS = tuple(
    pltpu.VMEM(shape, f32) for shape in ((384, 128), (384, 128), (8, 128), (72, 128))
)


def finish(first, second, weights, cells, response, density):
    for c in range(2):
        for b in range(2):
            at = slice(192 * c + 96 * b, 192 * c + 96 * b + 96)
            response[c, b] = (
                weights[b : b + 1, :] * first[at, :] + weights[2 + b : 3 + b, :] * second[at, :]
            )
    for y in range(12):
        density[:, 96 * y : 96 * y + 96] = cells[pl.ds(y, PLANES, stride=12), :][:, 0:96]


def per_device(psi, vloc, dv, beta, dij, atom_type, stick_xy, band_shift):
    vmem = pl.BlockSpec(memory_space=pltpu.VMEM)
    smem = pl.BlockSpec(memory_space=pltpu.SMEM)
    dma = pltpu.SemaphoreType.DMA
    every = tables(2)
    early, late = every[:2], every[2:]
    pieces = pl.pallas_call(
        kernel,
        out_shape=OUTS,
        in_specs=[smem] * 3 + [pl.BlockSpec(memory_space=pl.ANY)] * 16,
        out_specs=(vmem,) * 4,
        scratch_shapes=[
            pltpu.VMEM((2, 2, GRID, 128), bf16),
            pltpu.VMEM((GROUPS, 128), jnp.int32),
            *[pltpu.VMEM(t.shape, t.dtype) for t in early],
            pltpu.VMEM((PLANES, GRID * GRID), f32),
            pltpu.VMEM((PLANES, GRID * GRID), f32),
            *[pltpu.VMEM(t.shape, t.dtype) for t in late],
            pltpu.VMEM((2, 128, GRID, 128), f32),
            pltpu.VMEM((GRID, 768), f32),
            pltpu.VMEM((GRID, 768), f32),
            pltpu.VMEM((768, 128), f32),
            pltpu.VMEM((8, 2, 2, GRID, 128), bf16),
            pltpu.VMEM((512, 2048), bf16),
            pltpu.VMEM((8, 2048), f32),
            pltpu.VMEM((5, GROUPS, ROWS, 128), f32),
            pltpu.VMEM((5, GROUPS, ROWS, 128), f32),
            pltpu.VMEM((5, 8, 128), f32),
            pltpu.VMEM((5, GROUPS, 8, 128), f32),
            pltpu.VMEM((8, 72, 128), f32),
            pltpu.VMEM((8, 72, 128), f32),
            pltpu.VMEM((384, 2048), bf16),
            pltpu.VMEM((192, 512), f32),
            pltpu.VMEM((384, 512), f32),
            pltpu.VMEM((384, 512), bf16),
            pltpu.VMEM((384, 512), bf16),
            pltpu.VMEM((128, 1536), bf16),
            pltpu.VMEM((128, 1536), bf16),
            pltpu.VMEM((192, 1536), f32),
            pltpu.VMEM((192, 1536), f32),
            pltpu.VMEM((192, 1536), f32),
            pltpu.VMEM((384, 512), bf16),
            pltpu.VMEM((4, 128, 128), f32),
            pltpu.VMEM((4, 128, 128), f32),
            pltpu.VMEM((128, 128), f32),
            pltpu.VMEM((2, 384, 128), f32),
            pltpu.VMEM((384, 128), f32),
            pltpu.VMEM((GRID, 128), f32),
            pltpu.VMEM((8, 2048), f32),
            pltpu.VMEM((192, 1536), f32),
            dma((16,)),
            dma((8,)),
            dma((8,)),
            dma((5, GROUPS)),
            dma((5, GROUPS)),
            dma((5, GROUPS)),
            dma((5, GROUPS)),
            dma((8,)),
            dma((8,)),
        ],
        compiler_params=pltpu.CompilerParams(
            collective_id=0, has_side_effects=True, vmem_limit_bytes=60 * 1024 * 1024
        ),
    )(
        band_shift, dij, atom_type, psi, stick_xy.reshape(GROUPS, 128), *early,
        vloc, dv, *late, beta,
    )
    return pl.pallas_call(
        finish,
        out_shape=(
            jax.ShapeDtypeStruct((2, 2, GRID, 128), f32),
            jax.ShapeDtypeStruct((PLANES, 12 * GRID), f32),
        ),
        in_specs=[vmem] * 4,
        out_specs=(vmem, vmem),
    )(*(pltpu.with_memory_space_constraint(p, pltpu.VMEM) for p in pieces))


def solution(mesh):
    return jax.shard_map(
        per_device,
        mesh=mesh,
        in_specs=(
            P(None, "band", None, "ga"),
            P("ga", None),
            P("ga", None),
            P(None, None, None, "ga"),
            P(),
            P(),
            P(),
            P("band"),
        ),
        out_specs=(P(None, "band", None, "ga"), P("ga", "band")),
        check_vma=False,
    )
```

```python
import functools
import math

import jax
import jax.numpy as jnp
import numpy as np
from jax import lax
from jax.experimental import pallas as pl
from jax.experimental.pallas import tpu as pltpu
from jax.sharding import PartitionSpec as P

GRID = 96
SIDE = 64
GROUPS = 16
PLANES = 6
ROWS = 24
MESH = pl.DeviceIdType.MESH
f32 = jnp.float32
bf16 = jnp.bfloat16


def complex_table(angle):
    cos, sin = np.cos(angle), np.sin(angle)
    return np.array([[cos, -sin], [sin, cos]]) / math.sqrt(GRID)


def halves(table):
    high = np.asarray(table, np.float32).astype(jnp.bfloat16)
    low = (table - high.astype(np.float64)).astype(jnp.bfloat16)
    return high, low


def tables():
    unit = 2.0 * math.pi / GRID
    cells = np.arange(GRID)
    freqs = np.arange(SIDE) - SIDE // 2
    along_z = complex_table(unit * (cells[:, None] * cells[None, :] % GRID))
    along_z = along_z.reshape(2, 2, GROUPS, PLANES, GRID)
    z_table = np.einsum("oidpk->dopik", along_z).reshape(GROUPS, 12, 2 * GRID)
    z_table = np.concatenate(
        [z_table[:, :8].reshape(128, -1), z_table[:, 8:].reshape(64, -1)], axis=0
    )
    along_x = np.zeros((2, 2, SIDE, 128))
    along_x[..., :GRID] = complex_table(unit * (freqs[:, None] * cells[None, :] % GRID))
    x_table = np.einsum("oikx,be->ibkoex", along_x, np.eye(2)).reshape(256, 512)
    along_y = complex_table(unit * (cells[:, None] * freqs[None, :] % GRID))
    along_y = along_y.reshape(2, 2, GRID, 8, 8)
    y_table = np.einsum("oiygl->oyilg", along_y).reshape(192, 128)
    out = []
    for table in (z_table, z_table.T):
        high, low = halves(np.ascontiguousarray(table))
        out.append(np.concatenate([high, low, high], axis=1))
    for table in (x_table, x_table.T, y_table):
        out.extend(halves(np.ascontiguousarray(table)))
    high, low = halves(np.ascontiguousarray(y_table.T))
    out.append(np.concatenate([high, high, low], axis=1))
    return [jnp.asarray(t) for t in out]


def dot(a, b):
    return lax.dot_general(a, b, (((1,), (0,)), ((), ())), preferred_element_type=f32)


def dot_nt(a, b):
    return lax.dot_general(a, b, (((1,), (1,)), ((), ())), preferred_element_type=f32)


def split(x):
    high = x.astype(bf16)
    return high, (x - high.astype(f32)).astype(bf16)


def deep(table, x):
    xh, xl = split(x)
    return dot(table, jnp.concatenate([xh, xh, xl], axis=0))


def right(ah, al, high, low):
    return dot(
        jnp.concatenate([ah, al, ah], axis=1), jnp.concatenate([high, high, low], axis=0)
    )


def row_sum(x):
    return jnp.sum(jnp.sum(x.reshape(-1, 8, 128), axis=0), axis=0, keepdims=True)


def lane_total(row):
    return jnp.sum(row, axis=1, keepdims=True)


def kernel(
    shift, dij, kind, psi_hbm, sticks_hbm, z3_hbm, vloc_hbm, dv_hbm, zt3_hbm, xh_hbm, xl_hbm, xth_hbm, xtl_hbm,
    yh_hbm, yl_hbm, yt3_hbm, beta_hbm,
    first_out, second_out, weights_out, cells_out,
    psi, sticks, z3, vloc_flat, dv_flat, zt3, xh, xl, xth, xtl, yh, yl, yt3,
    beta, vloc, dv, cells, occupied, onehot, mask, send, recv, small_send, small_recv,
    part_send, part_recv, lhs, grid, ex, eh, el, dh, dl, psi_field, field0, field1,
    q, proj, coef, couple, vec, image, kin, own, dens,
    load_sem, psi_sem, ssem, rsem, rall, tssem, trsem, part_sem,
):
    me = lax.axis_index("ga")
    mb = lax.axis_index("band")
    nb = 8

    barrier = pltpu.get_barrier_semaphore()

    def greet_ga(k, c):
        pl.semaphore_signal(
            barrier, inc=1, device_id=(lax.rem(me + k, GROUPS), mb), device_id_type=MESH
        )
        return c

    def greet_band(k, c):
        pl.semaphore_signal(
            barrier, inc=1, device_id=(me, lax.rem(mb + k, nb)), device_id_type=MESH
        )
        return c

    lax.fori_loop(1, GROUPS, greet_ga, 0)
    lax.fori_loop(1, nb, greet_band, 0)
    loads = {}
    pairs = dict(
        psi=(psi_hbm, psi), z3=(z3_hbm, z3), sticks=(sticks_hbm, sticks),
        dv=(dv_hbm, dv_flat), xh=(xh_hbm, xh), xl=(xl_hbm, xl), yh=(yh_hbm, yh),
        yl=(yl_hbm, yl), yt3=(yt3_hbm, yt3), xth=(xth_hbm, xth), xtl=(xtl_hbm, xtl),
        zt3=(zt3_hbm, zt3), vloc=(vloc_hbm, vloc_flat),
        beta=(beta_hbm, beta),
    )
    for at, (name, (source, target)) in enumerate(pairs.items()):
        loads[name] = pltpu.make_async_copy(source, target, load_sem.at[at])
        loads[name].start()

    def came(rnd, owner):
        return rsem.at[rnd // 2, owner] if rnd % 2 == 0 else rall.at[rnd // 2]

    def copy(source, target, gone, landed, where):
        return pltpu.make_async_remote_copy(
            src_ref=source, dst_ref=target, send_sem=gone, recv_sem=landed,
            device_id=where, device_id_type=MESH,
        )

    def ga_copy(rnd, k):
        other = lax.rem(me + k, GROUPS)
        return copy(
            send.at[rnd, other], recv.at[rnd, me], ssem.at[rnd], came(rnd, me), (other, mb)
        )

    def ga_landed(rnd, k):
        other = lax.rem(me + k, GROUPS)
        return copy(
            send.at[rnd, other], recv.at[rnd, other], ssem.at[rnd], came(rnd, other), (other, mb)
        )

    others = pl.ds(0, GROUPS - 1)
    right_of = (lax.rem(me + 1, GROUPS), mb)

    def ga_all(rnd):
        return copy(
            send.at[rnd, others], recv.at[rnd, others], ssem.at[rnd], came(rnd, 0), right_of
        )

    def exchange(rnd):
        def body(k, c):
            ga_copy(rnd, k).start()
            return c

        lax.fori_loop(1, GROUPS, body, 0)
        recv[rnd, me] = send[rnd, me]

    @jax.named_scope("arrived")
    def arrived(rnd):
        ga_all(rnd).wait_recv()

    def small_exchange(rnd):
        def body(k, c):
            copy(
                small_send.at[rnd], small_recv.at[rnd, me], tssem.at[rnd], trsem.at[rnd],
                (lax.rem(me + k, GROUPS), mb),
            ).start()
            return c

        lax.fori_loop(1, GROUPS, body, 0)
        small_recv[rnd, me] = small_send[rnd]

    def small_all(rnd):
        landed = small_recv.at[rnd, others]
        return copy(landed, landed, tssem.at[rnd], trsem.at[rnd], right_of)

    def small_total(rnd):
        with jax.named_scope("small_wait"):
            small_all(rnd).wait_recv()
        return jnp.sum(small_recv[rnd], axis=0)

    def psi_copy(k):
        where = (me, lax.rem(mb + k, nb))
        return copy(psi, occupied.at[mb], psi_sem.at[0], psi_sem.at[1], where)

    rest = pl.ds(0, nb - 1)
    after = (me, lax.rem(mb + 1, nb))

    def psi_all():
        return copy(occupied.at[rest], occupied.at[rest], psi_sem.at[0], psi_sem.at[1], after)

    def part_copy(k):
        other = lax.rem(mb + k, nb)
        return copy(
            part_send.at[other], part_recv.at[mb], part_sem.at[0], part_sem.at[1], (me, other)
        )

    def part_all():
        return copy(part_send.at[rest], part_recv.at[rest], part_sem.at[0], part_sem.at[1], after)

    def dealt(rnd, planes):
        for d in range(GROUPS):
            head = planes[8 * d : 8 * d + 8]
            tail = planes[128 + 4 * d : 132 + 4 * d]
            send[rnd, d, 0:8] = head[:, 0:128]
            send[rnd, d, 8:16] = jnp.concatenate([tail[:, 0:128], tail[:, 128:256]], axis=0)
            send[rnd, d, 16:24] = head[:, 128:256]

    def collected(rnd):
        rows = [
            jnp.concatenate([recv[rnd, d, 0:8], recv[rnd, d, 16:24]], axis=1)
            for d in range(GROUPS)
        ]
        for d in range(0, GROUPS, 2):
            even, odd = recv[rnd, d, 8:16], recv[rnd, d + 1, 8:16]
            rows.append(
                jnp.concatenate(
                    [
                        jnp.concatenate([even[0:4], odd[0:4]], axis=0),
                        jnp.concatenate([even[4:8], odd[4:8]], axis=0),
                    ],
                    axis=1,
                )
            )
        return jnp.concatenate(rows, axis=0)

    for name in ("psi", "z3"):
        loads[name].wait()
    with jax.named_scope("z_psi"):
        wide = jnp.concatenate(
            [jnp.concatenate([psi[c, 0], psi[c, 1]], axis=1) for c in range(2)], axis=0
        )
        dealt(0, dot(z3[:, 0:384], jnp.concatenate([wide, wide], axis=0)))

    def places(xy):
        flat = xy.astype(f32)
        y = jnp.floor((flat + 0.5) * (1.0 / GRID))
        x = flat - GRID * y
        fy = jnp.where(y >= GRID // 2, y - GRID, y)
        fx = jnp.where(x >= GRID // 2, x - GRID, x)
        return fy, fx

    loads["sticks"].wait()
    with jax.named_scope("tables"):
        fy, fx = places(sticks[...])
        ky = fy + SIDE // 2
        kx = fx + SIDE // 2
        high = jnp.floor(ky * 0.125)
        low = (ky - 8.0 * high) * SIDE + kx
        for k in range(GROUPS):
            own[0:1, 128 * k : 128 * k + 128] = low[k : k + 1, :]
            own[1:2, 128 * k : 128 * k + 128] = high[k : k + 1, :]
        mask[...] = (
            lax.broadcasted_iota(jnp.int32, (8, 2048), 0).astype(f32) == own[1:2, :]
        ).astype(f32)

        def fill(k, c):
            lanes = pl.ds(pl.multiple_of(k * 256, 256), 256)
            ids = lax.broadcasted_iota(jnp.int32, (512, 256), 0).astype(f32)
            onehot[:, lanes] = (ids == own[0:1, lanes]).astype(f32).astype(bf16)
            return c

        lax.fori_loop(0, 8, fill, 0)
        oy, ox = places(sticks[pl.ds(me, 1), :])
        kz = lax.broadcasted_iota(jnp.int32, (GRID, 128), 0).astype(f32)
        fz = jnp.where(kz >= GRID // 2, kz - GRID, kz)
        kin[...] = (fz * fz + (oy * oy + ox * ox)) * (4.0 / (GRID * GRID))

    row = lax.broadcasted_iota(jnp.int32, (128, 128), 0)
    lane = lax.broadcasted_iota(jnp.int32, (128, 128), 1)

    def couple_all():
        atom = lax.broadcasted_iota(jnp.int32, (1, 128), 1) // 4
        kinds = jnp.zeros((1, 128), jnp.int32)
        for a in range(32):
            kinds = jnp.where(atom == a, kind[a], kinds)
        same = (row // 4) == (lane // 4)
        first = kinds == 0
        total = jnp.zeros((128, 128), f32)
        for i in range(4):
            for k in range(4):
                value = jnp.where(first, dij[0, i, k], dij[1, i, k])
                here = same & ((row % 4) == i) & ((lane % 4) == k)
                total = total + jnp.where(here, value, 0.0)
        couple[...] = total

    def unpack(flat, out):
        def body(g, c):
            piece = flat[:, pl.ds(pl.multiple_of(g * 384, 384), 384)]
            tail = jnp.zeros((PLANES, 32), f32)
            for r in range(4):
                if r < 3:
                    cut = piece[:, 96 * r : 96 * r + 128]
                else:
                    cut = jnp.concatenate([piece[:, 288:384], tail], axis=1)
                cells[pl.ds(pl.multiple_of(g * 32, 32) + 8 * r, PLANES), :] = cut
            return c

        lax.fori_loop(0, 24, body, 0)
        for p in range(PLANES):
            out[:, 128 * p : 128 * p + 128] = cells[pl.ds(p, GRID, stride=8), :]

    with jax.named_scope("couple"):
        couple_all()
    with jax.named_scope("barrier"):
        pl.semaphore_wait(barrier, GROUPS - 1 + nb - 1)
    exchange(0)

    def psi_out(k, c):
        psi_copy(k).start()
        return c

    lax.fori_loop(1, nb, psi_out, 0)
    occupied[mb] = psi[...]

    with jax.named_scope("unpack"):
        loads["dv"].wait()
        unpack(dv_flat, dv)
    for name in ("xh", "xl", "yh", "yl", "yt3", "xth", "xtl", "zt3"):
        loads[name].wait()
    ones = jnp.ones((256, 128), bf16)

    def fill_planes(rnd, out):

        def body(k, c):
            src = lax.rem(me + k, GROUPS)

            @pl.when(k > 0)
            def _():
                ga_landed(rnd, k).wait_recv()

            piece = recv[rnd, src]
            upper = piece.astype(bf16).astype(f32)
            lower = piece - upper
            cols = pl.ds(pl.multiple_of(src * 128, 128), 128)
            keep = mask[:, cols]
            for n, part in enumerate((upper, lower)):
                for index in range(12):
                    pair = (index, index + 16 if index < 8 else index + 4)
                    two = [jnp.broadcast_to(part[r : r + 1], (8, 128)) * keep for r in pair]
                    at = 192 * n + 16 * index
                    lhs[at : at + 16, cols] = jnp.concatenate(two, axis=0).astype(bf16)
            return c

        with jax.named_scope("fill_lhs"):
            lax.fori_loop(0, GROUPS, body, 0)
        with jax.named_scope("fill_dot"):
            both = dot_nt(lhs[...], onehot[...])
            grid[...] = both[0:192] + both[192:384]
        with jax.named_scope("fill_x"):
            data = [
                jnp.concatenate(
                    [grid[0:96, 128 * t : 128 * t + 128], grid[96:192, 128 * t : 128 * t + 128]],
                    axis=1,
                )
                for t in range(4)
            ]
            ah, al = split(jnp.concatenate(data, axis=0))
            ex[...] = right(ah, al, xh[...], xl[...])
            for c in range(2):
                for t in range(4):
                    rows = slice(16 * (4 * c + t), 16 * (4 * c + t) + 16)
                    for i in range(12):
                        at = 96 * t + 8 * i
                        two = [ex[at : at + 8, 128 * (2 * c + j) : 128 * (2 * c + j) + 128] for j in (0, 1)]
                        uh, ul = split(jnp.concatenate(two, axis=0))
                        dh[rows, 128 * i : 128 * i + 128] = uh
                        dl[rows, 128 * i : 128 * i + 128] = ul
        with jax.named_scope("fill_y"):
            for part in range(6):
                lanes = slice(256 * part, 256 * part + 256)
                out[:, lanes] = dot(
                    jnp.concatenate([yh[...], yh[...], yl[...]], axis=1),
                    jnp.concatenate([dh[:, lanes], dl[:, lanes], dh[:, lanes]], axis=0),
                )

    def to_sticks(rnd, potential, source):
        with jax.named_scope("stick_y"):
            for p in range(PLANES):
                lanes = slice(256 * p, 256 * p + 256)
                pot = potential[:, 128 * p : 128 * p + 128]
                pot = jnp.concatenate([pot, pot], axis=1)
                pot = jnp.concatenate([pot, pot], axis=0)
                ah, al = split(source[:, lanes] * pot)
                along = dot(yt3[...], jnp.concatenate([ah, al, ah], axis=0))
                for c in range(2):
                    for t in range(4):
                        for j in range(2):
                            rows = slice(8 * (8 * c + 2 * t + j), 8 * (8 * c + 2 * t + j) + 8)
                            two = jnp.concatenate([along[rows, 0:128], along[rows, 128:256]], axis=0)
                            uh, ul = split(two)
                            at = 96 * t + 16 * p
                            cols = slice(128 * (2 * c + j), 128 * (2 * c + j) + 128)
                            eh[at : at + 16, cols] = uh
                            el[at : at + 16, cols] = ul
        with jax.named_scope("stick_x"):
            along = right(eh[...], el[...], xth[...], xtl[...])
            for r in range(0, ROWS, 2):
                if r < 12:
                    index, b = r, 0
                else:
                    index, b = (r - 4, 1) if r < 16 else (r - 16, 1)
                for t in range(4):
                    two = []
                    for n in (index, index + 1):
                        at = 96 * t + 8 * (2 * (n % PLANES) + b)
                        col = 128 * (n // PLANES)
                        two.append(along[at : at + 8, col : col + 128])
                    uh, ul = split(jnp.concatenate(two, axis=0))
                    lanes = slice(128 * t, 128 * t + 128)
                    q[8 * r : 8 * r + 16, lanes] = uh
                    q[192 + 8 * r : 208 + 8 * r, lanes] = ul

        with jax.named_scope("stick_pick"):
            for k in range(5):
                if k < 4:
                    quad = lax.rem(me // 4 + k, 4)
                    lanes = pl.ds(pl.multiple_of(quad * 512, 512), 512)
                    both = dot(q[...], onehot[:, lanes])
                    found = both[0:192] + both[192:384]
                    picked = jnp.sum(found.reshape(ROWS, 8, 512) * mask[:, lanes][None], axis=1)
                    for n in range(4):
                        send[rnd, 4 * quad + n] = picked[:, 128 * n : 128 * n + 128]
                if k > 0:
                    post(rnd, lax.rem(me // 4 + k + 3, 4))
            recv[rnd, me] = send[rnd, me]

    def post(rnd, quad):
        for n in range(4):
            owner = 4 * quad + n

            @pl.when(owner != me)
            def _():
                ga_copy(rnd, owner - me + GROUPS).start()

    def z_forward(rnd):
        return deep(zt3[...], collected(rnd))

    def project(load, count, source):
        step = 4

        def body(g, c):
            sums = [[None] * 4 for _ in range(step)]
            for z in range(GRID // 8):
                v = [
                    source[96 * c + 8 * z : 96 * c + 8 * z + 8, 128 * b : 128 * b + 128]
                    for c in range(2)
                    for b in range(2)
                ]
                for t in range(step):
                    p0, p1 = load(g * step + t, 8 * z, 8)
                    for b in range(2):
                        re = p0 * v[b] + p1 * v[2 + b]
                        im = p0 * v[2 + b] - p1 * v[b]
                        sums[t][b] = re if z == 0 else sums[t][b] + re
                        sums[t][2 + b] = im if z == 0 else sums[t][2 + b] + im
            for t in range(step):
                for o in range(4):
                    proj[o, pl.ds(g * step + t, 1), :] = jnp.sum(
                        sums[t][o], axis=0, keepdims=True
                    )
            return c

        with jax.named_scope("project"):
            lax.fori_loop(0, count // step, body, 0)

    def projections(o, count):
        ph, pl_ = split(proj[o, 0:count, :])
        one = jnp.ones((8, 128), bf16)
        return dot_nt(
            jnp.concatenate([one, one], axis=1), jnp.concatenate([ph, pl_], axis=1)
        )[0:1, :]

    def spread(matrix, values):
        count = matrix.shape[0]
        for o in range(4):
            mh, ml = split(matrix * values[o : o + 1, :])
            coef[o, 0:count, :] = dot(jnp.concatenate([mh, ml], axis=1), ones)

    def apply(load, count, base):
        rows = 24
        for z in range(GRID // rows):

            def body(g, acc):
                for t in range(4):
                    j = g * 4 + t
                    p0, p1 = load(j, z * rows, rows)
                    out = []
                    for b in range(2):
                        cr = coef[b, pl.ds(j, 1), :]
                        ci = coef[2 + b, pl.ds(j, 1), :]
                        out.append(acc[2 * b] + (p0 * cr - p1 * ci))
                        out.append(acc[2 * b + 1] + (p0 * ci + p1 * cr))
                    acc = out
                return tuple(acc)

            init = tuple(
                base[96 * c + z * rows : 96 * c + z * rows + rows, 128 * b : 128 * b + 128]
                for b in range(2)
                for c in range(2)
            )
            with jax.named_scope("apply"):
                done = lax.fori_loop(0, count // 4, body, init)
            for b in range(2):
                for c in range(2):
                    at = 96 * c + z * rows
                    image[at : at + rows, 128 * b : 128 * b + 128] = done[2 * b + c]

    def beta_rows(j, at=0, rows=GRID):
        return beta[0, j, at : at + rows, :], beta[1, j, at : at + rows, :]

    def psi_rows(m, at=0, rows=GRID):
        owner, b = m // 2, m % 2
        return (
            occupied[owner, 0, b, at : at + rows, :].astype(f32),
            occupied[owner, 1, b, at : at + rows, :].astype(f32),
        )

    fill_planes(0, psi_field)
    to_sticks(1, dv, psi_field)

    arrived(1)
    vec[1] = z_forward(1)
    psi_all().wait_recv()

    project(psi_rows, 16, vec.at[1])
    small_send[0] = jnp.zeros((8, 128), f32)
    for o in range(4):
        small_send[0, o : o + 1, 0:16] = projections(o, 16)
    small_exchange(0)
    with jax.named_scope("unpack"):
        loads["vloc"].wait()
        unpack(vloc_flat, vloc)
    found = small_total(0) * (1.0 / (2.0 * GRID * 2048))
    eye = (row[0:16] == lane[0:16]).astype(f32)
    spread(eye, found)
    vec[1] = -vec[1]
    apply(psi_rows, 16, vec.at[1])
    vec[0] = image[...]

    def transform_out(rnd, source):
        dealt(rnd, deep(z3[...], source[...]))
        exchange(rnd)

    def stick_sum(a, b, weight=None):
        out = []
        for n in range(2):
            at = slice(128 * n, 128 * n + 128)
            both = a[0:96, at] * b[0:96, at] + a[96:192, at] * b[96:192, at]
            if weight is not None:
                both = both * (kin[...] + shift[n])
            out.append(row_sum(both))
        return out

    def grid_sum(a, b):
        out = []
        for n in range(2):
            total = jnp.zeros((1, 128), f32)
            for p in range(PLANES):
                lanes = slice(128 * (2 * p + n), 128 * (2 * p + n) + 128)
                pot = vloc[:, 128 * p : 128 * p + 128]
                both = a[0:96, lanes] * b[0:96, lanes] + a[96:192, lanes] * b[96:192, lanes]
                total = total + row_sum(both * pot)
            out.append(total)
        return out

    half = lax.broadcasted_iota(jnp.int32, (1, 128), 1) < 64

    def packed(pair):
        a, b = (r + pltpu.roll(r, 64, 1) for r in pair)
        return jnp.where(half, a, b)

    def unpacked(both):
        return [
            lane_total(jnp.where(half, both, 0.0)),
            lane_total(jnp.where(half, 0.0, both)),
        ]

    def band_dots(values, coupled):
        both = values * coupled
        return [lane_total(both[b : b + 1] + both[2 + b : 3 + b]) for b in range(2)]

    ch, cl = split(couple[...])

    def coupled_rows(values):
        vh, vl = split(values)
        return dot_nt(
            jnp.concatenate([vh, vl, vh], axis=1), jnp.concatenate([ch, ch, cl], axis=1)
        )

    direction = vec.at[0]
    transform_out(2, direction)
    loads["beta"].wait()
    project(beta_rows, 128, direction)
    small_send[1] = jnp.zeros((8, 128), f32)
    for o in range(4):
        small_send[1, o : o + 1, :] = projections(o, 128)
    small_send[1, 4:5, :] = packed(stick_sum(direction, direction))
    small_exchange(1)
    curves = stick_sum(direction, direction, True)
    fill_planes(2, field0)
    local = grid_sum(field0, field0)
    small_send[3] = jnp.zeros((8, 128), f32)
    small_send[3, 0:1, :] = packed([curves[b] + local[b] for b in range(2)])
    small_exchange(3)
    to_sticks(3, vloc, field0)
    sums = small_total(1)
    values0 = sums[0:4]
    coupled0 = coupled_rows(sums)[0:4]
    nonlocal0 = band_dots(values0, coupled0)
    norm0 = unpacked(sums[4:5])
    spread(couple[...], values0)
    for c in range(2):
        for b in range(2):
            at, of = slice(96 * c, 96 * c + 96), slice(128 * b, 128 * b + 128)
            vec[1, at, of] = direction[at, of] * (kin[...] + shift[b])
    apply(beta_rows, 128, vec.at[1])
    curve0 = [c + n for c, n in zip(unpacked(small_total(3)[0:1]), nonlocal0)]
    alpha0 = [norm0[b] / curve0[b] for b in range(2)]
    arrived(3)
    image[...] += z_forward(3)
    residual = vec.at[1]
    for c in range(2):
        for b in range(2):
            at, of = slice(96 * c, 96 * c + 96), slice(128 * b, 128 * b + 128)
            residual[at, of] = direction[at, of] - alpha0[b] * image[at, of]

    transform_out(4, residual)
    project(beta_rows, 128, residual)
    small_send[2] = jnp.zeros((8, 128), f32)
    for o in range(4):
        small_send[2, o : o + 1, :] = projections(o, 128)
    small_send[2, 4:5, :] = packed(stick_sum(residual, residual))
    small_exchange(2)
    selfs = stick_sum(residual, residual, True)
    crosses = stick_sum(residual, direction, True)
    fill_planes(4, field1)
    self_local = grid_sum(field1, field1)
    cross_local = grid_sum(field1, field0)
    small_send[4] = jnp.zeros((8, 128), f32)
    small_send[4, 0:1, :] = packed([selfs[b] + self_local[b] for b in range(2)])
    small_send[4, 1:2, :] = packed([crosses[b] + cross_local[b] for b in range(2)])
    small_exchange(4)
    with jax.named_scope("products"):
        for p in range(PLANES):
            for b in range(2):
                lanes = slice(128 * (2 * p + b), 128 * (2 * p + b) + 128)
                for n, field in enumerate((field0, field1)):
                    dens[96 * n : 96 * n + 96, lanes] = 4.0 * (
                        psi_field[0:96, lanes] * field[0:96, lanes]
                        + psi_field[96:192, lanes] * field[96:192, lanes]
                    )
    sums = small_total(2)
    values1 = sums[0:4]
    coupled1 = coupled_rows(sums)[0:4]
    self_dots = band_dots(values1, coupled1)
    cross_dots = band_dots(values1, coupled0)
    weight0, weight1 = [], []
    norm1 = unpacked(sums[4:5])
    sums = small_total(4)
    self1, cross1 = (unpacked(sums[n : n + 1]) for n in range(2))
    for b in range(2):
        ratio = norm1[b] / norm0[b]
        self_curve = self1[b] + self_dots[b]
        cross_curve = cross1[b] + cross_dots[b]
        curve = self_curve + ratio * (2.0 * cross_curve + ratio * curve0[b])
        alpha = norm1[b] / curve
        weight0.append(alpha0[b] + alpha * ratio)
        weight1.append(alpha)

    with jax.named_scope("density"):
        for p in range(PLANES):
            total = jnp.zeros((GRID, 128), f32)
            for b in range(2):
                lanes = slice(128 * (2 * p + b), 128 * (2 * p + b) + 128)
                total = total + weight0[b] * dens[0:96, lanes] + weight1[b] * dens[96:192, lanes]
            for i in range(nb):
                part_send[i, 12 * p : 12 * p + 12, :] = total[12 * i : 12 * i + 12, :]

    def part_out(k, c):
        part_copy(k).start()
        return c

    lax.fori_loop(1, nb, part_out, 0)
    part_recv[mb] = part_send[mb]
    first_out[...] = direction[...]
    second_out[...] = residual[...]
    for b in range(2):
        weights_out[b : b + 1, :] = jnp.broadcast_to(weight0[b], (1, 128))
        weights_out[2 + b : 3 + b, :] = jnp.broadcast_to(weight1[b], (1, 128))
    weights_out[4:8, :] = jnp.zeros((4, 128), f32)

    for rnd in range(5):
        ga_all(rnd).wait_send()
        small_all(rnd).wait_send()
    psi_all().wait_send()
    with jax.named_scope("part_wait"):
        part_all().wait_recv()
    cells_out[...] = jnp.sum(part_recv[...], axis=0)

    part_all().wait_send()


OUTS = tuple(
    pltpu.VMEM(shape, f32) for shape in ((192, 256), (192, 256), (8, 128), (72, 128))
)


def finish(first, second, weights, cells, response, density):
    for c in range(2):
        for b in range(2):
            at, of = slice(96 * c, 96 * c + 96), slice(128 * b, 128 * b + 128)
            response[c, b] = (
                weights[b : b + 1, :] * first[at, of] + weights[2 + b : 3 + b, :] * second[at, of]
            )
    for y in range(12):
        density[:, 96 * y : 96 * y + 96] = cells[pl.ds(y, PLANES, stride=12), :][:, 0:96]


def per_device(psi, vloc, dv, beta, dij, atom_type, stick_xy, band_shift):
    vmem = pl.BlockSpec(memory_space=pltpu.VMEM)
    smem = pl.BlockSpec(memory_space=pltpu.SMEM)
    dma = pltpu.SemaphoreType.DMA
    every = tables()
    early, late = every[:1], every[1:]
    pieces = pl.pallas_call(
        kernel,
        out_shape=OUTS,
        in_specs=[smem] * 3 + [pl.BlockSpec(memory_space=pl.ANY)] * 14,
        out_specs=(vmem,) * 4,
        scratch_shapes=[
            pltpu.VMEM((2, 2, GRID, 128), bf16),
            pltpu.VMEM((GROUPS, 128), jnp.int32),
            *[pltpu.VMEM(t.shape, t.dtype) for t in early],
            pltpu.VMEM((PLANES, GRID * GRID), f32),
            pltpu.VMEM((PLANES, GRID * GRID), f32),
            *[pltpu.VMEM(t.shape, t.dtype) for t in late],
            pltpu.VMEM((2, 128, GRID, 128), f32),
            pltpu.VMEM((GRID, 768), f32),
            pltpu.VMEM((GRID, 768), f32),
            pltpu.VMEM((768, 128), f32),
            pltpu.VMEM((8, 2, 2, GRID, 128), bf16),
            pltpu.VMEM((512, 2048), bf16),
            pltpu.VMEM((8, 2048), f32),
            pltpu.VMEM((5, GROUPS, ROWS, 128), f32),
            pltpu.VMEM((5, GROUPS, ROWS, 128), f32),
            pltpu.VMEM((5, 8, 128), f32),
            pltpu.VMEM((5, GROUPS, 8, 128), f32),
            pltpu.VMEM((8, 72, 128), f32),
            pltpu.VMEM((8, 72, 128), f32),
            pltpu.VMEM((384, 2048), bf16),
            pltpu.VMEM((192, 512), f32),
            pltpu.VMEM((384, 512), f32),
            pltpu.VMEM((384, 512), bf16),
            pltpu.VMEM((384, 512), bf16),
            pltpu.VMEM((128, 1536), bf16),
            pltpu.VMEM((128, 1536), bf16),
            pltpu.VMEM((192, 1536), f32),
            pltpu.VMEM((192, 1536), f32),
            pltpu.VMEM((192, 1536), f32),
            pltpu.VMEM((384, 512), bf16),
            pltpu.VMEM((4, 128, 128), f32),
            pltpu.VMEM((4, 128, 128), f32),
            pltpu.VMEM((128, 128), f32),
            pltpu.VMEM((2, 192, 256), f32),
            pltpu.VMEM((192, 256), f32),
            pltpu.VMEM((GRID, 128), f32),
            pltpu.VMEM((8, 2048), f32),
            pltpu.VMEM((192, 1536), f32),
            dma((16,)),
            dma((2,)),
            dma((5,)),
            dma((3, GROUPS)),
            dma((2,)),
            dma((5,)),
            dma((5,)),
            dma((2,)),
        ],
        compiler_params=pltpu.CompilerParams(
            collective_id=0, has_side_effects=True, vmem_limit_bytes=60 * 1024 * 1024
        ),
    )(
        band_shift, dij, atom_type, psi, stick_xy.reshape(GROUPS, 128), *early,
        vloc, dv, *late, beta,
    )
    return pl.pallas_call(
        finish,
        out_shape=(
            jax.ShapeDtypeStruct((2, 2, GRID, 128), f32),
            jax.ShapeDtypeStruct((PLANES, 12 * GRID), f32),
        ),
        in_specs=[vmem] * 4,
        out_specs=(vmem, vmem),
    )(*(pltpu.with_memory_space_constraint(p, pltpu.VMEM) for p in pieces))


def solution(mesh):
    return jax.shard_map(
        per_device,
        mesh=mesh,
        in_specs=(
            P(None, "band", None, "ga"),
            P("ga", None),
            P("ga", None),
            P(None, None, None, "ga"),
            P(),
            P(),
            P(),
            P("band"),
        ),
        out_specs=(P(None, "band", None, "ga"), P("ga", "band")),
        check_vma=False,
    )
```

```python
import functools
import math

import jax
import jax.numpy as jnp
import numpy as np
from jax import lax
from jax.experimental import pallas as pl
from jax.experimental.pallas import tpu as pltpu
from jax.sharding import PartitionSpec as P

GRID = 96
SIDE = 64
GROUPS = 16
PLANES = 6
ROWS = 24
MESH = pl.DeviceIdType.MESH
f32 = jnp.float32
bf16 = jnp.bfloat16


def complex_table(angle):
    cos, sin = np.cos(angle), np.sin(angle)
    return np.array([[cos, -sin], [sin, cos]]) / math.sqrt(GRID)


def halves(table):
    high = np.asarray(table, np.float32).astype(jnp.bfloat16)
    low = (table - high.astype(np.float64)).astype(jnp.bfloat16)
    return high, low


def tables():
    unit = 2.0 * math.pi / GRID
    cells = np.arange(GRID)
    freqs = np.arange(SIDE) - SIDE // 2
    along_z = complex_table(unit * (cells[:, None] * cells[None, :] % GRID))
    along_z = along_z.reshape(2, 2, GROUPS, PLANES, GRID)
    z_table = np.einsum("oidpk->dopik", along_z).reshape(GROUPS, 12, 2 * GRID)
    z_table = np.concatenate(
        [z_table[:, :8].reshape(128, -1), z_table[:, 8:].reshape(64, -1)], axis=0
    )
    along_x = np.zeros((2, 2, SIDE, 128))
    along_x[..., :GRID] = complex_table(unit * (freqs[:, None] * cells[None, :] % GRID))
    x_table = np.einsum("oikx,be->ibkoex", along_x, np.eye(2)).reshape(256, 512)
    along_y = complex_table(unit * (cells[:, None] * freqs[None, :] % GRID))
    along_y = along_y.reshape(2, 2, GRID, 8, 8)
    y_table = np.einsum("oiygl->oyilg", along_y).reshape(192, 128)
    out = []
    for table in (z_table, z_table.T):
        high, low = halves(np.ascontiguousarray(table))
        out.append(np.concatenate([high, low, high], axis=1))
    for table in (x_table, x_table.T, y_table):
        out.extend(halves(np.ascontiguousarray(table)))
    high, low = halves(np.ascontiguousarray(y_table.T))
    out.append(np.concatenate([high, high, low], axis=1))
    return [jnp.asarray(t) for t in out]


def dot(a, b):
    return lax.dot_general(a, b, (((1,), (0,)), ((), ())), preferred_element_type=f32)


def dot_nt(a, b):
    return lax.dot_general(a, b, (((1,), (1,)), ((), ())), preferred_element_type=f32)


def split(x):
    high = x.astype(bf16)
    return high, (x - high.astype(f32)).astype(bf16)


def deep(table, x):
    xh, xl = split(x)
    return dot(table, jnp.concatenate([xh, xh, xl], axis=0))


def right(ah, al, high, low):
    return dot(
        jnp.concatenate([ah, al, ah], axis=1), jnp.concatenate([high, high, low], axis=0)
    )


def row_sum(x):
    return jnp.sum(jnp.sum(x.reshape(-1, 8, 128), axis=0), axis=0, keepdims=True)


def lane_total(row):
    return jnp.sum(row, axis=1, keepdims=True)


def kernel(
    shift_hbm, dij_hbm, kind_hbm, psi_hbm, sticks_hbm, z3_hbm, vloc_hbm, dv_hbm, zt3_hbm, xh_hbm, xl_hbm, xth_hbm, xtl_hbm,
    yh_hbm, yl_hbm, yt3_hbm, beta_hbm,
    first_out, second_out, weights_out, cells_out,
    shift, dij, kind, psi, sticks, z3, vloc_flat, dv_flat, zt3, xh, xl, xth, xtl, yh, yl, yt3,
    beta, vloc, dv, cells, occupied, onehot, mask, send, recv, small_send, small_recv,
    part_send, part_recv, lhs, grid, ex, eh, el, dh, dl, psi_field, field0, field1,
    q, proj, coef, couple, vec, image, kin, own, dens,
    load_sem, psi_sem, ssem, rsem, rall, tssem, trsem, part_sem,
):
    me = lax.axis_index("ga")
    mb = lax.axis_index("band")
    nb = 8
    mx, my = me // 4, lax.rem(me, 4)

    def peer(dx, dy):
        return lax.rem(mx + dx, 4) * 4 + lax.rem(my + dy, 4)

    OFFSETS = sorted(
        ((dx, dy) for dx in range(4) for dy in range(4) if dx or dy),
        key=lambda o: -(min(o[0], 4 - o[0]) + min(o[1], 4 - o[1])),
    )
    X_ORDER = (2, 1, 3, 0)
    BANDS_FAR = (4, 5, 3, 2, 6, 7, 1)

    barrier = pltpu.get_barrier_semaphore()

    for offset in OFFSETS:
        pl.semaphore_signal(barrier, inc=1, device_id=(peer(*offset), mb), device_id_type=MESH)
    for k in BANDS_FAR:
        pl.semaphore_signal(
            barrier, inc=1, device_id=(me, lax.rem(mb + k, nb)), device_id_type=MESH
        )
    loads = {}
    pairs = dict(
        psi=(psi_hbm, psi), z3=(z3_hbm, z3), sticks=(sticks_hbm, sticks),
        kind=(kind_hbm, kind), dij=(dij_hbm, dij), shift=(shift_hbm, shift),
        dv=(dv_hbm, dv_flat), xh=(xh_hbm, xh), xl=(xl_hbm, xl), yh=(yh_hbm, yh),
        yl=(yl_hbm, yl), yt3=(yt3_hbm, yt3), xth=(xth_hbm, xth), xtl=(xtl_hbm, xtl),
        zt3=(zt3_hbm, zt3), vloc=(vloc_hbm, vloc_flat),
        beta=(beta_hbm, beta),
    )
    for at, (name, (source, target)) in enumerate(pairs.items()):
        loads[name] = pltpu.make_async_copy(source, target, load_sem.at[at])
        loads[name].start()

    def came(rnd, owner):
        return rsem.at[owner] if rnd == 0 else rall.at[rnd - 1]

    def copy(source, target, gone, landed, where):
        return pltpu.make_async_remote_copy(
            src_ref=source, dst_ref=target, send_sem=gone, recv_sem=landed,
            device_id=where, device_id_type=MESH,
        )

    def ga_copy(rnd, other):
        return copy(
            send.at[rnd, other], recv.at[rnd, me], ssem.at[rnd], came(rnd, me), (other, mb)
        )

    def ga_landed(rnd, other):
        return copy(
            send.at[rnd, other], recv.at[rnd, other], ssem.at[rnd], came(rnd, other), (other, mb)
        )

    others = pl.ds(0, GROUPS - 1)
    right_of = (lax.rem(me + 1, GROUPS), mb)

    def ga_all(rnd):
        return copy(
            send.at[rnd, others], recv.at[rnd, others], ssem.at[rnd], came(rnd, 0), right_of
        )

    def exchange(rnd):
        for offset in OFFSETS:
            ga_copy(rnd, peer(*offset)).start()
        recv[rnd, me] = send[rnd, me]

    @jax.named_scope("arrived")
    def arrived(rnd):
        ga_all(rnd).wait_recv()

    def small_exchange(rnd):
        for offset in OFFSETS:
            copy(
                small_send.at[rnd], small_recv.at[rnd, me], tssem.at[rnd], trsem.at[rnd],
                (peer(*offset), mb),
            ).start()
        small_recv[rnd, me] = small_send[rnd]

    def small_all(rnd):
        landed = small_recv.at[rnd, others]
        return copy(landed, landed, tssem.at[rnd], trsem.at[rnd], right_of)

    def small_total(rnd):
        with jax.named_scope("small_wait"):
            small_all(rnd).wait_recv()
        return jnp.sum(small_recv[rnd], axis=0)

    def psi_copy(k):
        where = (me, lax.rem(mb + k, nb))
        return copy(psi, occupied.at[mb], psi_sem.at[0], psi_sem.at[1], where)

    rest = pl.ds(0, nb - 1)
    after = (me, lax.rem(mb + 1, nb))

    def psi_all():
        return copy(occupied.at[rest], occupied.at[rest], psi_sem.at[0], psi_sem.at[1], after)

    def part_copy(k):
        other = lax.rem(mb + k, nb)
        return copy(
            part_send.at[other], part_recv.at[mb], part_sem.at[0], part_sem.at[1], (me, other)
        )

    def part_all():
        return copy(part_send.at[rest], part_recv.at[rest], part_sem.at[0], part_sem.at[1], after)

    def dealt(rnd, planes):
        for d in range(GROUPS):
            head = planes[8 * d : 8 * d + 8]
            tail = planes[128 + 4 * d : 132 + 4 * d]
            send[rnd, d, 0:8] = head[:, 0:128]
            send[rnd, d, 8:16] = jnp.concatenate([tail[:, 0:128], tail[:, 128:256]], axis=0)
            send[rnd, d, 16:24] = head[:, 128:256]

    def collected(rnd):
        rows = [
            jnp.concatenate([recv[rnd, d, 0:8], recv[rnd, d, 16:24]], axis=1)
            for d in range(GROUPS)
        ]
        for d in range(0, GROUPS, 2):
            even, odd = recv[rnd, d, 8:16], recv[rnd, d + 1, 8:16]
            rows.append(
                jnp.concatenate(
                    [
                        jnp.concatenate([even[0:4], odd[0:4]], axis=0),
                        jnp.concatenate([even[4:8], odd[4:8]], axis=0),
                    ],
                    axis=1,
                )
            )
        return jnp.concatenate(rows, axis=0)

    for name in ("psi", "z3"):
        loads[name].wait()
    with jax.named_scope("z_psi"):
        wide = jnp.concatenate(
            [jnp.concatenate([psi[c, 0], psi[c, 1]], axis=1) for c in range(2)], axis=0
        )
        dealt(0, dot(z3[:, 0:384], jnp.concatenate([wide, wide], axis=0)))

    def places(xy):
        flat = xy.astype(f32)
        y = jnp.floor((flat + 0.5) * (1.0 / GRID))
        x = flat - GRID * y
        fy = jnp.where(y >= GRID // 2, y - GRID, y)
        fx = jnp.where(x >= GRID // 2, x - GRID, x)
        return fy, fx

    loads["sticks"].wait()
    with jax.named_scope("tables"):
        fy, fx = places(sticks[...])
        ky = fy + SIDE // 2
        kx = fx + SIDE // 2
        high = jnp.floor(ky * 0.125)
        low = (ky - 8.0 * high) * SIDE + kx
        for k in range(GROUPS):
            own[0:1, 128 * k : 128 * k + 128] = low[k : k + 1, :]
            own[1:2, 128 * k : 128 * k + 128] = high[k : k + 1, :]
        mask[...] = (
            lax.broadcasted_iota(jnp.int32, (8, 2048), 0).astype(f32) == own[1:2, :]
        ).astype(f32)

        def fill(k, c):
            lanes = pl.ds(pl.multiple_of(k * 256, 256), 256)
            ids = lax.broadcasted_iota(jnp.int32, (512, 256), 0).astype(f32)
            onehot[:, lanes] = (ids == own[0:1, lanes]).astype(f32).astype(bf16)
            return c

        lax.fori_loop(0, 8, fill, 0)
        oy, ox = places(sticks[pl.ds(me, 1), :])
        kz = lax.broadcasted_iota(jnp.int32, (GRID, 128), 0).astype(f32)
        fz = jnp.where(kz >= GRID // 2, kz - GRID, kz)
        kin[...] = (fz * fz + (oy * oy + ox * ox)) * (4.0 / (GRID * GRID))

    row = lax.broadcasted_iota(jnp.int32, (128, 128), 0)
    lane = lax.broadcasted_iota(jnp.int32, (128, 128), 1)

    def couple_all():
        atom = lax.broadcasted_iota(jnp.int32, (1, 128), 1) // 4
        kinds = jnp.zeros((1, 128), jnp.int32)
        for a in range(32):
            kinds = jnp.where(atom == a, kind[a], kinds)
        same = (row // 4) == (lane // 4)
        first = kinds == 0
        total = jnp.zeros((128, 128), f32)
        for i in range(4):
            for k in range(4):
                value = jnp.where(first, dij[0, i, k], dij[1, i, k])
                here = same & ((row % 4) == i) & ((lane % 4) == k)
                total = total + jnp.where(here, value, 0.0)
        couple[...] = total

    def unpack(flat, out):
        def body(g, c):
            piece = flat[:, pl.ds(pl.multiple_of(g * 384, 384), 384)]
            tail = jnp.zeros((PLANES, 32), f32)
            for r in range(4):
                if r < 3:
                    cut = piece[:, 96 * r : 96 * r + 128]
                else:
                    cut = jnp.concatenate([piece[:, 288:384], tail], axis=1)
                cells[pl.ds(pl.multiple_of(g * 32, 32) + 8 * r, PLANES), :] = cut
            return c

        lax.fori_loop(0, 24, body, 0)
        for p in range(PLANES):
            out[:, 128 * p : 128 * p + 128] = cells[pl.ds(p, GRID, stride=8), :]

    for name in ("kind", "dij", "shift"):
        loads[name].wait()
    with jax.named_scope("couple"):
        couple_all()
    with jax.named_scope("barrier"):
        pl.semaphore_wait(barrier, GROUPS - 1 + nb - 1)
    exchange(0)

    for k in BANDS_FAR:
        psi_copy(k).start()
    occupied[mb] = psi[...]

    with jax.named_scope("unpack"):
        loads["dv"].wait()
        unpack(dv_flat, dv)
    for name in ("xh", "xl", "yh", "yl", "yt3", "xth", "xtl", "zt3"):
        loads[name].wait()
    ones = jnp.ones((256, 128), bf16)

    def fill_planes(rnd, out):

        def laid(src):
            piece = recv[rnd, src]
            upper = piece.astype(bf16).astype(f32)
            lower = piece - upper
            cols = pl.ds(pl.multiple_of(src * 128, 128) if rnd == 0 else src * 128, 128)
            keep = mask[:, cols]
            for n, part in enumerate((upper, lower)):
                for index in range(12):
                    pair = (index, index + 16 if index < 8 else index + 4)
                    two = [jnp.broadcast_to(part[r : r + 1], (8, 128)) * keep for r in pair]
                    at = 192 * n + 16 * index
                    lhs[at : at + 16, cols] = jnp.concatenate(two, axis=0).astype(bf16)

        def body(k, c):
            src = lax.rem(me + k, GROUPS)

            @pl.when(k > 0)
            def _():
                ga_landed(rnd, src).wait_recv()

            laid(src)
            return c

        with jax.named_scope("fill_lhs"):
            if rnd == 0:
                lax.fori_loop(0, GROUPS, body, 0)
            else:
                arrived(rnd)
        if rnd:
            for src in range(GROUPS):
                laid(src)
        with jax.named_scope("fill_dot"):
            both = dot_nt(lhs[...], onehot[...])
            grid[...] = both[0:192] + both[192:384]
        with jax.named_scope("fill_x"):
            data = [
                jnp.concatenate(
                    [grid[0:96, 128 * t : 128 * t + 128], grid[96:192, 128 * t : 128 * t + 128]],
                    axis=1,
                )
                for t in range(4)
            ]
            ah, al = split(jnp.concatenate(data, axis=0))
            ex[...] = right(ah, al, xh[...], xl[...])
            for c in range(2):
                for t in range(4):
                    rows = slice(16 * (4 * c + t), 16 * (4 * c + t) + 16)
                    for i in range(12):
                        at = 96 * t + 8 * i
                        two = [ex[at : at + 8, 128 * (2 * c + j) : 128 * (2 * c + j) + 128] for j in (0, 1)]
                        uh, ul = split(jnp.concatenate(two, axis=0))
                        dh[rows, 128 * i : 128 * i + 128] = uh
                        dl[rows, 128 * i : 128 * i + 128] = ul
        with jax.named_scope("fill_y"):
            for part in range(6):
                lanes = slice(256 * part, 256 * part + 256)
                out[:, lanes] = dot(
                    jnp.concatenate([yh[...], yh[...], yl[...]], axis=1),
                    jnp.concatenate([dh[:, lanes], dl[:, lanes], dh[:, lanes]], axis=0),
                )

    def to_sticks(rnd, potential, source):
        with jax.named_scope("stick_y"):
            for p in range(PLANES):
                lanes = slice(256 * p, 256 * p + 256)
                pot = potential[:, 128 * p : 128 * p + 128]
                pot = jnp.concatenate([pot, pot], axis=1)
                pot = jnp.concatenate([pot, pot], axis=0)
                ah, al = split(source[:, lanes] * pot)
                along = dot(yt3[...], jnp.concatenate([ah, al, ah], axis=0))
                for c in range(2):
                    for t in range(4):
                        for j in range(2):
                            rows = slice(8 * (8 * c + 2 * t + j), 8 * (8 * c + 2 * t + j) + 8)
                            two = jnp.concatenate([along[rows, 0:128], along[rows, 128:256]], axis=0)
                            uh, ul = split(two)
                            at = 96 * t + 16 * p
                            cols = slice(128 * (2 * c + j), 128 * (2 * c + j) + 128)
                            eh[at : at + 16, cols] = uh
                            el[at : at + 16, cols] = ul
        with jax.named_scope("stick_x"):
            along = right(eh[...], el[...], xth[...], xtl[...])
            for r in range(0, ROWS, 2):
                if r < 12:
                    index, b = r, 0
                else:
                    index, b = (r - 4, 1) if r < 16 else (r - 16, 1)
                for t in range(4):
                    two = []
                    for n in (index, index + 1):
                        at = 96 * t + 8 * (2 * (n % PLANES) + b)
                        col = 128 * (n // PLANES)
                        two.append(along[at : at + 8, col : col + 128])
                    uh, ul = split(jnp.concatenate(two, axis=0))
                    lanes = slice(128 * t, 128 * t + 128)
                    q[8 * r : 8 * r + 16, lanes] = uh
                    q[192 + 8 * r : 208 + 8 * r, lanes] = ul

        with jax.named_scope("stick_pick"):
            for k, dx in enumerate(X_ORDER + (None,)):
                if dx is not None:
                    quad = lax.rem(mx + dx, 4)
                    lanes = pl.ds(pl.multiple_of(quad * 512, 512), 512)
                    both = dot(q[...], onehot[:, lanes])
                    found = both[0:192] + both[192:384]
                    picked = jnp.sum(found.reshape(ROWS, 8, 512) * mask[:, lanes][None], axis=1)
                    for n in range(4):
                        send[rnd, 4 * quad + n] = picked[:, 128 * n : 128 * n + 128]
                if k > 0:
                    for dy in (2, 1, 3, 0):
                        if X_ORDER[k - 1] or dy:
                            ga_copy(rnd, peer(X_ORDER[k - 1], dy)).start()
            recv[rnd, me] = send[rnd, me]

    def z_forward(rnd):
        return deep(zt3[...], collected(rnd))

    def project(load, count, source):
        step = 4

        def body(g, c):
            sums = [[None] * 4 for _ in range(step)]
            for z in range(GRID // 8):
                v = [
                    source[96 * c + 8 * z : 96 * c + 8 * z + 8, 128 * b : 128 * b + 128]
                    for c in range(2)
                    for b in range(2)
                ]
                for t in range(step):
                    p0, p1 = load(g * step + t, 8 * z, 8)
                    for b in range(2):
                        re = p0 * v[b] + p1 * v[2 + b]
                        im = p0 * v[2 + b] - p1 * v[b]
                        sums[t][b] = re if z == 0 else sums[t][b] + re
                        sums[t][2 + b] = im if z == 0 else sums[t][2 + b] + im
            for t in range(step):
                for o in range(4):
                    proj[o, pl.ds(g * step + t, 1), :] = jnp.sum(
                        sums[t][o], axis=0, keepdims=True
                    )
            return c

        with jax.named_scope("project"):
            lax.fori_loop(0, count // step, body, 0)

    def projections(o, count):
        ph, pl_ = split(proj[o, 0:count, :])
        one = jnp.ones((8, 128), bf16)
        return dot_nt(
            jnp.concatenate([one, one], axis=1), jnp.concatenate([ph, pl_], axis=1)
        )[0:1, :]

    def spread(matrix, values):
        count = matrix.shape[0]
        for o in range(4):
            mh, ml = split(matrix * values[o : o + 1, :])
            coef[o, 0:count, :] = dot(jnp.concatenate([mh, ml], axis=1), ones)

    def apply(load, count, base):
        rows = 24
        for z in range(GRID // rows):

            def body(g, acc):
                for t in range(4):
                    j = g * 4 + t
                    p0, p1 = load(j, z * rows, rows)
                    out = []
                    for b in range(2):
                        cr = coef[b, pl.ds(j, 1), :]
                        ci = coef[2 + b, pl.ds(j, 1), :]
                        out.append(acc[2 * b] + (p0 * cr - p1 * ci))
                        out.append(acc[2 * b + 1] + (p0 * ci + p1 * cr))
                    acc = out
                return tuple(acc)

            init = tuple(
                base[96 * c + z * rows : 96 * c + z * rows + rows, 128 * b : 128 * b + 128]
                for b in range(2)
                for c in range(2)
            )
            with jax.named_scope("apply"):
                done = lax.fori_loop(0, count // 4, body, init)
            for b in range(2):
                for c in range(2):
                    at = 96 * c + z * rows
                    image[at : at + rows, 128 * b : 128 * b + 128] = done[2 * b + c]

    def beta_rows(j, at=0, rows=GRID):
        return beta[0, j, at : at + rows, :], beta[1, j, at : at + rows, :]

    def psi_rows(m, at=0, rows=GRID):
        owner, b = m // 2, m % 2
        return (
            occupied[owner, 0, b, at : at + rows, :].astype(f32),
            occupied[owner, 1, b, at : at + rows, :].astype(f32),
        )

    fill_planes(0, psi_field)
    to_sticks(1, dv, psi_field)

    arrived(1)
    vec[1] = z_forward(1)
    psi_all().wait_recv()

    project(psi_rows, 16, vec.at[1])
    small_send[0] = jnp.zeros((8, 128), f32)
    for o in range(4):
        small_send[0, o : o + 1, 0:16] = projections(o, 16)
    small_exchange(0)
    with jax.named_scope("unpack"):
        loads["vloc"].wait()
        unpack(vloc_flat, vloc)
    found = small_total(0) * (1.0 / (2.0 * GRID * 2048))
    eye = (row[0:16] == lane[0:16]).astype(f32)
    spread(eye, found)
    vec[1] = -vec[1]
    apply(psi_rows, 16, vec.at[1])
    vec[0] = image[...]

    def transform_out(rnd, source):
        dealt(rnd, deep(z3[...], source[...]))
        exchange(rnd)

    def stick_sum(a, b, weight=None):
        out = []
        for n in range(2):
            at = slice(128 * n, 128 * n + 128)
            both = a[0:96, at] * b[0:96, at] + a[96:192, at] * b[96:192, at]
            if weight is not None:
                both = both * (kin[...] + shift[n])
            out.append(row_sum(both))
        return out

    def grid_sum(a, b):
        out = []
        for n in range(2):
            total = jnp.zeros((1, 128), f32)
            for p in range(PLANES):
                lanes = slice(128 * (2 * p + n), 128 * (2 * p + n) + 128)
                pot = vloc[:, 128 * p : 128 * p + 128]
                both = a[0:96, lanes] * b[0:96, lanes] + a[96:192, lanes] * b[96:192, lanes]
                total = total + row_sum(both * pot)
            out.append(total)
        return out

    half = lax.broadcasted_iota(jnp.int32, (1, 128), 1) < 64

    def packed(pair):
        a, b = (r + pltpu.roll(r, 64, 1) for r in pair)
        return jnp.where(half, a, b)

    def unpacked(both):
        return [
            lane_total(jnp.where(half, both, 0.0)),
            lane_total(jnp.where(half, 0.0, both)),
        ]

    def band_dots(values, coupled):
        both = values * coupled
        return [lane_total(both[b : b + 1] + both[2 + b : 3 + b]) for b in range(2)]

    ch, cl = split(couple[...])

    def coupled_rows(values):
        vh, vl = split(values)
        return dot_nt(
            jnp.concatenate([vh, vl, vh], axis=1), jnp.concatenate([ch, ch, cl], axis=1)
        )

    direction = vec.at[0]
    transform_out(2, direction)
    loads["beta"].wait()
    project(beta_rows, 128, direction)
    small_send[1] = jnp.zeros((8, 128), f32)
    for o in range(4):
        small_send[1, o : o + 1, :] = projections(o, 128)
    small_send[1, 4:5, :] = packed(stick_sum(direction, direction))
    small_exchange(1)
    curves = stick_sum(direction, direction, True)
    fill_planes(2, field0)
    local = grid_sum(field0, field0)
    small_send[3] = jnp.zeros((8, 128), f32)
    small_send[3, 0:1, :] = packed([curves[b] + local[b] for b in range(2)])
    small_exchange(3)
    to_sticks(3, vloc, field0)
    sums = small_total(1)
    values0 = sums[0:4]
    coupled0 = coupled_rows(sums)[0:4]
    nonlocal0 = band_dots(values0, coupled0)
    norm0 = unpacked(sums[4:5])
    spread(couple[...], values0)
    for c in range(2):
        for b in range(2):
            at, of = slice(96 * c, 96 * c + 96), slice(128 * b, 128 * b + 128)
            vec[1, at, of] = direction[at, of] * (kin[...] + shift[b])
    apply(beta_rows, 128, vec.at[1])
    curve0 = [c + n for c, n in zip(unpacked(small_total(3)[0:1]), nonlocal0)]
    alpha0 = [norm0[b] / curve0[b] for b in range(2)]
    arrived(3)
    image[...] += z_forward(3)
    residual = vec.at[1]
    for c in range(2):
        for b in range(2):
            at, of = slice(96 * c, 96 * c + 96), slice(128 * b, 128 * b + 128)
            residual[at, of] = direction[at, of] - alpha0[b] * image[at, of]

    transform_out(4, residual)
    project(beta_rows, 128, residual)
    small_send[2] = jnp.zeros((8, 128), f32)
    for o in range(4):
        small_send[2, o : o + 1, :] = projections(o, 128)
    small_send[2, 4:5, :] = packed(stick_sum(residual, residual))
    small_exchange(2)
    selfs = stick_sum(residual, residual, True)
    crosses = stick_sum(residual, direction, True)
    fill_planes(4, field1)
    self_local = grid_sum(field1, field1)
    cross_local = grid_sum(field1, field0)
    small_send[4] = jnp.zeros((8, 128), f32)
    small_send[4, 0:1, :] = packed([selfs[b] + self_local[b] for b in range(2)])
    small_send[4, 1:2, :] = packed([crosses[b] + cross_local[b] for b in range(2)])
    small_exchange(4)
    with jax.named_scope("products"):
        for p in range(PLANES):
            for b in range(2):
                lanes = slice(128 * (2 * p + b), 128 * (2 * p + b) + 128)
                for n, field in enumerate((field0, field1)):
                    dens[96 * n : 96 * n + 96, lanes] = 4.0 * (
                        psi_field[0:96, lanes] * field[0:96, lanes]
                        + psi_field[96:192, lanes] * field[96:192, lanes]
                    )
    sums = small_total(2)
    values1 = sums[0:4]
    coupled1 = coupled_rows(sums)[0:4]
    self_dots = band_dots(values1, coupled1)
    cross_dots = band_dots(values1, coupled0)
    weight0, weight1 = [], []
    norm1 = unpacked(sums[4:5])
    sums = small_total(4)
    self1, cross1 = (unpacked(sums[n : n + 1]) for n in range(2))
    for b in range(2):
        ratio = norm1[b] / norm0[b]
        self_curve = self1[b] + self_dots[b]
        cross_curve = cross1[b] + cross_dots[b]
        curve = self_curve + ratio * (2.0 * cross_curve + ratio * curve0[b])
        alpha = norm1[b] / curve
        weight0.append(alpha0[b] + alpha * ratio)
        weight1.append(alpha)

    with jax.named_scope("density"):
        for p in range(PLANES):
            total = jnp.zeros((GRID, 128), f32)
            for b in range(2):
                lanes = slice(128 * (2 * p + b), 128 * (2 * p + b) + 128)
                total = total + weight0[b] * dens[0:96, lanes] + weight1[b] * dens[96:192, lanes]
            for i in range(nb):
                part_send[i, 12 * p : 12 * p + 12, :] = total[12 * i : 12 * i + 12, :]

    for k in BANDS_FAR:
        part_copy(k).start()
    part_recv[mb] = part_send[mb]
    first_out[...] = direction[...]
    second_out[...] = residual[...]
    for b in range(2):
        weights_out[b : b + 1, :] = jnp.broadcast_to(weight0[b], (1, 128))
        weights_out[2 + b : 3 + b, :] = jnp.broadcast_to(weight1[b], (1, 128))
    weights_out[4:8, :] = jnp.zeros((4, 128), f32)

    for rnd in range(5):
        ga_all(rnd).wait_send()
        small_all(rnd).wait_send()
    psi_all().wait_send()
    with jax.named_scope("part_wait"):
        part_all().wait_recv()
    cells_out[...] = jnp.sum(part_recv[...], axis=0)

    part_all().wait_send()


OUTS = tuple(
    pltpu.VMEM(shape, f32) for shape in ((192, 256), (192, 256), (8, 128), (72, 128))
)


def finish(first, second, weights, cells, response, density):
    for c in range(2):
        for b in range(2):
            at, of = slice(96 * c, 96 * c + 96), slice(128 * b, 128 * b + 128)
            response[c, b] = (
                weights[b : b + 1, :] * first[at, of] + weights[2 + b : 3 + b, :] * second[at, of]
            )
    for y in range(12):
        density[:, 96 * y : 96 * y + 96] = cells[pl.ds(y, PLANES, stride=12), :][:, 0:96]


def per_device(psi, vloc, dv, beta, dij, atom_type, stick_xy, band_shift):
    vmem = pl.BlockSpec(memory_space=pltpu.VMEM)
    dma = pltpu.SemaphoreType.DMA
    every = tables()
    early, late = every[:1], every[1:]
    pieces = pl.pallas_call(
        kernel,
        out_shape=OUTS,
        in_specs=[pl.BlockSpec(memory_space=pl.ANY)] * 17,
        out_specs=(vmem,) * 4,
        scratch_shapes=[
            pltpu.SMEM((2,), f32),
            pltpu.SMEM((2, 4, 4), f32),
            pltpu.SMEM((32,), jnp.int32),
            pltpu.VMEM((2, 2, GRID, 128), bf16),
            pltpu.VMEM((GROUPS, 128), jnp.int32),
            *[pltpu.VMEM(t.shape, t.dtype) for t in early],
            pltpu.VMEM((PLANES, GRID * GRID), f32),
            pltpu.VMEM((PLANES, GRID * GRID), f32),
            *[pltpu.VMEM(t.shape, t.dtype) for t in late],
            pltpu.VMEM((2, 128, GRID, 128), f32),
            pltpu.VMEM((GRID, 768), f32),
            pltpu.VMEM((GRID, 768), f32),
            pltpu.VMEM((768, 128), f32),
            pltpu.VMEM((8, 2, 2, GRID, 128), bf16),
            pltpu.VMEM((512, 2048), bf16),
            pltpu.VMEM((8, 2048), f32),
            pltpu.VMEM((5, GROUPS, ROWS, 128), f32),
            pltpu.VMEM((5, GROUPS, ROWS, 128), f32),
            pltpu.VMEM((5, 8, 128), f32),
            pltpu.VMEM((5, GROUPS, 8, 128), f32),
            pltpu.VMEM((8, 72, 128), f32),
            pltpu.VMEM((8, 72, 128), f32),
            pltpu.VMEM((384, 2048), bf16),
            pltpu.VMEM((192, 512), f32),
            pltpu.VMEM((384, 512), f32),
            pltpu.VMEM((384, 512), bf16),
            pltpu.VMEM((384, 512), bf16),
            pltpu.VMEM((128, 1536), bf16),
            pltpu.VMEM((128, 1536), bf16),
            pltpu.VMEM((192, 1536), f32),
            pltpu.VMEM((192, 1536), f32),
            pltpu.VMEM((192, 1536), f32),
            pltpu.VMEM((384, 512), bf16),
            pltpu.VMEM((4, 128, 128), f32),
            pltpu.VMEM((4, 128, 128), f32),
            pltpu.VMEM((128, 128), f32),
            pltpu.VMEM((2, 192, 256), f32),
            pltpu.VMEM((192, 256), f32),
            pltpu.VMEM((GRID, 128), f32),
            pltpu.VMEM((8, 2048), f32),
            pltpu.VMEM((192, 1536), f32),
            dma((17,)),
            dma((2,)),
            dma((5,)),
            dma((GROUPS,)),
            dma((4,)),
            dma((5,)),
            dma((5,)),
            dma((2,)),
        ],
        compiler_params=pltpu.CompilerParams(
            collective_id=0, has_side_effects=True, vmem_limit_bytes=60 * 1024 * 1024
        ),
    )(
        band_shift, dij, atom_type, psi, stick_xy.reshape(GROUPS, 128), *early,
        vloc, dv, *late, beta,
    )
    return pl.pallas_call(
        finish,
        out_shape=(
            jax.ShapeDtypeStruct((2, 2, GRID, 128), f32),
            jax.ShapeDtypeStruct((PLANES, 12 * GRID), f32),
        ),
        in_specs=[vmem] * 4,
        out_specs=(vmem, vmem),
    )(*(pltpu.with_memory_space_constraint(p, pltpu.VMEM) for p in pieces))


def solution(mesh):
    return jax.shard_map(
        per_device,
        mesh=mesh,
        in_specs=(
            P(None, "band", None, "ga"),
            P("ga", None),
            P("ga", None),
            P(None, None, None, "ga"),
            P(),
            P(),
            P(),
            P("band"),
        ),
        out_specs=(P(None, "band", None, "ga"), P("ga", "band")),
        check_vma=False,
    )
```

```python
import functools
import math

import jax
import jax.numpy as jnp
import numpy as np
from jax import lax
from jax.experimental import pallas as pl
from jax.experimental.pallas import tpu as pltpu
from jax.sharding import PartitionSpec as P

GRID = 96
SIDE = 64
GROUPS = 16
PLANES = 6
ROWS = 24
MESH = pl.DeviceIdType.MESH
f32 = jnp.float32
bf16 = jnp.bfloat16


def complex_table(angle):
    cos, sin = np.cos(angle), np.sin(angle)
    return np.array([[cos, -sin], [sin, cos]]) / math.sqrt(GRID)


def halves(table):
    high = np.asarray(table, np.float32).astype(jnp.bfloat16)
    low = (table - high.astype(np.float64)).astype(jnp.bfloat16)
    return high, low


def tables():
    unit = 2.0 * math.pi / GRID
    cells = np.arange(GRID)
    freqs = np.arange(SIDE) - SIDE // 2
    along_z = complex_table(unit * (cells[:, None] * cells[None, :] % GRID))
    along_z = along_z.reshape(2, 2, GROUPS, PLANES, GRID)
    z_table = np.einsum("oidpk->dopik", along_z).reshape(GROUPS, 12, 2 * GRID)
    z_table = np.concatenate(
        [z_table[:, :8].reshape(128, -1), z_table[:, 8:].reshape(64, -1)], axis=0
    )
    along_x = np.zeros((2, 2, SIDE, 128))
    along_x[..., :GRID] = complex_table(unit * (freqs[:, None] * cells[None, :] % GRID))
    x_table = np.einsum("oikx,be->ibkoex", along_x, np.eye(2)).reshape(256, 512)
    along_y = complex_table(unit * (cells[:, None] * freqs[None, :] % GRID))
    along_y = along_y.reshape(2, 2, GRID, 8, 8)
    y_table = np.einsum("oiygl->oyilg", along_y).reshape(192, 128)
    out = []
    for table in (z_table, z_table.T):
        high, low = halves(np.ascontiguousarray(table))
        out.append(np.concatenate([high, low, high], axis=1))
    for table in (x_table, x_table.T, y_table):
        out.extend(halves(np.ascontiguousarray(table)))
    high, low = halves(np.ascontiguousarray(y_table.T))
    out.append(np.concatenate([high, high, low], axis=1))
    pick = np.zeros((128, 256))
    signs = np.zeros((4, 24, 256))

    def place(index, b):
        return index if b == 0 else (index + 16 if index < 8 else index + 4)

    def enter(out_row, n, col, c_out, c_in):
        if c_out == c_in:
            signs[n, out_row, col] = 1.0
        else:
            signs[2 + n, out_row, col] = 1.0 if c_out else -1.0

    for m in range(16):
        owner, b = m // 2, m % 2
        for c in range(2):
            for p in range(PLANES):
                pick[m, 24 * owner + place(6 * c + p, b)] = 1.0
            pick[m, 192 + 8 * owner + 2 * c + b] = 1.0
            for n in range(2):
                for c_out in range(2):
                    for p in range(PLANES):
                        enter(
                            place(6 * c_out + p, n), n, 24 * owner + place(6 * c + p, b), c_out, c
                        )
                    enter(2 * c_out + n, n, 192 + 8 * owner + 2 * c + b, c_out, c)
    out.append(pick.astype(jnp.bfloat16))
    out.append(signs.reshape(96, 256).astype(np.float32))
    return [jnp.asarray(t) for t in out]


def dot(a, b):
    return lax.dot_general(a, b, (((1,), (0,)), ((), ())), preferred_element_type=f32)


def dot_nt(a, b):
    return lax.dot_general(a, b, (((1,), (1,)), ((), ())), preferred_element_type=f32)


def split(x):
    high = x.astype(bf16)
    return high, (x - high.astype(f32)).astype(bf16)


def deep(table, x):
    xh, xl = split(x)
    return dot(table, jnp.concatenate([xh, xh, xl], axis=0))


def right(ah, al, high, low):
    return dot(
        jnp.concatenate([ah, al, ah], axis=1), jnp.concatenate([high, high, low], axis=0)
    )


def row_sum(x):
    return jnp.sum(jnp.sum(x.reshape(-1, 8, 128), axis=0), axis=0, keepdims=True)


def lane_total(row):
    return jnp.sum(row, axis=1, keepdims=True)


def kernel(
    shift_hbm, dij_hbm, kind_hbm, psi_hbm, sticks_hbm, z3_hbm, vloc_hbm, dv_hbm, zt3_hbm, xh_hbm, xl_hbm, xth_hbm, xtl_hbm,
    yh_hbm, yl_hbm, yt3_hbm, pick_hbm, signs_hbm, beta_hbm,
    first_out, second_out, weights_out, cells_out,
    shift, dij, kind, psi, sticks, z3, vloc_flat, dv_flat, zt3, xh, xl, xth, xtl, yh, yl, yt3, pick, signs,
    beta, vloc, dv, cells, occupied, onehot, mask, send, recv, small_send, small_recv,
    part_send, part_recv, lhs, grid, ex, eh, el, dh, dl, psi_field, field0, field1,
    q, found_all, zall, zbh, zbl, psi_proj, proj, coef, couple, vec, image, kin, own, dens,
    load_sem, psi_sem, z_sem, pp_sem, ssem, rsem, rall, tssem, trsem, part_sem,
):
    me = lax.axis_index("ga")
    mb = lax.axis_index("band")
    nb = 8
    mx, my = me // 4, lax.rem(me, 4)

    def peer(dx, dy):
        return lax.rem(mx + dx, 4) * 4 + lax.rem(my + dy, 4)

    OFFSETS = sorted(
        ((dx, dy) for dx in range(4) for dy in range(4) if dx or dy),
        key=lambda o: -(min(o[0], 4 - o[0]) + min(o[1], 4 - o[1])),
    )
    X_ORDER = (2, 1, 3, 0)
    BANDS_FAR = (4, 5, 3, 2, 6, 7, 1)

    barrier = pltpu.get_barrier_semaphore()

    for offset in OFFSETS:
        pl.semaphore_signal(barrier, inc=1, device_id=(peer(*offset), mb), device_id_type=MESH)
    for k in BANDS_FAR:
        pl.semaphore_signal(
            barrier, inc=1, device_id=(me, lax.rem(mb + k, nb)), device_id_type=MESH
        )
    loads = {}
    pairs = dict(
        psi=(psi_hbm, psi), z3=(z3_hbm, z3), sticks=(sticks_hbm, sticks),
        kind=(kind_hbm, kind), dij=(dij_hbm, dij), shift=(shift_hbm, shift),
        dv=(dv_hbm, dv_flat), xh=(xh_hbm, xh), xl=(xl_hbm, xl), yh=(yh_hbm, yh),
        yl=(yl_hbm, yl), yt3=(yt3_hbm, yt3), xth=(xth_hbm, xth), xtl=(xtl_hbm, xtl),
        zt3=(zt3_hbm, zt3), pick=(pick_hbm, pick), signs=(signs_hbm, signs), vloc=(vloc_hbm, vloc_flat),
        beta=(beta_hbm, beta),
    )
    for at, (name, (source, target)) in enumerate(pairs.items()):
        loads[name] = pltpu.make_async_copy(source, target, load_sem.at[at])
        loads[name].start()

    def came(rnd, owner):
        return rsem.at[owner] if rnd == 0 else rall.at[rnd - 1]

    def copy(source, target, gone, landed, where):
        return pltpu.make_async_remote_copy(
            src_ref=source, dst_ref=target, send_sem=gone, recv_sem=landed,
            device_id=where, device_id_type=MESH,
        )

    def ga_copy(rnd, other):
        return copy(
            send.at[rnd, other], recv.at[rnd, me], ssem.at[rnd], came(rnd, me), (other, mb)
        )

    def ga_landed(rnd, other):
        return copy(
            send.at[rnd, other], recv.at[rnd, other], ssem.at[rnd], came(rnd, other), (other, mb)
        )

    others = pl.ds(0, GROUPS - 1)
    right_of = (lax.rem(me + 1, GROUPS), mb)

    def ga_all(rnd):
        return copy(
            send.at[rnd, others], recv.at[rnd, others], ssem.at[rnd], came(rnd, 0), right_of
        )

    def exchange(rnd):
        for offset in OFFSETS:
            ga_copy(rnd, peer(*offset)).start()
        recv[rnd, me] = send[rnd, me]

    @jax.named_scope("arrived")
    def arrived(rnd):
        ga_all(rnd).wait_recv()

    def small_exchange(rnd):
        for offset in OFFSETS:
            copy(
                small_send.at[rnd], small_recv.at[rnd, me], tssem.at[rnd], trsem.at[rnd],
                (peer(*offset), mb),
            ).start()
        small_recv[rnd, me] = small_send[rnd]

    def small_all(rnd):
        landed = small_recv.at[rnd, others]
        return copy(landed, landed, tssem.at[rnd], trsem.at[rnd], right_of)

    def small_total(rnd):
        with jax.named_scope("small_wait"):
            small_all(rnd).wait_recv()
        return jnp.sum(small_recv[rnd], axis=0)

    mz, mc = mb // 2, lax.rem(mb, 2)
    partner = mz * 2 + 1 - mc

    def alike(dz):
        return lax.rem(mz + dz, 4) * 2 + mc

    def gather_out(block, slot, sems):
        for dz in (2, 1, 3):
            copy(block, slot, sems.at[0], sems.at[1], (me, alike(dz))).start()
        copy(block, slot, sems.at[0], sems.at[2], (me, partner)).start()

    def planes_out(first):
        some = pl.ds(first, 8)
        gather_out(recv.at[0, some], zall.at[mb, some], z_sem)

    def gather_bytes(count, held, sems, which):
        some = held.at[pl.ds(0, count)]
        return copy(some, some, sems.at[0], sems.at[which], (me, partner))

    def gather_on(held, sems):
        gather_bytes(3, held, sems, 1).wait_recv()
        for dz in (1, 3, 2):
            slot = held.at[alike(dz)]
            copy(slot, slot, sems.at[0], sems.at[2], (me, partner)).start()

    def gather_done(held, sems):
        gather_bytes(4, held, sems, 2).wait_recv()

    def gather_sent(held, sems):
        gather_bytes(7, held, sems, 1).wait_send()

    rest = pl.ds(0, nb - 1)
    after = (me, lax.rem(mb + 1, nb))

    def proj_copy(k):
        where = (me, lax.rem(mb + k, nb))
        return copy(psi_proj.at[16], psi_proj.at[8 + mb], pp_sem.at[0], pp_sem.at[1], where)

    def proj_all():
        some = psi_proj.at[rest]
        return copy(some, some, pp_sem.at[0], pp_sem.at[1], after)

    def part_copy(k):
        other = lax.rem(mb + k, nb)
        return copy(
            part_send.at[other], part_recv.at[mb], part_sem.at[0], part_sem.at[1], (me, other)
        )

    def part_all():
        return copy(part_send.at[rest], part_recv.at[rest], part_sem.at[0], part_sem.at[1], after)

    def dealt(rnd, planes):
        for d in range(GROUPS):
            head = planes[8 * d : 8 * d + 8]
            tail = planes[128 + 4 * d : 132 + 4 * d]
            send[rnd, d, 0:8] = head[:, 0:128]
            send[rnd, d, 8:16] = jnp.concatenate([tail[:, 0:128], tail[:, 128:256]], axis=0)
            send[rnd, d, 16:24] = head[:, 128:256]

    def collected(rnd):
        rows = [
            jnp.concatenate([recv[rnd, d, 0:8], recv[rnd, d, 16:24]], axis=1)
            for d in range(GROUPS)
        ]
        for d in range(0, GROUPS, 2):
            even, odd = recv[rnd, d, 8:16], recv[rnd, d + 1, 8:16]
            rows.append(
                jnp.concatenate(
                    [
                        jnp.concatenate([even[0:4], odd[0:4]], axis=0),
                        jnp.concatenate([even[4:8], odd[4:8]], axis=0),
                    ],
                    axis=1,
                )
            )
        return jnp.concatenate(rows, axis=0)

    for name in ("psi", "z3"):
        loads[name].wait()
    with jax.named_scope("z_psi"):
        wide = jnp.concatenate(
            [jnp.concatenate([psi[c, 0], psi[c, 1]], axis=1) for c in range(2)], axis=0
        )
        dealt(0, dot(z3[:, 0:384], jnp.concatenate([wide, wide], axis=0)))

    def places(xy):
        flat = xy.astype(f32)
        y = jnp.floor((flat + 0.5) * (1.0 / GRID))
        x = flat - GRID * y
        fy = jnp.where(y >= GRID // 2, y - GRID, y)
        fx = jnp.where(x >= GRID // 2, x - GRID, x)
        return fy, fx

    loads["sticks"].wait()
    with jax.named_scope("tables"):
        fy, fx = places(sticks[...])
        ky = fy + SIDE // 2
        kx = fx + SIDE // 2
        high = jnp.floor(ky * 0.125)
        low = (ky - 8.0 * high) * SIDE + kx
        for k in range(GROUPS):
            own[0:1, 128 * k : 128 * k + 128] = low[k : k + 1, :]
            own[1:2, 128 * k : 128 * k + 128] = high[k : k + 1, :]
        mask[...] = (
            lax.broadcasted_iota(jnp.int32, (8, 2048), 0).astype(f32) == own[1:2, :]
        ).astype(f32)

        def fill(k, c):
            lanes = pl.ds(pl.multiple_of(k * 256, 256), 256)
            ids = lax.broadcasted_iota(jnp.int32, (512, 256), 0).astype(f32)
            onehot[:, lanes] = (ids == own[0:1, lanes]).astype(f32).astype(bf16)
            return c

        lax.fori_loop(0, 8, fill, 0)
        oy, ox = places(sticks[pl.ds(me, 1), :])
        kz = lax.broadcasted_iota(jnp.int32, (GRID, 128), 0).astype(f32)
        fz = jnp.where(kz >= GRID // 2, kz - GRID, kz)
        kin[...] = (fz * fz + (oy * oy + ox * ox)) * (4.0 / (GRID * GRID))

    row = lax.broadcasted_iota(jnp.int32, (128, 128), 0)
    lane = lax.broadcasted_iota(jnp.int32, (128, 128), 1)

    def couple_all():
        atom = lax.broadcasted_iota(jnp.int32, (1, 128), 1) // 4
        kinds = jnp.zeros((1, 128), jnp.int32)
        for a in range(32):
            kinds = jnp.where(atom == a, kind[a], kinds)
        same = (row // 4) == (lane // 4)
        first = kinds == 0
        total = jnp.zeros((128, 128), f32)
        for i in range(4):
            for k in range(4):
                value = jnp.where(first, dij[0, i, k], dij[1, i, k])
                here = same & ((row % 4) == i) & ((lane % 4) == k)
                total = total + jnp.where(here, value, 0.0)
        couple[...] = total

    def unpack(flat, out):
        def body(g, c):
            piece = flat[:, pl.ds(pl.multiple_of(g * 384, 384), 384)]
            tail = jnp.zeros((PLANES, 32), f32)
            for r in range(4):
                if r < 3:
                    cut = piece[:, 96 * r : 96 * r + 128]
                else:
                    cut = jnp.concatenate([piece[:, 288:384], tail], axis=1)
                cells[pl.ds(pl.multiple_of(g * 32, 32) + 8 * r, PLANES), :] = cut
            return c

        lax.fori_loop(0, 24, body, 0)
        for p in range(PLANES):
            out[:, 128 * p : 128 * p + 128] = cells[pl.ds(p, GRID, stride=8), :]

    for name in ("kind", "dij", "shift"):
        loads[name].wait()
    with jax.named_scope("couple"):
        couple_all()
    with jax.named_scope("unpack"):
        loads["dv"].wait()
        unpack(dv_flat, dv)
    zbh[192:256, :] = jnp.zeros((64, 2048), bf16)
    zbl[192:256, :] = jnp.zeros((64, 2048), bf16)
    psi_proj[0:8] = jnp.zeros((8, 8, 128), f32)
    psi_proj[16] = jnp.zeros((8, 128), f32)
    vec[0] = wide.astype(f32)
    with jax.named_scope("barrier"):
        pl.semaphore_wait(barrier, GROUPS - 1 + nb - 1)
    exchange(0)

    gather_out(psi, occupied.at[mb], psi_sem)
    occupied[mb] = psi[...]
    for name in ("xh", "xl", "yh", "yl", "yt3", "xth", "xtl", "zt3", "pick", "signs"):
        loads[name].wait()
    ones = jnp.ones((256, 128), bf16)

    def fill_planes(rnd, out):

        def laid(src):
            piece = recv[rnd, src]
            upper = piece.astype(bf16).astype(f32)
            lower = piece - upper
            cols = pl.ds(pl.multiple_of(src * 128, 128) if rnd == 0 else src * 128, 128)
            keep = mask[:, cols]
            for n, part in enumerate((upper, lower)):
                for index in range(12):
                    pair = (index, index + 16 if index < 8 else index + 4)
                    two = [jnp.broadcast_to(part[r : r + 1], (8, 128)) * keep for r in pair]
                    at = 192 * n + 16 * index
                    lhs[at : at + 16, cols] = jnp.concatenate(two, axis=0).astype(bf16)

        def body(k, c):
            src = lax.rem(me + k, GROUPS)

            @pl.when(k > 0)
            def _():
                ga_landed(rnd, src).wait_recv()

            laid(src)
            return c

        with jax.named_scope("fill_lhs"):
            if rnd == 0:
                lax.fori_loop(0, GROUPS, body, 0)
                planes_out(0)
                zall[mb] = recv[0]
            elif rnd != 2:
                arrived(rnd)
        if rnd:
            for src in range(GROUPS):
                laid(src)
        with jax.named_scope("fill_dot"):
            both = dot_nt(lhs[...], onehot[...])
            grid[...] = both[0:192] + both[192:384]
        with jax.named_scope("fill_x"):
            data = [
                jnp.concatenate(
                    [grid[0:96, 128 * t : 128 * t + 128], grid[96:192, 128 * t : 128 * t + 128]],
                    axis=1,
                )
                for t in range(4)
            ]
            ah, al = split(jnp.concatenate(data, axis=0))
            ex[...] = right(ah, al, xh[...], xl[...])
            for c in range(2):
                for t in range(4):
                    rows = slice(16 * (4 * c + t), 16 * (4 * c + t) + 16)
                    for i in range(12):
                        at = 96 * t + 8 * i
                        two = [ex[at : at + 8, 128 * (2 * c + j) : 128 * (2 * c + j) + 128] for j in (0, 1)]
                        uh, ul = split(jnp.concatenate(two, axis=0))
                        dh[rows, 128 * i : 128 * i + 128] = uh
                        dl[rows, 128 * i : 128 * i + 128] = ul
        with jax.named_scope("fill_y"):
            for part in range(6):
                lanes = slice(256 * part, 256 * part + 256)
                out[:, lanes] = dot(
                    jnp.concatenate([yh[...], yh[...], yl[...]], axis=1),
                    jnp.concatenate([dh[:, lanes], dl[:, lanes], dh[:, lanes]], axis=0),
                )

    def to_sticks(rnd, potential, source, between=None):
        with jax.named_scope("stick_y"):
            for p in range(PLANES):
                lanes = slice(256 * p, 256 * p + 256)
                pot = potential[:, 128 * p : 128 * p + 128]
                pot = jnp.concatenate([pot, pot], axis=1)
                pot = jnp.concatenate([pot, pot], axis=0)
                ah, al = split(source[:, lanes] * pot)
                along = dot(yt3[...], jnp.concatenate([ah, al, ah], axis=0))
                for c in range(2):
                    for t in range(4):
                        for j in range(2):
                            rows = slice(8 * (8 * c + 2 * t + j), 8 * (8 * c + 2 * t + j) + 8)
                            two = jnp.concatenate([along[rows, 0:128], along[rows, 128:256]], axis=0)
                            uh, ul = split(two)
                            at = 96 * t + 16 * p
                            cols = slice(128 * (2 * c + j), 128 * (2 * c + j) + 128)
                            eh[at : at + 16, cols] = uh
                            el[at : at + 16, cols] = ul
        with jax.named_scope("stick_x"):
            along = right(eh[...], el[...], xth[...], xtl[...])
            for r in range(0, ROWS, 2):
                if r < 12:
                    index, b = r, 0
                else:
                    index, b = (r - 4, 1) if r < 16 else (r - 16, 1)
                for t in range(4):
                    two = []
                    for n in (index, index + 1):
                        at = 96 * t + 8 * (2 * (n % PLANES) + b)
                        col = 128 * (n // PLANES)
                        two.append(along[at : at + 8, col : col + 128])
                    uh, ul = split(jnp.concatenate(two, axis=0))
                    lanes = slice(128 * t, 128 * t + 128)
                    q[8 * r : 8 * r + 16, lanes] = uh
                    q[192 + 8 * r : 208 + 8 * r, lanes] = ul

        if between is not None:
            between()
        with jax.named_scope("stick_pick"):
            for k in range(6):
                if k > 1:
                    dx = X_ORDER[k - 2]
                    for dy in (2, 1, 3, 0):
                        if dx or dy:
                            ga_copy(rnd, peer(dx, dy)).start()
                if k < 4:
                    quad = lax.rem(mx + X_ORDER[k], 4)
                    lanes = pl.ds(pl.multiple_of(quad * 512, 512), 512)
                    found_all[k % 2] = dot(q[...], onehot[:, lanes])
                if 0 < k < 5:
                    quad = lax.rem(mx + X_ORDER[k - 1], 4)
                    lanes = pl.ds(pl.multiple_of(quad * 512, 512), 512)
                    both = found_all[(k - 1) % 2, 0:192] + found_all[(k - 1) % 2, 192:384]
                    picked = jnp.sum(both.reshape(ROWS, 8, 512) * mask[:, lanes][None], axis=1)
                    for n in range(4):
                        send[rnd, 4 * quad + n] = picked[:, 128 * n : 128 * n + 128]
            recv[rnd, me] = send[rnd, me]

    def z_forward(rnd):
        return deep(zt3[...], collected(rnd))

    def project(load, count, source, begin=0):
        step = 4

        def body(g, c):
            sums = [[None] * 4 for _ in range(step)]
            for z in range(GRID // 8):
                v = [
                    source[96 * c + 8 * z : 96 * c + 8 * z + 8, 128 * b : 128 * b + 128]
                    for c in range(2)
                    for b in range(2)
                ]
                for t in range(step):
                    p0, p1 = load(g * step + t, 8 * z, 8)
                    for b in range(2):
                        re = p0 * v[b] + p1 * v[2 + b]
                        im = p0 * v[2 + b] - p1 * v[b]
                        sums[t][b] = re if z == 0 else sums[t][b] + re
                        sums[t][2 + b] = im if z == 0 else sums[t][2 + b] + im
            for t in range(step):
                for o in range(4):
                    proj[o, pl.ds(g * step + t, 1), :] = jnp.sum(
                        sums[t][o], axis=0, keepdims=True
                    )
            return c

        with jax.named_scope("project"):
            lax.fori_loop(begin // step, count // step, body, 0)

    def projections(o, count):
        ph, pl_ = split(proj[o, 0:count, :])
        one = jnp.ones((8, 128), bf16)
        return dot_nt(
            jnp.concatenate([one, one], axis=1), jnp.concatenate([ph, pl_], axis=1)
        )[0:1, :]

    def spread(matrix, values):
        count = matrix.shape[0]
        for o in range(4):
            mh, ml = split(matrix * values[o : o + 1, :])
            coef[o, 0:count, :] = dot(jnp.concatenate([mh, ml], axis=1), ones)

    def apply(load, count, base):
        rows = 24
        for z in range(GRID // rows):

            def body(g, acc):
                for t in range(4):
                    j = g * 4 + t
                    p0, p1 = load(j, z * rows, rows)
                    out = []
                    for b in range(2):
                        cr = coef[b, pl.ds(j, 1), :]
                        ci = coef[2 + b, pl.ds(j, 1), :]
                        out.append(acc[2 * b] + (p0 * cr - p1 * ci))
                        out.append(acc[2 * b + 1] + (p0 * ci + p1 * cr))
                    acc = out
                return tuple(acc)

            init = tuple(
                base[96 * c + z * rows : 96 * c + z * rows + rows, 128 * b : 128 * b + 128]
                for b in range(2)
                for c in range(2)
            )
            with jax.named_scope("apply"):
                done = lax.fori_loop(0, count // 4, body, init)
            for b in range(2):
                for c in range(2):
                    at = 96 * c + z * rows
                    image[at : at + rows, 128 * b : 128 * b + 128] = done[2 * b + c]

    def beta_rows(j, at=0, rows=GRID):
        return beta[0, j, at : at + rows, :], beta[1, j, at : at + rows, :]

    def psi_rows(m, at=0, rows=GRID):
        owner, b = m // 2, m % 2
        return (
            occupied[owner, 0, b, at : at + rows, :].astype(f32),
            occupied[owner, 1, b, at : at + rows, :].astype(f32),
        )

    with jax.named_scope("unpack"):
        loads["vloc"].wait()
        unpack(vloc_flat, vloc)
    loads["beta"].wait()
    project(beta_rows, 16, vec.at[0])
    fill_planes(0, psi_field)
    with jax.named_scope("pass_psi"):
        gather_on(occupied, psi_sem)
    to_sticks(1, dv, psi_field)
    planes_out(8)
    project(beta_rows, 128, vec.at[0], 16)
    for o in range(4):
        psi_proj[16, o : o + 1, :] = projections(o, 128)
    for k in BANDS_FAR:
        proj_copy(k).start()
    psi_proj[8 + mb] = psi_proj[16]
    arrived(1)
    vec[1] = z_forward(1)
    gather_done(occupied, psi_sem)

    project(psi_rows, 16, vec.at[1])
    small_send[0] = jnp.zeros((8, 128), f32)
    for o in range(4):
        small_send[0, o : o + 1, 0:16] = projections(o, 16)
    small_exchange(0)
    project(beta_rows, 64, vec.at[1])
    with jax.named_scope("pass_z"):
        gather_on(zall, z_sem)
    project(beta_rows, 128, vec.at[1], 64)
    image_proj = [projections(o, 128) for o in range(4)]
    proj_all().wait_recv()
    with jax.named_scope("z_wait"):
        gather_done(zall, z_sem)

    def halve(src, c):
        lanes = pl.ds(pl.multiple_of(src * 128, 128), 128)
        for e in range(4):
            both = jnp.concatenate([zall[2 * e, src], zall[2 * e + 1, src]], axis=0)
            uh, ul = split(both)
            zbh[48 * e : 48 * e + 48, lanes] = uh
            zbl[48 * e : 48 * e + 48, lanes] = ul
        return c

    with jax.named_scope("halve"):
        lax.fori_loop(0, GROUPS, halve, 0)
    found = small_total(0) * (1.0 / (2.0 * GRID * 2048))
    with jax.named_scope("enter"):
        fh, fl = split(found)
        laid_out = dot(
            jnp.concatenate([fh, fl], axis=1), jnp.concatenate([pick[...], pick[...]], axis=0)
        )
        entry = jnp.zeros((24, 256), f32)
        for o in range(4):
            entry = entry + signs[24 * o : 24 * o + 24, :] * laid_out[o : o + 1, :]
        nh, nl = split(entry[0:8, 128:256])
        ph, plow = split(psi_proj[0:16].reshape(128, 128))
        joined = dot(
            jnp.concatenate([nh, nl, nh], axis=1), jnp.concatenate([ph, ph, plow], axis=0)
        )
        small_send[1] = jnp.zeros((8, 128), f32)
        for o in range(4):
            small_send[1, o : o + 1, :] = joined[o : o + 1, :] - image_proj[o]
        small_exchange(1)
        mh, ml = split(entry)
        weights = jnp.concatenate([mh, ml, mh], axis=1)
        for part in range(4):
            lanes = slice(512 * part, 512 * part + 512)
            planes = dot(
                weights,
                jnp.concatenate([zbh[:, lanes], zbh[:, lanes], zbl[:, lanes]], axis=0),
            )
            for n in range(4):
                src = 4 * part + n
                recv[2, src] = planes[:, 128 * n : 128 * n + 128] - send[1, src]

    def transform_out(rnd, source):
        dealt(rnd, deep(z3[...], source[...]))
        exchange(rnd)

    def stick_sum(a, b, weight=None):
        out = []
        for n in range(2):
            at = slice(128 * n, 128 * n + 128)
            both = a[0:96, at] * b[0:96, at] + a[96:192, at] * b[96:192, at]
            if weight is not None:
                both = both * (kin[...] + shift[n])
            out.append(row_sum(both))
        return out

    def grid_sum(a, b):
        out = []
        for n in range(2):
            total = jnp.zeros((1, 128), f32)
            for p in range(PLANES):
                lanes = slice(128 * (2 * p + n), 128 * (2 * p + n) + 128)
                pot = vloc[:, 128 * p : 128 * p + 128]
                both = a[0:96, lanes] * b[0:96, lanes] + a[96:192, lanes] * b[96:192, lanes]
                total = total + row_sum(both * pot)
            out.append(total)
        return out

    half = lax.broadcasted_iota(jnp.int32, (1, 128), 1) < 64

    def packed(pair):
        a, b = (r + pltpu.roll(r, 64, 1) for r in pair)
        return jnp.where(half, a, b)

    def unpacked(both):
        return [
            lane_total(jnp.where(half, both, 0.0)),
            lane_total(jnp.where(half, 0.0, both)),
        ]

    def band_dots(values, coupled):
        both = values * coupled
        return [lane_total(both[b : b + 1] + both[2 + b : 3 + b]) for b in range(2)]

    ch, cl = split(couple[...])

    def coupled_rows(values):
        vh, vl = split(values)
        return dot_nt(
            jnp.concatenate([vh, vl, vh], axis=1), jnp.concatenate([ch, ch, cl], axis=1)
        )

    direction = vec.at[0]
    fill_planes(2, field0)
    local = grid_sum(field0, field0)

    def rhs():
        with jax.named_scope("rhs"):
            eye = (row[0:16] == lane[0:16]).astype(f32)
            spread(eye, found)
            vec[1] = -vec[1]
            apply(psi_rows, 16, vec.at[1])
            vec[0] = image[...]
            curves = stick_sum(direction, direction, True)
            small_send[3] = jnp.zeros((8, 128), f32)
            small_send[3, 0:1, :] = packed([curves[b] + local[b] for b in range(2)])
            small_send[3, 1:2, :] = packed(stick_sum(direction, direction))
            small_exchange(3)

    to_sticks(3, vloc, field0, rhs)
    sums = small_total(1)
    values0 = sums[0:4]
    coupled0 = coupled_rows(sums)[0:4]
    nonlocal0 = band_dots(values0, coupled0)
    spread(couple[...], values0)
    for c in range(2):
        for b in range(2):
            at, of = slice(96 * c, 96 * c + 96), slice(128 * b, 128 * b + 128)
            vec[1, at, of] = direction[at, of] * (kin[...] + shift[b])
    apply(beta_rows, 128, vec.at[1])
    sums = small_total(3)
    norm0 = unpacked(sums[1:2])
    curve0 = [c + n for c, n in zip(unpacked(sums[0:1]), nonlocal0)]
    alpha0 = [norm0[b] / curve0[b] for b in range(2)]
    arrived(3)
    image[...] += z_forward(3)
    residual = vec.at[1]
    for c in range(2):
        for b in range(2):
            at, of = slice(96 * c, 96 * c + 96), slice(128 * b, 128 * b + 128)
            residual[at, of] = direction[at, of] - alpha0[b] * image[at, of]

    transform_out(4, residual)
    project(beta_rows, 128, residual)
    small_send[2] = jnp.zeros((8, 128), f32)
    for o in range(4):
        small_send[2, o : o + 1, :] = projections(o, 128)
    small_send[2, 4:5, :] = packed(stick_sum(residual, residual))
    small_exchange(2)
    selfs = stick_sum(residual, residual, True)
    crosses = stick_sum(residual, direction, True)
    fill_planes(4, field1)
    self_local = grid_sum(field1, field1)
    cross_local = grid_sum(field1, field0)
    small_send[4] = jnp.zeros((8, 128), f32)
    small_send[4, 0:1, :] = packed([selfs[b] + self_local[b] for b in range(2)])
    small_send[4, 1:2, :] = packed([crosses[b] + cross_local[b] for b in range(2)])
    small_exchange(4)
    with jax.named_scope("products"):
        for p in range(PLANES):
            for b in range(2):
                lanes = slice(128 * (2 * p + b), 128 * (2 * p + b) + 128)
                for n, field in enumerate((field0, field1)):
                    dens[96 * n : 96 * n + 96, lanes] = 4.0 * (
                        psi_field[0:96, lanes] * field[0:96, lanes]
                        + psi_field[96:192, lanes] * field[96:192, lanes]
                    )
    sums = small_total(2)
    values1 = sums[0:4]
    coupled1 = coupled_rows(sums)[0:4]
    self_dots = band_dots(values1, coupled1)
    cross_dots = band_dots(values1, coupled0)
    weight0, weight1 = [], []
    norm1 = unpacked(sums[4:5])
    sums = small_total(4)
    self1, cross1 = (unpacked(sums[n : n + 1]) for n in range(2))
    for b in range(2):
        ratio = norm1[b] / norm0[b]
        self_curve = self1[b] + self_dots[b]
        cross_curve = cross1[b] + cross_dots[b]
        curve = self_curve + ratio * (2.0 * cross_curve + ratio * curve0[b])
        alpha = norm1[b] / curve
        weight0.append(alpha0[b] + alpha * ratio)
        weight1.append(alpha)

    with jax.named_scope("density"):
        for p in range(PLANES):
            total = jnp.zeros((GRID, 128), f32)
            for b in range(2):
                lanes = slice(128 * (2 * p + b), 128 * (2 * p + b) + 128)
                total = total + weight0[b] * dens[0:96, lanes] + weight1[b] * dens[96:192, lanes]
            for i in range(nb):
                part_send[i, 12 * p : 12 * p + 12, :] = total[12 * i : 12 * i + 12, :]

    for k in BANDS_FAR:
        part_copy(k).start()
    part_recv[mb] = part_send[mb]
    first_out[...] = direction[...]
    second_out[...] = residual[...]
    for b in range(2):
        weights_out[b : b + 1, :] = jnp.broadcast_to(weight0[b], (1, 128))
        weights_out[2 + b : 3 + b, :] = jnp.broadcast_to(weight1[b], (1, 128))
    weights_out[4:8, :] = jnp.zeros((4, 128), f32)

    for rnd in range(5):
        if rnd != 2:
            ga_all(rnd).wait_send()
        small_all(rnd).wait_send()
    gather_sent(occupied, psi_sem)
    gather_sent(zall, z_sem)
    proj_all().wait_send()
    with jax.named_scope("part_wait"):
        part_all().wait_recv()
    cells_out[...] = jnp.sum(part_recv[...], axis=0)

    part_all().wait_send()


OUTS = tuple(
    pltpu.VMEM(shape, f32) for shape in ((192, 256), (192, 256), (8, 128), (72, 128))
)


def finish(first, second, weights, cells, response, density):
    for c in range(2):
        for b in range(2):
            at, of = slice(96 * c, 96 * c + 96), slice(128 * b, 128 * b + 128)
            response[c, b] = (
                weights[b : b + 1, :] * first[at, of] + weights[2 + b : 3 + b, :] * second[at, of]
            )
    for y in range(12):
        density[:, 96 * y : 96 * y + 96] = cells[pl.ds(y, PLANES, stride=12), :][:, 0:96]


def per_device(psi, vloc, dv, beta, dij, atom_type, stick_xy, band_shift):
    vmem = pl.BlockSpec(memory_space=pltpu.VMEM)
    dma = pltpu.SemaphoreType.DMA
    every = tables()
    early, late = every[:1], every[1:]
    pieces = pl.pallas_call(
        kernel,
        out_shape=OUTS,
        in_specs=[pl.BlockSpec(memory_space=pl.ANY)] * 19,
        out_specs=(vmem,) * 4,
        scratch_shapes=[
            pltpu.SMEM((2,), f32),
            pltpu.SMEM((2, 4, 4), f32),
            pltpu.SMEM((32,), jnp.int32),
            pltpu.VMEM((2, 2, GRID, 128), bf16),
            pltpu.VMEM((GROUPS, 128), jnp.int32),
            *[pltpu.VMEM(t.shape, t.dtype) for t in early],
            pltpu.VMEM((PLANES, GRID * GRID), f32),
            pltpu.VMEM((PLANES, GRID * GRID), f32),
            *[pltpu.VMEM(t.shape, t.dtype) for t in late],
            pltpu.VMEM((2, 128, GRID, 128), f32),
            pltpu.VMEM((GRID, 768), f32),
            pltpu.VMEM((GRID, 768), f32),
            pltpu.VMEM((768, 128), f32),
            pltpu.VMEM((8, 2, 2, GRID, 128), bf16),
            pltpu.VMEM((512, 2048), bf16),
            pltpu.VMEM((8, 2048), f32),
            pltpu.VMEM((5, GROUPS, ROWS, 128), f32),
            pltpu.VMEM((5, GROUPS, ROWS, 128), f32),
            pltpu.VMEM((5, 8, 128), f32),
            pltpu.VMEM((5, GROUPS, 8, 128), f32),
            pltpu.VMEM((8, 72, 128), f32),
            pltpu.VMEM((8, 72, 128), f32),
            pltpu.VMEM((384, 2048), bf16),
            pltpu.VMEM((192, 512), f32),
            pltpu.VMEM((384, 512), f32),
            pltpu.VMEM((384, 512), bf16),
            pltpu.VMEM((384, 512), bf16),
            pltpu.VMEM((128, 1536), bf16),
            pltpu.VMEM((128, 1536), bf16),
            pltpu.VMEM((192, 1536), f32),
            pltpu.VMEM((192, 1536), f32),
            pltpu.VMEM((192, 1536), f32),
            pltpu.VMEM((384, 512), bf16),
            pltpu.VMEM((2, 384, 512), f32),
            pltpu.VMEM((8, GROUPS, ROWS, 128), f32),
            pltpu.VMEM((256, 2048), bf16),
            pltpu.VMEM((256, 2048), bf16),
            pltpu.VMEM((17, 8, 128), f32),
            pltpu.VMEM((4, 128, 128), f32),
            pltpu.VMEM((4, 128, 128), f32),
            pltpu.VMEM((128, 128), f32),
            pltpu.VMEM((2, 192, 256), f32),
            pltpu.VMEM((192, 256), f32),
            pltpu.VMEM((GRID, 128), f32),
            pltpu.VMEM((8, 2048), f32),
            pltpu.VMEM((192, 1536), f32),
            dma((19,)),
            dma((3,)),
            dma((3,)),
            dma((2,)),
            dma((5,)),
            dma((GROUPS,)),
            dma((4,)),
            dma((5,)),
            dma((5,)),
            dma((2,)),
        ],
        compiler_params=pltpu.CompilerParams(
            collective_id=0, has_side_effects=True, vmem_limit_bytes=60 * 1024 * 1024
        ),
    )(
        band_shift, dij, atom_type, psi, stick_xy.reshape(GROUPS, 128), *early,
        vloc, dv, *late, beta,
    )
    return pl.pallas_call(
        finish,
        out_shape=(
            jax.ShapeDtypeStruct((2, 2, GRID, 128), f32),
            jax.ShapeDtypeStruct((PLANES, 12 * GRID), f32),
        ),
        in_specs=[vmem] * 4,
        out_specs=(vmem, vmem),
    )(*(pltpu.with_memory_space_constraint(p, pltpu.VMEM) for p in pieces))


def solution(mesh):
    return jax.shard_map(
        per_device,
        mesh=mesh,
        in_specs=(
            P(None, "band", None, "ga"),
            P("ga", None),
            P("ga", None),
            P(None, None, None, "ga"),
            P(),
            P(),
            P(),
            P("band"),
        ),
        out_specs=(P(None, "band", None, "ga"), P("ga", "band")),
        check_vma=False,
    )
```

```python
import functools
import math

import jax
import jax.numpy as jnp
import numpy as np
from jax import lax
from jax.experimental import pallas as pl
from jax.experimental.pallas import tpu as pltpu
from jax.sharding import PartitionSpec as P

GRID = 96
SIDE = 64
GROUPS = 16
PLANES = 6
ROWS = 24
MESH = pl.DeviceIdType.MESH
f32 = jnp.float32
bf16 = jnp.bfloat16


def complex_table(angle):
    cos, sin = np.cos(angle), np.sin(angle)
    return np.array([[cos, -sin], [sin, cos]]) / math.sqrt(GRID)


def halves(table):
    high = np.asarray(table, np.float32).astype(jnp.bfloat16)
    low = (table - high.astype(np.float64)).astype(jnp.bfloat16)
    return high, low


def tables():
    unit = 2.0 * math.pi / GRID
    cells = np.arange(GRID)
    freqs = np.arange(SIDE) - SIDE // 2
    along_z = complex_table(unit * (cells[:, None] * cells[None, :] % GRID))
    along_z = along_z.reshape(2, 2, GROUPS, PLANES, GRID)
    z_table = np.einsum("oidpk->dopik", along_z).reshape(GROUPS, 12, 2 * GRID)
    z_table = np.concatenate(
        [z_table[:, :8].reshape(128, -1), z_table[:, 8:].reshape(64, -1)], axis=0
    )
    along_x = np.zeros((2, 2, SIDE, 128))
    along_x[..., :GRID] = complex_table(unit * (freqs[:, None] * cells[None, :] % GRID))
    x_table = np.einsum("oikx,be->ibkoex", along_x, np.eye(2)).reshape(256, 512)
    along_y = complex_table(unit * (cells[:, None] * freqs[None, :] % GRID))
    along_y = along_y.reshape(2, 2, GRID, 8, 8)
    y_table = np.einsum("oiygl->oyilg", along_y).reshape(192, 128)
    out = []
    for table in (z_table, z_table.T):
        high, low = halves(np.ascontiguousarray(table))
        out.append(np.concatenate([high, low, high], axis=1))
    for table in (x_table, x_table.T, y_table):
        out.extend(halves(np.ascontiguousarray(table)))
    high, low = halves(np.ascontiguousarray(y_table.T))
    out.append(np.concatenate([high, high, low], axis=1))
    pick = np.zeros((128, 256))
    signs = np.zeros((4, 24, 256))

    def place(index, b):
        return index if b == 0 else (index + 16 if index < 8 else index + 4)

    def enter(out_row, n, col, c_out, c_in):
        if c_out == c_in:
            signs[n, out_row, col] = 1.0
        else:
            signs[2 + n, out_row, col] = 1.0 if c_out else -1.0

    for m in range(16):
        owner, b = m // 2, m % 2
        for c in range(2):
            for p in range(PLANES):
                pick[m, 24 * owner + place(6 * c + p, b)] = 1.0
            pick[m, 192 + 8 * owner + 2 * c + b] = 1.0
            for n in range(2):
                for c_out in range(2):
                    for p in range(PLANES):
                        enter(
                            place(6 * c_out + p, n), n, 24 * owner + place(6 * c + p, b), c_out, c
                        )
                    enter(2 * c_out + n, n, 192 + 8 * owner + 2 * c + b, c_out, c)
    out.append(pick.astype(jnp.bfloat16))
    out.append(signs.reshape(96, 256).astype(np.float32))
    return [jnp.asarray(t) for t in out]


def dot(a, b):
    return lax.dot_general(a, b, (((1,), (0,)), ((), ())), preferred_element_type=f32)


def dot_nt(a, b):
    return lax.dot_general(a, b, (((1,), (1,)), ((), ())), preferred_element_type=f32)


def split(x):
    high = x.astype(bf16)
    return high, (x - high.astype(f32)).astype(bf16)


def deep(table, x):
    xh, xl = split(x)
    return dot(table, jnp.concatenate([xh, xh, xl], axis=0))


def right(ah, al, high, low):
    return dot(
        jnp.concatenate([ah, al, ah], axis=1), jnp.concatenate([high, high, low], axis=0)
    )


def row_sum(x):
    return jnp.sum(jnp.sum(x.reshape(-1, 8, 128), axis=0), axis=0, keepdims=True)


def lane_total(row):
    return jnp.sum(row, axis=1, keepdims=True)


def kernel(
    shift_hbm, dij_hbm, kind_hbm, psi_hbm, sticks_hbm, z3_hbm, vloc_hbm, dv_hbm, zt3_hbm, xh_hbm, xl_hbm, xth_hbm, xtl_hbm,
    yh_hbm, yl_hbm, yt3_hbm, pick_hbm, signs_hbm, beta_hbm,
    first_out, second_out, weights_out, cells_out,
    shift, dij, kind, psi, sticks, z3, vloc_flat, dv_flat, zt3, xh, xl, xth, xtl, yh, yl, yt3, pick, signs,
    beta, vloc, dv, cells, occupied, onehot, mask, send, recv, small_send, small_recv,
    part_send, part_recv, lhs, grid, ex, eh, el, dh, dl, psi_field, field0, field1,
    q, found_all, zall, zbh, zbl, psi_proj, proj, coef, couple, vec, image, kin, own, dens,
    load_sem, psi_sem, z_sem, pp_sem, ssem, rsem, rall, tssem, trsem, part_sem,
):
    me = lax.axis_index("ga")
    mb = lax.axis_index("band")
    nb = 8
    mx, my = me // 4, lax.rem(me, 4)

    def peer(dx, dy):
        return lax.rem(mx + dx, 4) * 4 + lax.rem(my + dy, 4)

    OFFSETS = sorted(
        ((dx, dy) for dx in range(4) for dy in range(4) if dx or dy),
        key=lambda o: -(min(o[0], 4 - o[0]) + min(o[1], 4 - o[1])),
    )
    X_ORDER = (2, 1, 3, 0)
    BANDS_FAR = (4, 5, 3, 2, 6, 7, 1)

    barrier = pltpu.get_barrier_semaphore()

    for offset in OFFSETS:
        pl.semaphore_signal(barrier, inc=1, device_id=(peer(*offset), mb), device_id_type=MESH)
    for k in BANDS_FAR:
        pl.semaphore_signal(
            barrier, inc=1, device_id=(me, lax.rem(mb + k, nb)), device_id_type=MESH
        )
    loads = {}
    pairs = dict(
        psi=(psi_hbm, psi), z3=(z3_hbm, z3), sticks=(sticks_hbm, sticks),
        kind=(kind_hbm, kind), dij=(dij_hbm, dij), shift=(shift_hbm, shift),
        dv=(dv_hbm, dv_flat), xh=(xh_hbm, xh), xl=(xl_hbm, xl), yh=(yh_hbm, yh),
        yl=(yl_hbm, yl), yt3=(yt3_hbm, yt3), xth=(xth_hbm, xth), xtl=(xtl_hbm, xtl),
        zt3=(zt3_hbm, zt3), pick=(pick_hbm, pick), signs=(signs_hbm, signs), vloc=(vloc_hbm, vloc_flat),
        beta=(beta_hbm, beta),
    )
    for at, (name, (source, target)) in enumerate(pairs.items()):
        loads[name] = pltpu.make_async_copy(source, target, load_sem.at[at])
        loads[name].start()

    def came(rnd, owner):
        return rsem.at[owner] if rnd == 0 else rall.at[rnd - 1]

    def copy(source, target, gone, landed, where):
        return pltpu.make_async_remote_copy(
            src_ref=source, dst_ref=target, send_sem=gone, recv_sem=landed,
            device_id=where, device_id_type=MESH,
        )

    def ga_copy(rnd, other):
        return copy(
            send.at[rnd, other], recv.at[rnd, me], ssem.at[rnd], came(rnd, me), (other, mb)
        )

    def ga_landed(rnd, other):
        return copy(
            send.at[rnd, other], recv.at[rnd, other], ssem.at[rnd], came(rnd, other), (other, mb)
        )

    others = pl.ds(0, GROUPS - 1)
    right_of = (lax.rem(me + 1, GROUPS), mb)

    def ga_all(rnd):
        return copy(
            send.at[rnd, others], recv.at[rnd, others], ssem.at[rnd], came(rnd, 0), right_of
        )

    def exchange(rnd):
        for offset in OFFSETS:
            ga_copy(rnd, peer(*offset)).start()
        recv[rnd, me] = send[rnd, me]

    @jax.named_scope("arrived")
    def arrived(rnd):
        ga_all(rnd).wait_recv()

    def small_exchange(rnd):
        for offset in OFFSETS:
            copy(
                small_send.at[rnd], small_recv.at[rnd, me], tssem.at[rnd], trsem.at[rnd],
                (peer(*offset), mb),
            ).start()
        small_recv[rnd, me] = small_send[rnd]

    def small_all(rnd):
        landed = small_recv.at[rnd, others]
        return copy(landed, landed, tssem.at[rnd], trsem.at[rnd], right_of)

    def small_total(rnd):
        with jax.named_scope("small_wait"):
            small_all(rnd).wait_recv()
        return jnp.sum(small_recv[rnd], axis=0)

    mz, mc = mb // 2, lax.rem(mb, 2)
    partner = mz * 2 + 1 - mc

    def alike(dz):
        return lax.rem(mz + dz, 4) * 2 + mc

    def gather_out(block, slot, sems):
        for dz in (2, 1, 3):
            copy(block, slot, sems.at[0], sems.at[1], (me, alike(dz))).start()
        copy(block, slot, sems.at[0], sems.at[2], (me, partner)).start()

    def gather_bytes(count, held, sems, which):
        some = held.at[pl.ds(0, count)]
        return copy(some, some, sems.at[0], sems.at[which], (me, partner))

    def gather_on(held, sems):
        gather_bytes(3, held, sems, 1).wait_recv()
        for dz in (1, 3, 2):
            slot = held.at[alike(dz)]
            copy(slot, slot, sems.at[0], sems.at[2], (me, partner)).start()

    def gather_done(held, sems):
        gather_bytes(4, held, sems, 2).wait_recv()

    def gather_sent(held, sems):
        gather_bytes(7, held, sems, 1).wait_send()

    rest = pl.ds(0, nb - 1)
    after = (me, lax.rem(mb + 1, nb))

    def proj_copy(k):
        where = (me, lax.rem(mb + k, nb))
        return copy(psi_proj.at[16], psi_proj.at[8 + mb], pp_sem.at[0], pp_sem.at[1], where)

    def proj_all():
        some = psi_proj.at[rest]
        return copy(some, some, pp_sem.at[0], pp_sem.at[1], after)

    def part_copy(k):
        other = lax.rem(mb + k, nb)
        return copy(
            part_send.at[other], part_recv.at[mb], part_sem.at[0], part_sem.at[1], (me, other)
        )

    def part_all():
        return copy(part_send.at[rest], part_recv.at[rest], part_sem.at[0], part_sem.at[1], after)

    def dealt(rnd, planes):
        for d in range(GROUPS):
            head = planes[8 * d : 8 * d + 8]
            tail = planes[128 + 4 * d : 132 + 4 * d]
            send[rnd, d, 0:8] = head[:, 0:128]
            send[rnd, d, 8:16] = jnp.concatenate([tail[:, 0:128], tail[:, 128:256]], axis=0)
            send[rnd, d, 16:24] = head[:, 128:256]

    def collected(rnd):
        rows = [
            jnp.concatenate([recv[rnd, d, 0:8], recv[rnd, d, 16:24]], axis=1)
            for d in range(GROUPS)
        ]
        for d in range(0, GROUPS, 2):
            even, odd = recv[rnd, d, 8:16], recv[rnd, d + 1, 8:16]
            rows.append(
                jnp.concatenate(
                    [
                        jnp.concatenate([even[0:4], odd[0:4]], axis=0),
                        jnp.concatenate([even[4:8], odd[4:8]], axis=0),
                    ],
                    axis=1,
                )
            )
        return jnp.concatenate(rows, axis=0)

    for name in ("psi", "z3"):
        loads[name].wait()
    with jax.named_scope("z_psi"):
        wide = jnp.concatenate(
            [jnp.concatenate([psi[c, 0], psi[c, 1]], axis=1) for c in range(2)], axis=0
        )
        dealt(0, dot(z3[:, 0:384], jnp.concatenate([wide, wide], axis=0)))

    def places(xy):
        flat = xy.astype(f32)
        y = jnp.floor((flat + 0.5) * (1.0 / GRID))
        x = flat - GRID * y
        fy = jnp.where(y >= GRID // 2, y - GRID, y)
        fx = jnp.where(x >= GRID // 2, x - GRID, x)
        return fy, fx

    loads["sticks"].wait()
    with jax.named_scope("tables"):
        fy, fx = places(sticks[...])
        ky = fy + SIDE // 2
        kx = fx + SIDE // 2
        high = jnp.floor(ky * 0.125)
        low = (ky - 8.0 * high) * SIDE + kx
        for k in range(GROUPS):
            own[0:1, 128 * k : 128 * k + 128] = low[k : k + 1, :]
            own[1:2, 128 * k : 128 * k + 128] = high[k : k + 1, :]
        mask[...] = (
            lax.broadcasted_iota(jnp.int32, (8, 2048), 0).astype(f32) == own[1:2, :]
        ).astype(f32)

        def fill(k, c):
            lanes = pl.ds(pl.multiple_of(k * 256, 256), 256)
            ids = lax.broadcasted_iota(jnp.int32, (512, 256), 0).astype(f32)
            onehot[:, lanes] = (ids == own[0:1, lanes]).astype(f32).astype(bf16)
            return c

        lax.fori_loop(0, 8, fill, 0)
        oy, ox = places(sticks[pl.ds(me, 1), :])
        kz = lax.broadcasted_iota(jnp.int32, (GRID, 128), 0).astype(f32)
        fz = jnp.where(kz >= GRID // 2, kz - GRID, kz)
        kin[...] = (fz * fz + (oy * oy + ox * ox)) * (4.0 / (GRID * GRID))

    row = lax.broadcasted_iota(jnp.int32, (128, 128), 0)
    lane = lax.broadcasted_iota(jnp.int32, (128, 128), 1)

    def couple_all():
        atom = lax.broadcasted_iota(jnp.int32, (1, 128), 1) // 4
        kinds = jnp.zeros((1, 128), jnp.int32)
        for a in range(32):
            kinds = jnp.where(atom == a, kind[a], kinds)
        same = (row // 4) == (lane // 4)
        first = kinds == 0
        total = jnp.zeros((128, 128), f32)
        for i in range(4):
            for k in range(4):
                value = jnp.where(first, dij[0, i, k], dij[1, i, k])
                here = same & ((row % 4) == i) & ((lane % 4) == k)
                total = total + jnp.where(here, value, 0.0)
        couple[...] = total

    def unpack(flat, out):
        def body(g, c):
            piece = flat[:, pl.ds(pl.multiple_of(g * 384, 384), 384)]
            tail = jnp.zeros((PLANES, 32), f32)
            for r in range(4):
                if r < 3:
                    cut = piece[:, 96 * r : 96 * r + 128]
                else:
                    cut = jnp.concatenate([piece[:, 288:384], tail], axis=1)
                cells[pl.ds(pl.multiple_of(g * 32, 32) + 8 * r, PLANES), :] = cut
            return c

        lax.fori_loop(0, 24, body, 0)
        for p in range(PLANES):
            out[:, 128 * p : 128 * p + 128] = cells[pl.ds(p, GRID, stride=8), :]

    for name in ("kind", "dij", "shift"):
        loads[name].wait()
    with jax.named_scope("couple"):
        couple_all()
    with jax.named_scope("unpack"):
        loads["dv"].wait()
        unpack(dv_flat, dv)
    zbh[192:256, :] = jnp.zeros((64, 2048), bf16)
    zbl[192:256, :] = jnp.zeros((64, 2048), bf16)
    psi_proj[0:8] = jnp.zeros((8, 8, 128), f32)
    psi_proj[16] = jnp.zeros((8, 128), f32)
    vec[0] = wide.astype(f32)
    with jax.named_scope("barrier"):
        pl.semaphore_wait(barrier, GROUPS - 1 + nb - 1)
    exchange(0)

    gather_out(psi, occupied.at[mb], psi_sem)
    occupied[mb] = psi[...]
    for name in ("xh", "xl", "yh", "yl", "yt3", "xth", "xtl", "zt3", "pick", "signs"):
        loads[name].wait()
    ones = jnp.ones((256, 128), bf16)

    def fill_planes(rnd, out):

        def laid(src):
            piece = recv[rnd, src]
            upper = piece.astype(bf16).astype(f32)
            lower = piece - upper
            cols = pl.ds(pl.multiple_of(src * 128, 128) if rnd == 0 else src * 128, 128)
            keep = mask[:, cols]
            for n, part in enumerate((upper, lower)):
                for index in range(12):
                    pair = (index, index + 16 if index < 8 else index + 4)
                    two = [jnp.broadcast_to(part[r : r + 1], (8, 128)) * keep for r in pair]
                    at = 192 * n + 16 * index
                    lhs[at : at + 16, cols] = jnp.concatenate(two, axis=0).astype(bf16)

        def body(k, c):
            src = lax.rem(me + k, GROUPS)

            @pl.when(k > 0)
            def _():
                ga_landed(rnd, src).wait_recv()

            laid(src)
            return c

        with jax.named_scope("fill_lhs"):
            if rnd == 0:
                lax.fori_loop(0, GROUPS, body, 0)
                gather_out(recv.at[0], zall.at[mb], z_sem)
                zall[mb] = recv[0]
            elif rnd != 2:
                arrived(rnd)
        if rnd:
            for src in range(GROUPS):
                laid(src)
        with jax.named_scope("fill_dot"):
            both = dot_nt(lhs[...], onehot[...])
            grid[...] = both[0:192] + both[192:384]
        with jax.named_scope("fill_x"):
            data = [
                jnp.concatenate(
                    [grid[0:96, 128 * t : 128 * t + 128], grid[96:192, 128 * t : 128 * t + 128]],
                    axis=1,
                )
                for t in range(4)
            ]
            ah, al = split(jnp.concatenate(data, axis=0))
            ex[...] = right(ah, al, xh[...], xl[...])
            for c in range(2):
                for t in range(4):
                    rows = slice(16 * (4 * c + t), 16 * (4 * c + t) + 16)
                    for i in range(12):
                        at = 96 * t + 8 * i
                        two = [ex[at : at + 8, 128 * (2 * c + j) : 128 * (2 * c + j) + 128] for j in (0, 1)]
                        uh, ul = split(jnp.concatenate(two, axis=0))
                        dh[rows, 128 * i : 128 * i + 128] = uh
                        dl[rows, 128 * i : 128 * i + 128] = ul
        with jax.named_scope("fill_y"):
            for part in range(6):
                lanes = slice(256 * part, 256 * part + 256)
                out[:, lanes] = dot(
                    jnp.concatenate([yh[...], yh[...], yl[...]], axis=1),
                    jnp.concatenate([dh[:, lanes], dl[:, lanes], dh[:, lanes]], axis=0),
                )

    def to_sticks(rnd, potential, source, between=None):
        with jax.named_scope("stick_y"):
            for p in range(PLANES):
                lanes = slice(256 * p, 256 * p + 256)
                pot = potential[:, 128 * p : 128 * p + 128]
                pot = jnp.concatenate([pot, pot], axis=1)
                pot = jnp.concatenate([pot, pot], axis=0)
                ah, al = split(source[:, lanes] * pot)
                along = dot(yt3[...], jnp.concatenate([ah, al, ah], axis=0))
                for c in range(2):
                    for t in range(4):
                        for j in range(2):
                            rows = slice(8 * (8 * c + 2 * t + j), 8 * (8 * c + 2 * t + j) + 8)
                            two = jnp.concatenate([along[rows, 0:128], along[rows, 128:256]], axis=0)
                            uh, ul = split(two)
                            at = 96 * t + 16 * p
                            cols = slice(128 * (2 * c + j), 128 * (2 * c + j) + 128)
                            eh[at : at + 16, cols] = uh
                            el[at : at + 16, cols] = ul
        with jax.named_scope("stick_x"):
            along = right(eh[...], el[...], xth[...], xtl[...])
            for r in range(0, ROWS, 2):
                if r < 12:
                    index, b = r, 0
                else:
                    index, b = (r - 4, 1) if r < 16 else (r - 16, 1)
                for t in range(4):
                    two = []
                    for n in (index, index + 1):
                        at = 96 * t + 8 * (2 * (n % PLANES) + b)
                        col = 128 * (n // PLANES)
                        two.append(along[at : at + 8, col : col + 128])
                    uh, ul = split(jnp.concatenate(two, axis=0))
                    lanes = slice(128 * t, 128 * t + 128)
                    q[8 * r : 8 * r + 16, lanes] = uh
                    q[192 + 8 * r : 208 + 8 * r, lanes] = ul

        if between is not None:
            between()
        with jax.named_scope("stick_pick"):
            for k in range(6):
                if k > 1:
                    dx = X_ORDER[k - 2]
                    for dy in (2, 1, 3, 0):
                        if dx or dy:
                            ga_copy(rnd, peer(dx, dy)).start()
                if k < 4:
                    quad = lax.rem(mx + X_ORDER[k], 4)
                    lanes = pl.ds(pl.multiple_of(quad * 512, 512), 512)
                    found_all[k % 2] = dot(q[...], onehot[:, lanes])
                if 0 < k < 5:
                    quad = lax.rem(mx + X_ORDER[k - 1], 4)
                    lanes = pl.ds(pl.multiple_of(quad * 512, 512), 512)
                    both = found_all[(k - 1) % 2, 0:192] + found_all[(k - 1) % 2, 192:384]
                    picked = jnp.sum(both.reshape(ROWS, 8, 512) * mask[:, lanes][None], axis=1)
                    for n in range(4):
                        send[rnd, 4 * quad + n] = picked[:, 128 * n : 128 * n + 128]
            recv[rnd, me] = send[rnd, me]

    def z_forward(rnd):
        return deep(zt3[...], collected(rnd))

    def project(load, count, source, begin=0):
        step = 8

        def body(g, c):
            sums = [[None] * 4 for _ in range(step)]
            for z in range(GRID // 8):
                v = [
                    source[96 * c + 8 * z : 96 * c + 8 * z + 8, 128 * b : 128 * b + 128]
                    for c in range(2)
                    for b in range(2)
                ]
                for t in range(step):
                    p0, p1 = load(g * step + t, 8 * z, 8)
                    for b in range(2):
                        re = p0 * v[b] + p1 * v[2 + b]
                        im = p0 * v[2 + b] - p1 * v[b]
                        sums[t][b] = re if z == 0 else sums[t][b] + re
                        sums[t][2 + b] = im if z == 0 else sums[t][2 + b] + im
            for t in range(step):
                for o in range(4):
                    proj[o, pl.ds(g * step + t, 1), :] = jnp.sum(
                        sums[t][o], axis=0, keepdims=True
                    )
            return c

        with jax.named_scope("project"):
            lax.fori_loop(begin // step, count // step, body, 0)

    def projections(o, count):
        ph, pl_ = split(proj[o, 0:count, :])
        one = jnp.ones((8, 128), bf16)
        return dot_nt(
            jnp.concatenate([one, one], axis=1), jnp.concatenate([ph, pl_], axis=1)
        )[0:1, :]

    def spread(matrix, values):
        count = matrix.shape[0]
        for o in range(4):
            mh, ml = split(matrix * values[o : o + 1, :])
            coef[o, 0:count, :] = dot(jnp.concatenate([mh, ml], axis=1), ones)

    def apply(load, count, base):
        rows = 24
        for z in range(GRID // rows):

            def body(g, acc):
                for t in range(4):
                    j = g * 4 + t
                    p0, p1 = load(j, z * rows, rows)
                    out = []
                    for b in range(2):
                        cr = coef[b, pl.ds(j, 1), :]
                        ci = coef[2 + b, pl.ds(j, 1), :]
                        out.append(acc[2 * b] + (p0 * cr - p1 * ci))
                        out.append(acc[2 * b + 1] + (p0 * ci + p1 * cr))
                    acc = out
                return tuple(acc)

            init = tuple(
                base[96 * c + z * rows : 96 * c + z * rows + rows, 128 * b : 128 * b + 128]
                for b in range(2)
                for c in range(2)
            )
            with jax.named_scope("apply"):
                done = lax.fori_loop(0, count // 4, body, init)
            for b in range(2):
                for c in range(2):
                    at = 96 * c + z * rows
                    image[at : at + rows, 128 * b : 128 * b + 128] = done[2 * b + c]

    def beta_rows(j, at=0, rows=GRID):
        return beta[0, j, at : at + rows, :], beta[1, j, at : at + rows, :]

    def psi_rows(m, at=0, rows=GRID):
        owner, b = m // 2, m % 2
        return (
            occupied[owner, 0, b, at : at + rows, :].astype(f32),
            occupied[owner, 1, b, at : at + rows, :].astype(f32),
        )

    with jax.named_scope("unpack"):
        loads["vloc"].wait()
        unpack(vloc_flat, vloc)
    loads["beta"].wait()
    project(beta_rows, 16, vec.at[0])
    fill_planes(0, psi_field)
    to_sticks(1, dv, psi_field)
    project(beta_rows, 80, vec.at[0], 16)
    with jax.named_scope("pass_psi"):
        gather_on(occupied, psi_sem)
    project(beta_rows, 128, vec.at[0], 80)
    for o in range(4):
        psi_proj[16, o : o + 1, :] = projections(o, 128)
    for k in BANDS_FAR:
        proj_copy(k).start()
    psi_proj[8 + mb] = psi_proj[16]
    arrived(1)
    vec[1] = z_forward(1)
    gather_done(occupied, psi_sem)

    project(psi_rows, 16, vec.at[1])
    small_send[0] = jnp.zeros((8, 128), f32)
    for o in range(4):
        small_send[0, o : o + 1, 0:16] = projections(o, 16)
    small_exchange(0)
    project(beta_rows, 64, vec.at[1])
    with jax.named_scope("pass_z"):
        gather_on(zall, z_sem)
    project(beta_rows, 128, vec.at[1], 64)
    image_proj = [projections(o, 128) for o in range(4)]
    proj_all().wait_recv()
    with jax.named_scope("z_wait"):
        gather_done(zall, z_sem)

    def halve(src, c):
        lanes = pl.ds(pl.multiple_of(src * 128, 128), 128)
        for e in range(4):
            both = jnp.concatenate([zall[2 * e, src], zall[2 * e + 1, src]], axis=0)
            uh, ul = split(both)
            zbh[48 * e : 48 * e + 48, lanes] = uh
            zbl[48 * e : 48 * e + 48, lanes] = ul
        return c

    with jax.named_scope("halve"):
        lax.fori_loop(0, GROUPS, halve, 0, unroll=4)
    found = small_total(0) * (1.0 / (2.0 * GRID * 2048))
    with jax.named_scope("enter"):
        fh, fl = split(found)
        laid_out = dot(
            jnp.concatenate([fh, fl], axis=1), jnp.concatenate([pick[...], pick[...]], axis=0)
        )
        entry = jnp.zeros((24, 256), f32)
        for o in range(4):
            entry = entry + signs[24 * o : 24 * o + 24, :] * laid_out[o : o + 1, :]
        nh, nl = split(entry[0:8, 128:256])
        ph, plow = split(psi_proj[0:16].reshape(128, 128))
        joined = dot(
            jnp.concatenate([nh, nl, nh], axis=1), jnp.concatenate([ph, ph, plow], axis=0)
        )
        small_send[1] = jnp.zeros((8, 128), f32)
        for o in range(4):
            small_send[1, o : o + 1, :] = joined[o : o + 1, :] - image_proj[o]
        small_exchange(1)
        mh, ml = split(entry)
        weights = jnp.concatenate([mh, ml, mh], axis=1)
        for part in range(4):
            lanes = slice(512 * part, 512 * part + 512)
            planes = dot(
                weights,
                jnp.concatenate([zbh[:, lanes], zbh[:, lanes], zbl[:, lanes]], axis=0),
            )
            for n in range(4):
                src = 4 * part + n
                recv[2, src] = planes[:, 128 * n : 128 * n + 128] - send[1, src]

    def transform_out(rnd, source):
        dealt(rnd, deep(z3[...], source[...]))
        exchange(rnd)

    def stick_sum(a, b, weight=None):
        out = []
        for n in range(2):
            at = slice(128 * n, 128 * n + 128)
            both = a[0:96, at] * b[0:96, at] + a[96:192, at] * b[96:192, at]
            if weight is not None:
                both = both * (kin[...] + shift[n])
            out.append(row_sum(both))
        return out

    def grid_sum(a, b):
        out = []
        for n in range(2):
            total = jnp.zeros((1, 128), f32)
            for p in range(PLANES):
                lanes = slice(128 * (2 * p + n), 128 * (2 * p + n) + 128)
                pot = vloc[:, 128 * p : 128 * p + 128]
                both = a[0:96, lanes] * b[0:96, lanes] + a[96:192, lanes] * b[96:192, lanes]
                total = total + row_sum(both * pot)
            out.append(total)
        return out

    half = lax.broadcasted_iota(jnp.int32, (1, 128), 1) < 64

    def packed(pair):
        a, b = (r + pltpu.roll(r, 64, 1) for r in pair)
        return jnp.where(half, a, b)

    def unpacked(both):
        return [
            lane_total(jnp.where(half, both, 0.0)),
            lane_total(jnp.where(half, 0.0, both)),
        ]

    def band_dots(values, coupled):
        both = values * coupled
        return [lane_total(both[b : b + 1] + both[2 + b : 3 + b]) for b in range(2)]

    ch, cl = split(couple[...])

    def coupled_rows(values):
        vh, vl = split(values)
        return dot_nt(
            jnp.concatenate([vh, vl, vh], axis=1), jnp.concatenate([ch, ch, cl], axis=1)
        )

    direction = vec.at[0]
    fill_planes(2, field0)
    local = grid_sum(field0, field0)

    def rhs():
        with jax.named_scope("rhs"):
            eye = (row[0:16] == lane[0:16]).astype(f32)
            spread(eye, found)
            vec[1] = -vec[1]
            apply(psi_rows, 16, vec.at[1])
            vec[0] = image[...]
            curves = stick_sum(direction, direction, True)
            small_send[3] = jnp.zeros((8, 128), f32)
            small_send[3, 0:1, :] = packed([curves[b] + local[b] for b in range(2)])
            small_send[3, 1:2, :] = packed(stick_sum(direction, direction))
            small_exchange(3)

    to_sticks(3, vloc, field0, rhs)
    sums = small_total(1)
    values0 = sums[0:4]
    coupled0 = coupled_rows(sums)[0:4]
    nonlocal0 = band_dots(values0, coupled0)
    spread(couple[...], values0)
    for c in range(2):
        for b in range(2):
            at, of = slice(96 * c, 96 * c + 96), slice(128 * b, 128 * b + 128)
            vec[1, at, of] = direction[at, of] * (kin[...] + shift[b])
    apply(beta_rows, 128, vec.at[1])
    sums = small_total(3)
    norm0 = unpacked(sums[1:2])
    curve0 = [c + n for c, n in zip(unpacked(sums[0:1]), nonlocal0)]
    alpha0 = [norm0[b] / curve0[b] for b in range(2)]
    arrived(3)
    image[...] += z_forward(3)
    residual = vec.at[1]
    for c in range(2):
        for b in range(2):
            at, of = slice(96 * c, 96 * c + 96), slice(128 * b, 128 * b + 128)
            residual[at, of] = direction[at, of] - alpha0[b] * image[at, of]

    transform_out(4, residual)
    project(beta_rows, 128, residual)
    small_send[2] = jnp.zeros((8, 128), f32)
    for o in range(4):
        small_send[2, o : o + 1, :] = projections(o, 128)
    small_send[2, 4:5, :] = packed(stick_sum(residual, residual))
    small_exchange(2)
    selfs = stick_sum(residual, residual, True)
    crosses = stick_sum(residual, direction, True)
    fill_planes(4, field1)
    self_local = grid_sum(field1, field1)
    cross_local = grid_sum(field1, field0)
    small_send[4] = jnp.zeros((8, 128), f32)
    small_send[4, 0:1, :] = packed([selfs[b] + self_local[b] for b in range(2)])
    small_send[4, 1:2, :] = packed([crosses[b] + cross_local[b] for b in range(2)])
    small_exchange(4)
    with jax.named_scope("products"):
        for p in range(PLANES):
            for b in range(2):
                lanes = slice(128 * (2 * p + b), 128 * (2 * p + b) + 128)
                for n, field in enumerate((field0, field1)):
                    dens[96 * n : 96 * n + 96, lanes] = 4.0 * (
                        psi_field[0:96, lanes] * field[0:96, lanes]
                        + psi_field[96:192, lanes] * field[96:192, lanes]
                    )
    sums = small_total(2)
    values1 = sums[0:4]
    coupled1 = coupled_rows(sums)[0:4]
    self_dots = band_dots(values1, coupled1)
    cross_dots = band_dots(values1, coupled0)
    weight0, weight1 = [], []
    norm1 = unpacked(sums[4:5])
    sums = small_total(4)
    self1, cross1 = (unpacked(sums[n : n + 1]) for n in range(2))
    for b in range(2):
        ratio = norm1[b] / norm0[b]
        self_curve = self1[b] + self_dots[b]
        cross_curve = cross1[b] + cross_dots[b]
        curve = self_curve + ratio * (2.0 * cross_curve + ratio * curve0[b])
        alpha = norm1[b] / curve
        weight0.append(alpha0[b] + alpha * ratio)
        weight1.append(alpha)

    with jax.named_scope("density"):
        for p in range(PLANES):
            total = jnp.zeros((GRID, 128), f32)
            for b in range(2):
                lanes = slice(128 * (2 * p + b), 128 * (2 * p + b) + 128)
                total = total + weight0[b] * dens[0:96, lanes] + weight1[b] * dens[96:192, lanes]
            for i in range(nb):
                part_send[i, 12 * p : 12 * p + 12, :] = total[12 * i : 12 * i + 12, :]

    for k in BANDS_FAR:
        part_copy(k).start()
    part_recv[mb] = part_send[mb]
    first_out[...] = direction[...]
    second_out[...] = residual[...]
    for b in range(2):
        weights_out[b : b + 1, :] = jnp.broadcast_to(weight0[b], (1, 128))
        weights_out[2 + b : 3 + b, :] = jnp.broadcast_to(weight1[b], (1, 128))
    weights_out[4:8, :] = jnp.zeros((4, 128), f32)

    for rnd in range(5):
        if rnd != 2:
            ga_all(rnd).wait_send()
        small_all(rnd).wait_send()
    gather_sent(occupied, psi_sem)
    gather_sent(zall, z_sem)
    proj_all().wait_send()
    with jax.named_scope("part_wait"):
        part_all().wait_recv()
    cells_out[...] = jnp.sum(part_recv[...], axis=0)

    part_all().wait_send()


OUTS = tuple(
    pltpu.VMEM(shape, f32) for shape in ((192, 256), (192, 256), (8, 128), (72, 128))
)


def finish(first, second, weights, cells, response, density):
    for c in range(2):
        for b in range(2):
            at, of = slice(96 * c, 96 * c + 96), slice(128 * b, 128 * b + 128)
            response[c, b] = (
                weights[b : b + 1, :] * first[at, of] + weights[2 + b : 3 + b, :] * second[at, of]
            )
    for y in range(12):
        density[:, 96 * y : 96 * y + 96] = cells[pl.ds(y, PLANES, stride=12), :][:, 0:96]


def per_device(psi, vloc, dv, beta, dij, atom_type, stick_xy, band_shift):
    vmem = pl.BlockSpec(memory_space=pltpu.VMEM)
    dma = pltpu.SemaphoreType.DMA
    every = tables()
    early, late = every[:1], every[1:]
    pieces = pl.pallas_call(
        kernel,
        out_shape=OUTS,
        in_specs=[pl.BlockSpec(memory_space=pl.ANY)] * 19,
        out_specs=(vmem,) * 4,
        scratch_shapes=[
            pltpu.SMEM((2,), f32),
            pltpu.SMEM((2, 4, 4), f32),
            pltpu.SMEM((32,), jnp.int32),
            pltpu.VMEM((2, 2, GRID, 128), bf16),
            pltpu.VMEM((GROUPS, 128), jnp.int32),
            *[pltpu.VMEM(t.shape, t.dtype) for t in early],
            pltpu.VMEM((PLANES, GRID * GRID), f32),
            pltpu.VMEM((PLANES, GRID * GRID), f32),
            *[pltpu.VMEM(t.shape, t.dtype) for t in late],
            pltpu.VMEM((2, 128, GRID, 128), f32),
            pltpu.VMEM((GRID, 768), f32),
            pltpu.VMEM((GRID, 768), f32),
            pltpu.VMEM((768, 128), f32),
            pltpu.VMEM((8, 2, 2, GRID, 128), bf16),
            pltpu.VMEM((512, 2048), bf16),
            pltpu.VMEM((8, 2048), f32),
            pltpu.VMEM((5, GROUPS, ROWS, 128), f32),
            pltpu.VMEM((5, GROUPS, ROWS, 128), f32),
            pltpu.VMEM((5, 8, 128), f32),
            pltpu.VMEM((5, GROUPS, 8, 128), f32),
            pltpu.VMEM((8, 72, 128), f32),
            pltpu.VMEM((8, 72, 128), f32),
            pltpu.VMEM((384, 2048), bf16),
            pltpu.VMEM((192, 512), f32),
            pltpu.VMEM((384, 512), f32),
            pltpu.VMEM((384, 512), bf16),
            pltpu.VMEM((384, 512), bf16),
            pltpu.VMEM((128, 1536), bf16),
            pltpu.VMEM((128, 1536), bf16),
            pltpu.VMEM((192, 1536), f32),
            pltpu.VMEM((192, 1536), f32),
            pltpu.VMEM((192, 1536), f32),
            pltpu.VMEM((384, 512), bf16),
            pltpu.VMEM((2, 384, 512), f32),
            pltpu.VMEM((8, GROUPS, ROWS, 128), f32),
            pltpu.VMEM((256, 2048), bf16),
            pltpu.VMEM((256, 2048), bf16),
            pltpu.VMEM((17, 8, 128), f32),
            pltpu.VMEM((4, 128, 128), f32),
            pltpu.VMEM((4, 128, 128), f32),
            pltpu.VMEM((128, 128), f32),
            pltpu.VMEM((2, 192, 256), f32),
            pltpu.VMEM((192, 256), f32),
            pltpu.VMEM((GRID, 128), f32),
            pltpu.VMEM((8, 2048), f32),
            pltpu.VMEM((192, 1536), f32),
            dma((19,)),
            dma((3,)),
            dma((3,)),
            dma((2,)),
            dma((5,)),
            dma((GROUPS,)),
            dma((4,)),
            dma((5,)),
            dma((5,)),
            dma((2,)),
        ],
        compiler_params=pltpu.CompilerParams(
            collective_id=0, has_side_effects=True, vmem_limit_bytes=60 * 1024 * 1024
        ),
    )(
        band_shift, dij, atom_type, psi, stick_xy.reshape(GROUPS, 128), *early,
        vloc, dv, *late, beta,
    )
    return pl.pallas_call(
        finish,
        out_shape=(
            jax.ShapeDtypeStruct((2, 2, GRID, 128), f32),
            jax.ShapeDtypeStruct((PLANES, 12 * GRID), f32),
        ),
        in_specs=[vmem] * 4,
        out_specs=(vmem, vmem),
    )(*(pltpu.with_memory_space_constraint(p, pltpu.VMEM) for p in pieces))


def solution(mesh):
    return jax.shard_map(
        per_device,
        mesh=mesh,
        in_specs=(
            P(None, "band", None, "ga"),
            P("ga", None),
            P("ga", None),
            P(None, None, None, "ga"),
            P(),
            P(),
            P(),
            P("band"),
        ),
        out_specs=(P(None, "band", None, "ga"), P("ga", "band")),
        check_vma=False,
    )
```

```python
import functools
import math

import jax
import jax.numpy as jnp
import numpy as np
from jax import lax
from jax.experimental import pallas as pl
from jax.experimental.pallas import tpu as pltpu
from jax.sharding import PartitionSpec as P

GRID = 96
SIDE = 64
GROUPS = 16
PLANES = 6
ROWS = 24
MESH = pl.DeviceIdType.MESH
f32 = jnp.float32
bf16 = jnp.bfloat16


def complex_table(angle):
    cos, sin = np.cos(angle), np.sin(angle)
    return np.array([[cos, -sin], [sin, cos]]) / math.sqrt(GRID)


def halves(table):
    high = np.asarray(table, np.float32).astype(jnp.bfloat16)
    low = (table - high.astype(np.float64)).astype(jnp.bfloat16)
    return high, low


def tables():
    unit = 2.0 * math.pi / GRID
    cells = np.arange(GRID)
    freqs = np.arange(SIDE) - SIDE // 2
    along_z = complex_table(unit * (cells[:, None] * cells[None, :] % GRID))
    along_z = along_z.reshape(2, 2, GROUPS, PLANES, GRID)
    z_table = np.einsum("oidpk->dopik", along_z).reshape(GROUPS, 12, 2 * GRID)
    z_table = np.concatenate(
        [z_table[:, :8].reshape(128, -1), z_table[:, 8:].reshape(64, -1)], axis=0
    )
    along_x = np.zeros((2, 2, SIDE, 128))
    along_x[..., :GRID] = complex_table(unit * (freqs[:, None] * cells[None, :] % GRID))
    x_table = np.einsum("oikx,be->ibkoex", along_x, np.eye(2)).reshape(256, 512)
    along_y = complex_table(unit * (cells[:, None] * freqs[None, :] % GRID))
    along_y = along_y.reshape(2, 2, GRID, 8, 8)
    y_table = np.einsum("oiygl->oyilg", along_y).reshape(192, 128)
    out = []
    for table in (z_table, z_table.T):
        high, low = halves(np.ascontiguousarray(table))
        out.append(np.concatenate([high, low, high], axis=1))
    for table in (x_table, x_table.T, y_table):
        out.extend(halves(np.ascontiguousarray(table)))
    high, low = halves(np.ascontiguousarray(y_table.T))
    out.append(np.concatenate([high, high, low], axis=1))
    pick = np.zeros((128, 256))
    signs = np.zeros((4, 24, 256))

    def place(index, b):
        return index if b == 0 else (index + 16 if index < 8 else index + 4)

    def enter(out_row, n, col, c_out, c_in):
        if c_out == c_in:
            signs[n, out_row, col] = 1.0
        else:
            signs[2 + n, out_row, col] = 1.0 if c_out else -1.0

    for m in range(16):
        owner, b = m // 2, m % 2
        for c in range(2):
            for p in range(PLANES):
                pick[m, 24 * owner + place(6 * c + p, b)] = 1.0
            pick[m, 192 + 8 * owner + 2 * c + b] = 1.0
            for n in range(2):
                for c_out in range(2):
                    for p in range(PLANES):
                        enter(
                            place(6 * c_out + p, n), n, 24 * owner + place(6 * c + p, b), c_out, c
                        )
                    enter(2 * c_out + n, n, 192 + 8 * owner + 2 * c + b, c_out, c)
    out.append(pick.astype(jnp.bfloat16))
    out.append(signs.reshape(96, 256).astype(np.float32))
    return [jnp.asarray(t) for t in out]


def dot(a, b):
    return lax.dot_general(a, b, (((1,), (0,)), ((), ())), preferred_element_type=f32)


def dot_nt(a, b):
    return lax.dot_general(a, b, (((1,), (1,)), ((), ())), preferred_element_type=f32)


def split(x):
    high = x.astype(bf16)
    return high, (x - high.astype(f32)).astype(bf16)


def deep(table, x):
    xh, xl = split(x)
    return dot(table, jnp.concatenate([xh, xh, xl], axis=0))


def right(ah, al, high, low):
    return dot(
        jnp.concatenate([ah, al, ah], axis=1), jnp.concatenate([high, high, low], axis=0)
    )


def row_sum(x):
    return jnp.sum(jnp.sum(x.reshape(-1, 8, 128), axis=0), axis=0, keepdims=True)


def lane_total(row):
    return jnp.sum(row, axis=1, keepdims=True)


def kernel(
    shift_hbm, dij_hbm, kind_hbm, psi_hbm, sticks_hbm, z3_hbm, vloc_hbm, dv_hbm, zt3_hbm, xh_hbm, xl_hbm, xth_hbm, xtl_hbm,
    yh_hbm, yl_hbm, yt3_hbm, pick_hbm, signs_hbm, beta_hbm,
    first_out, second_out, weights_out, cells_out,
    shift, dij, kind, psi, sticks, z3, vloc_flat, dv_flat, zt3, xh, xl, xth, xtl, yh, yl, yt3, pick, signs,
    beta, vloc, dv, cells, occupied, onehot, mask, send, recv, small_send, small_recv,
    part_send, part_recv, lhs, grid, ex, eh, el, dh, dl, psi_field, field0, field1,
    q, found_all, zall, zbh, zbl, psi_proj, proj, coef, couple, vec, image, kin, own, dens,
    load_sem, psi_sem, z_sem, pp_sem, ssem, rsem, rall, tssem, trsem, part_sem,
):
    me = lax.axis_index("ga")
    mb = lax.axis_index("band")
    nb = 8
    mx, my = me // 4, lax.rem(me, 4)

    def peer(dx, dy):
        return lax.rem(mx + dx, 4) * 4 + lax.rem(my + dy, 4)

    OFFSETS = sorted(
        ((dx, dy) for dx in range(4) for dy in range(4) if dx or dy),
        key=lambda o: -(min(o[0], 4 - o[0]) + min(o[1], 4 - o[1])),
    )
    X_ORDER = (2, 1, 3, 0)
    BANDS_FAR = (4, 5, 3, 2, 6, 7, 1)

    barrier = pltpu.get_barrier_semaphore()

    for offset in OFFSETS:
        pl.semaphore_signal(barrier, inc=1, device_id=(peer(*offset), mb), device_id_type=MESH)
    for k in BANDS_FAR:
        pl.semaphore_signal(
            barrier, inc=1, device_id=(me, lax.rem(mb + k, nb)), device_id_type=MESH
        )
    loads = {}
    pairs = dict(
        psi=(psi_hbm, psi), z3=(z3_hbm, z3), sticks=(sticks_hbm, sticks),
        kind=(kind_hbm, kind), dij=(dij_hbm, dij), shift=(shift_hbm, shift),
        dv=(dv_hbm, dv_flat), xh=(xh_hbm, xh), xl=(xl_hbm, xl), yh=(yh_hbm, yh),
        yl=(yl_hbm, yl), yt3=(yt3_hbm, yt3), xth=(xth_hbm, xth), xtl=(xtl_hbm, xtl),
        zt3=(zt3_hbm, zt3), pick=(pick_hbm, pick), signs=(signs_hbm, signs), vloc=(vloc_hbm, vloc_flat),
        beta=(beta_hbm, beta),
    )
    for at, (name, (source, target)) in enumerate(pairs.items()):
        loads[name] = pltpu.make_async_copy(source, target, load_sem.at[at])
        loads[name].start()

    def came(rnd, owner):
        return rsem.at[owner] if rnd == 0 else rall.at[rnd - 1]

    def copy(source, target, gone, landed, where):
        return pltpu.make_async_remote_copy(
            src_ref=source, dst_ref=target, send_sem=gone, recv_sem=landed,
            device_id=where, device_id_type=MESH,
        )

    def ga_copy(rnd, other):
        return copy(
            send.at[rnd, other], recv.at[rnd, me], ssem.at[rnd], came(rnd, me), (other, mb)
        )

    def ga_landed(rnd, other):
        return copy(
            send.at[rnd, other], recv.at[rnd, other], ssem.at[rnd], came(rnd, other), (other, mb)
        )

    others = pl.ds(0, GROUPS - 1)
    right_of = (lax.rem(me + 1, GROUPS), mb)

    def ga_all(rnd):
        return copy(
            send.at[rnd, others], recv.at[rnd, others], ssem.at[rnd], came(rnd, 0), right_of
        )

    def exchange(rnd):
        for offset in OFFSETS:
            ga_copy(rnd, peer(*offset)).start()
        recv[rnd, me] = send[rnd, me]

    @jax.named_scope("arrived")
    def arrived(rnd):
        ga_all(rnd).wait_recv()

    def small_exchange(rnd):
        for offset in OFFSETS:
            copy(
                small_send.at[rnd], small_recv.at[rnd, me], tssem.at[rnd], trsem.at[rnd],
                (peer(*offset), mb),
            ).start()
        small_recv[rnd, me] = small_send[rnd]

    def small_all(rnd):
        landed = small_recv.at[rnd, others]
        return copy(landed, landed, tssem.at[rnd], trsem.at[rnd], right_of)

    def small_total(rnd):
        with jax.named_scope("small_wait"):
            small_all(rnd).wait_recv()
        return jnp.sum(small_recv[rnd], axis=0)

    mz, mc = mb // 2, lax.rem(mb, 2)
    partner = mz * 2 + 1 - mc

    def alike(dz):
        return lax.rem(mz + dz, 4) * 2 + mc

    def gather_out(block, slot, sems):
        for dz in (2, 1, 3):
            copy(block, slot, sems.at[0], sems.at[1], (me, alike(dz))).start()
        copy(block, slot, sems.at[0], sems.at[2], (me, partner)).start()

    def gather_bytes(count, held, sems, which):
        some = held.at[pl.ds(0, count)]
        return copy(some, some, sems.at[0], sems.at[which], (me, partner))

    def gather_on(held, sems):
        gather_bytes(3, held, sems, 1).wait_recv()
        for dz in (1, 3, 2):
            slot = held.at[alike(dz)]
            copy(slot, slot, sems.at[0], sems.at[2], (me, partner)).start()

    def gather_done(held, sems):
        gather_bytes(4, held, sems, 2).wait_recv()

    def gather_sent(held, sems):
        gather_bytes(7, held, sems, 1).wait_send()

    rest = pl.ds(0, nb - 1)
    after = (me, lax.rem(mb + 1, nb))

    def proj_copy(k):
        where = (me, lax.rem(mb + k, nb))
        return copy(psi_proj.at[16], psi_proj.at[8 + mb], pp_sem.at[0], pp_sem.at[1], where)

    def proj_all():
        some = psi_proj.at[rest]
        return copy(some, some, pp_sem.at[0], pp_sem.at[1], after)

    def part_copy(k):
        other = lax.rem(mb + k, nb)
        return copy(
            part_send.at[other], part_recv.at[mb], part_sem.at[0], part_sem.at[1], (me, other)
        )

    def part_all():
        return copy(part_send.at[rest], part_recv.at[rest], part_sem.at[0], part_sem.at[1], after)

    def dealt(rnd, planes):
        for d in range(GROUPS):
            head = planes[8 * d : 8 * d + 8]
            tail = planes[128 + 4 * d : 132 + 4 * d]
            send[rnd, d, 0:8] = head[:, 0:128]
            send[rnd, d, 8:16] = jnp.concatenate([tail[:, 0:128], tail[:, 128:256]], axis=0)
            send[rnd, d, 16:24] = head[:, 128:256]

    def collected(rnd):
        rows = [
            jnp.concatenate([recv[rnd, d, 0:8], recv[rnd, d, 16:24]], axis=1)
            for d in range(GROUPS)
        ]
        for d in range(0, GROUPS, 2):
            even, odd = recv[rnd, d, 8:16], recv[rnd, d + 1, 8:16]
            rows.append(
                jnp.concatenate(
                    [
                        jnp.concatenate([even[0:4], odd[0:4]], axis=0),
                        jnp.concatenate([even[4:8], odd[4:8]], axis=0),
                    ],
                    axis=1,
                )
            )
        return jnp.concatenate(rows, axis=0)

    for name in ("psi", "z3"):
        loads[name].wait()
    with jax.named_scope("z_psi"):
        wide = jnp.concatenate(
            [jnp.concatenate([psi[c, 0], psi[c, 1]], axis=1) for c in range(2)], axis=0
        )
        dealt(0, dot(z3[:, 0:384], jnp.concatenate([wide, wide], axis=0)))

    def places(xy):
        flat = xy.astype(f32)
        y = jnp.floor((flat + 0.5) * (1.0 / GRID))
        x = flat - GRID * y
        fy = jnp.where(y >= GRID // 2, y - GRID, y)
        fx = jnp.where(x >= GRID // 2, x - GRID, x)
        return fy, fx

    loads["sticks"].wait()
    with jax.named_scope("tables"):
        fy, fx = places(sticks[...])
        ky = fy + SIDE // 2
        kx = fx + SIDE // 2
        high = jnp.floor(ky * 0.125)
        low = (ky - 8.0 * high) * SIDE + kx
        for k in range(GROUPS):
            own[0:1, 128 * k : 128 * k + 128] = low[k : k + 1, :]
            own[1:2, 128 * k : 128 * k + 128] = high[k : k + 1, :]
        mask[...] = (
            lax.broadcasted_iota(jnp.int32, (8, 2048), 0).astype(f32) == own[1:2, :]
        ).astype(f32)

        def fill(k, c):
            lanes = pl.ds(pl.multiple_of(k * 256, 256), 256)
            ids = lax.broadcasted_iota(jnp.int32, (512, 256), 0).astype(f32)
            onehot[:, lanes] = (ids == own[0:1, lanes]).astype(f32).astype(bf16)
            return c

        lax.fori_loop(0, 8, fill, 0)
        oy, ox = places(sticks[pl.ds(me, 1), :])
        kz = lax.broadcasted_iota(jnp.int32, (GRID, 128), 0).astype(f32)
        fz = jnp.where(kz >= GRID // 2, kz - GRID, kz)
        kin[...] = (fz * fz + (oy * oy + ox * ox)) * (4.0 / (GRID * GRID))

    row = lax.broadcasted_iota(jnp.int32, (128, 128), 0)
    lane = lax.broadcasted_iota(jnp.int32, (128, 128), 1)

    def couple_all():
        atom = lax.broadcasted_iota(jnp.int32, (1, 128), 1) // 4
        kinds = jnp.zeros((1, 128), jnp.int32)
        for a in range(32):
            kinds = jnp.where(atom == a, kind[a], kinds)
        same = (row // 4) == (lane // 4)
        first = kinds == 0
        total = jnp.zeros((128, 128), f32)
        for i in range(4):
            for k in range(4):
                value = jnp.where(first, dij[0, i, k], dij[1, i, k])
                here = same & ((row % 4) == i) & ((lane % 4) == k)
                total = total + jnp.where(here, value, 0.0)
        couple[...] = total

    def unpack(flat, out):
        def body(g, c):
            piece = flat[:, pl.ds(pl.multiple_of(g * 384, 384), 384)]
            tail = jnp.zeros((PLANES, 32), f32)
            for r in range(4):
                if r < 3:
                    cut = piece[:, 96 * r : 96 * r + 128]
                else:
                    cut = jnp.concatenate([piece[:, 288:384], tail], axis=1)
                cells[pl.ds(pl.multiple_of(g * 32, 32) + 8 * r, PLANES), :] = cut
            return c

        lax.fori_loop(0, 24, body, 0)
        for p in range(PLANES):
            out[:, 128 * p : 128 * p + 128] = cells[pl.ds(p, GRID, stride=8), :]

    for name in ("kind", "dij", "shift"):
        loads[name].wait()
    with jax.named_scope("couple"):
        couple_all()
    with jax.named_scope("unpack"):
        loads["dv"].wait()
        unpack(dv_flat, dv)
    zbh[192:256, :] = jnp.zeros((64, 2048), bf16)
    zbl[192:256, :] = jnp.zeros((64, 2048), bf16)
    psi_proj[0:8] = jnp.zeros((8, 8, 128), f32)
    psi_proj[16] = jnp.zeros((8, 128), f32)
    vec[0] = wide.astype(f32)
    with jax.named_scope("barrier"):
        pl.semaphore_wait(barrier, GROUPS - 1 + nb - 1)
    exchange(0)

    gather_out(psi, occupied.at[mb], psi_sem)
    occupied[mb] = psi[...]
    for name in ("xh", "xl", "yh", "yl", "yt3", "xth", "xtl", "zt3", "pick", "signs"):
        loads[name].wait()
    ones = jnp.ones((256, 128), bf16)

    def fill_planes(rnd, out):

        def laid(src):
            piece = recv[rnd, src]
            upper = piece.astype(bf16).astype(f32)
            lower = piece - upper
            cols = pl.ds(pl.multiple_of(src * 128, 128) if rnd == 0 else src * 128, 128)
            keep = mask[:, cols]
            for n, part in enumerate((upper, lower)):
                for index in range(12):
                    pair = (index, index + 16 if index < 8 else index + 4)
                    two = [jnp.broadcast_to(part[r : r + 1], (8, 128)) * keep for r in pair]
                    at = 192 * n + 16 * index
                    lhs[at : at + 16, cols] = jnp.concatenate(two, axis=0).astype(bf16)

        def body(k, c):
            src = lax.rem(me + k, GROUPS)

            @pl.when(k > 0)
            def _():
                ga_landed(rnd, src).wait_recv()

            laid(src)
            return c

        with jax.named_scope("fill_lhs"):
            if rnd == 0:
                lax.fori_loop(0, GROUPS, body, 0)
                gather_out(recv.at[0], zall.at[mb], z_sem)
                zall[mb] = recv[0]
            elif rnd != 2:
                arrived(rnd)
        if rnd:
            for src in range(GROUPS):
                laid(src)
        with jax.named_scope("fill_dot"):
            both = dot_nt(lhs[...], onehot[...])
            grid[...] = both[0:192] + both[192:384]
        with jax.named_scope("fill_x"):
            data = [
                jnp.concatenate(
                    [grid[0:96, 128 * t : 128 * t + 128], grid[96:192, 128 * t : 128 * t + 128]],
                    axis=1,
                )
                for t in range(4)
            ]
            ah, al = split(jnp.concatenate(data, axis=0))
            ex[...] = right(ah, al, xh[...], xl[...])
            for c in range(2):
                for t in range(4):
                    rows = slice(16 * (4 * c + t), 16 * (4 * c + t) + 16)
                    for i in range(12):
                        at = 96 * t + 8 * i
                        two = [ex[at : at + 8, 128 * (2 * c + j) : 128 * (2 * c + j) + 128] for j in (0, 1)]
                        uh, ul = split(jnp.concatenate(two, axis=0))
                        dh[rows, 128 * i : 128 * i + 128] = uh
                        dl[rows, 128 * i : 128 * i + 128] = ul
        with jax.named_scope("fill_y"):
            for part in range(6):
                lanes = slice(256 * part, 256 * part + 256)
                out[:, lanes] = dot(
                    jnp.concatenate([yh[...], yh[...], yl[...]], axis=1),
                    jnp.concatenate([dh[:, lanes], dl[:, lanes], dh[:, lanes]], axis=0),
                )

    def to_sticks(rnd, potential, source, between=None):
        with jax.named_scope("stick_y"):
            for p in range(PLANES):
                lanes = slice(256 * p, 256 * p + 256)
                pot = potential[:, 128 * p : 128 * p + 128]
                pot = jnp.concatenate([pot, pot], axis=1)
                pot = jnp.concatenate([pot, pot], axis=0)
                ah, al = split(source[:, lanes] * pot)
                along = dot(yt3[...], jnp.concatenate([ah, al, ah], axis=0))
                for c in range(2):
                    for t in range(4):
                        for j in range(2):
                            rows = slice(8 * (8 * c + 2 * t + j), 8 * (8 * c + 2 * t + j) + 8)
                            two = jnp.concatenate([along[rows, 0:128], along[rows, 128:256]], axis=0)
                            uh, ul = split(two)
                            at = 96 * t + 16 * p
                            cols = slice(128 * (2 * c + j), 128 * (2 * c + j) + 128)
                            eh[at : at + 16, cols] = uh
                            el[at : at + 16, cols] = ul
        with jax.named_scope("stick_x"):
            along = right(eh[...], el[...], xth[...], xtl[...])
            for r in range(0, ROWS, 2):
                if r < 12:
                    index, b = r, 0
                else:
                    index, b = (r - 4, 1) if r < 16 else (r - 16, 1)
                for t in range(4):
                    two = []
                    for n in (index, index + 1):
                        at = 96 * t + 8 * (2 * (n % PLANES) + b)
                        col = 128 * (n // PLANES)
                        two.append(along[at : at + 8, col : col + 128])
                    uh, ul = split(jnp.concatenate(two, axis=0))
                    lanes = slice(128 * t, 128 * t + 128)
                    q[8 * r : 8 * r + 16, lanes] = uh
                    q[192 + 8 * r : 208 + 8 * r, lanes] = ul

        if between is not None:
            between()
        with jax.named_scope("stick_pick"):
            for k in range(6):
                if k > 1:
                    dx = X_ORDER[k - 2]
                    for dy in (2, 1, 3, 0):
                        if dx or dy:
                            ga_copy(rnd, peer(dx, dy)).start()
                if k < 4:
                    quad = lax.rem(mx + X_ORDER[k], 4)
                    lanes = pl.ds(pl.multiple_of(quad * 512, 512), 512)
                    found_all[k % 2] = dot(q[...], onehot[:, lanes])
                if 0 < k < 5:
                    quad = lax.rem(mx + X_ORDER[k - 1], 4)
                    lanes = pl.ds(pl.multiple_of(quad * 512, 512), 512)
                    both = found_all[(k - 1) % 2, 0:192] + found_all[(k - 1) % 2, 192:384]
                    picked = jnp.sum(both.reshape(ROWS, 8, 512) * mask[:, lanes][None], axis=1)
                    for n in range(4):
                        send[rnd, 4 * quad + n] = picked[:, 128 * n : 128 * n + 128]
            recv[rnd, me] = send[rnd, me]

    def z_forward(rnd):
        return deep(zt3[...], collected(rnd))

    def project(load, count, source, begin=0):
        step = 8

        def body(g, c):
            sums = [[None] * 4 for _ in range(step)]
            for z in range(GRID // 8):
                v = [
                    source[96 * c + 8 * z : 96 * c + 8 * z + 8, 128 * b : 128 * b + 128]
                    for c in range(2)
                    for b in range(2)
                ]
                for t in range(step):
                    p0, p1 = load(g * step + t, 8 * z, 8)
                    for b in range(2):
                        re = p0 * v[b] + p1 * v[2 + b]
                        im = p0 * v[2 + b] - p1 * v[b]
                        sums[t][b] = re if z == 0 else sums[t][b] + re
                        sums[t][2 + b] = im if z == 0 else sums[t][2 + b] + im
            for t in range(step):
                for o in range(4):
                    proj[o, pl.ds(g * step + t, 1), :] = jnp.sum(
                        sums[t][o], axis=0, keepdims=True
                    )
            return c

        with jax.named_scope("project"):
            lax.fori_loop(begin // step, count // step, body, 0)

    def projections(o, count):
        ph, pl_ = split(proj[o, 0:count, :])
        one = jnp.ones((8, 128), bf16)
        return dot_nt(
            jnp.concatenate([one, one], axis=1), jnp.concatenate([ph, pl_], axis=1)
        )[0:1, :]

    def spread(matrix, values):
        count = matrix.shape[0]
        for o in range(4):
            mh, ml = split(matrix * values[o : o + 1, :])
            coef[o, 0:count, :] = dot(jnp.concatenate([mh, ml], axis=1), ones)

    def apply(load, count, base):
        rows = 24
        for z in range(GRID // rows):

            def body(g, acc):
                for t in range(8):
                    j = g * 8 + t
                    p0, p1 = load(j, z * rows, rows)
                    out = []
                    for b in range(2):
                        cr = coef[b, pl.ds(j, 1), :]
                        ci = coef[2 + b, pl.ds(j, 1), :]
                        out.append(acc[2 * b] + (p0 * cr - p1 * ci))
                        out.append(acc[2 * b + 1] + (p0 * ci + p1 * cr))
                    acc = out
                return tuple(acc)

            init = tuple(
                base[96 * c + z * rows : 96 * c + z * rows + rows, 128 * b : 128 * b + 128]
                for b in range(2)
                for c in range(2)
            )
            with jax.named_scope("apply"):
                done = lax.fori_loop(0, count // 8, body, init)
            for b in range(2):
                for c in range(2):
                    at = 96 * c + z * rows
                    image[at : at + rows, 128 * b : 128 * b + 128] = done[2 * b + c]

    def beta_rows(j, at=0, rows=GRID):
        return beta[0, j, at : at + rows, :], beta[1, j, at : at + rows, :]

    def psi_rows(m, at=0, rows=GRID):
        owner, b = m // 2, m % 2
        return (
            occupied[owner, 0, b, at : at + rows, :].astype(f32),
            occupied[owner, 1, b, at : at + rows, :].astype(f32),
        )

    with jax.named_scope("unpack"):
        loads["vloc"].wait()
        unpack(vloc_flat, vloc)
    loads["beta"].wait()
    project(beta_rows, 16, vec.at[0])
    fill_planes(0, psi_field)
    to_sticks(1, dv, psi_field)
    project(beta_rows, 80, vec.at[0], 16)
    with jax.named_scope("pass_psi"):
        gather_on(occupied, psi_sem)
    project(beta_rows, 128, vec.at[0], 80)
    for o in range(4):
        psi_proj[16, o : o + 1, :] = projections(o, 128)
    for k in BANDS_FAR:
        proj_copy(k).start()
    psi_proj[8 + mb] = psi_proj[16]
    arrived(1)
    vec[1] = z_forward(1)
    gather_done(occupied, psi_sem)

    project(psi_rows, 16, vec.at[1])
    small_send[0] = jnp.zeros((8, 128), f32)
    for o in range(4):
        small_send[0, o : o + 1, 0:16] = projections(o, 16)
    small_exchange(0)
    project(beta_rows, 64, vec.at[1])
    with jax.named_scope("pass_z"):
        gather_on(zall, z_sem)
    project(beta_rows, 128, vec.at[1], 64)
    image_proj = [projections(o, 128) for o in range(4)]
    proj_all().wait_recv()
    with jax.named_scope("z_wait"):
        gather_done(zall, z_sem)

    def halve(src, c):
        lanes = pl.ds(pl.multiple_of(src * 128, 128), 128)
        for e in range(4):
            both = jnp.concatenate([zall[2 * e, src], zall[2 * e + 1, src]], axis=0)
            uh, ul = split(both)
            zbh[48 * e : 48 * e + 48, lanes] = uh
            zbl[48 * e : 48 * e + 48, lanes] = ul
        return c

    with jax.named_scope("halve"):
        lax.fori_loop(0, GROUPS, halve, 0, unroll=4)
    found = small_total(0) * (1.0 / (2.0 * GRID * 2048))
    with jax.named_scope("enter"):
        fh, fl = split(found)
        laid_out = dot(
            jnp.concatenate([fh, fl], axis=1), jnp.concatenate([pick[...], pick[...]], axis=0)
        )
        entry = jnp.zeros((24, 256), f32)
        for o in range(4):
            entry = entry + signs[24 * o : 24 * o + 24, :] * laid_out[o : o + 1, :]
        nh, nl = split(entry[0:8, 128:256])
        ph, plow = split(psi_proj[0:16].reshape(128, 128))
        joined = dot(
            jnp.concatenate([nh, nl, nh], axis=1), jnp.concatenate([ph, ph, plow], axis=0)
        )
        small_send[1] = jnp.zeros((8, 128), f32)
        for o in range(4):
            small_send[1, o : o + 1, :] = joined[o : o + 1, :] - image_proj[o]
        small_exchange(1)
        mh, ml = split(entry)
        weights = jnp.concatenate([mh, ml, mh], axis=1)
        for part in range(4):
            lanes = slice(512 * part, 512 * part + 512)
            planes = dot(
                weights,
                jnp.concatenate([zbh[:, lanes], zbh[:, lanes], zbl[:, lanes]], axis=0),
            )
            for n in range(4):
                src = 4 * part + n
                recv[2, src] = planes[:, 128 * n : 128 * n + 128] - send[1, src]

    def transform_out(rnd, source):
        dealt(rnd, deep(z3[...], source[...]))
        exchange(rnd)

    def stick_sum(a, b, weight=None):
        out = []
        for n in range(2):
            at = slice(128 * n, 128 * n + 128)
            both = a[0:96, at] * b[0:96, at] + a[96:192, at] * b[96:192, at]
            if weight is not None:
                both = both * (kin[...] + shift[n])
            out.append(row_sum(both))
        return out

    def grid_sum(a, b):
        out = []
        for n in range(2):
            total = jnp.zeros((1, 128), f32)
            for p in range(PLANES):
                lanes = slice(128 * (2 * p + n), 128 * (2 * p + n) + 128)
                pot = vloc[:, 128 * p : 128 * p + 128]
                both = a[0:96, lanes] * b[0:96, lanes] + a[96:192, lanes] * b[96:192, lanes]
                total = total + row_sum(both * pot)
            out.append(total)
        return out

    half = lax.broadcasted_iota(jnp.int32, (1, 128), 1) < 64

    def packed(pair):
        a, b = (r + pltpu.roll(r, 64, 1) for r in pair)
        return jnp.where(half, a, b)

    def unpacked(both):
        return [
            lane_total(jnp.where(half, both, 0.0)),
            lane_total(jnp.where(half, 0.0, both)),
        ]

    def band_dots(values, coupled):
        both = values * coupled
        return [lane_total(both[b : b + 1] + both[2 + b : 3 + b]) for b in range(2)]

    ch, cl = split(couple[...])

    def coupled_rows(values):
        vh, vl = split(values)
        return dot_nt(
            jnp.concatenate([vh, vl, vh], axis=1), jnp.concatenate([ch, ch, cl], axis=1)
        )

    direction = vec.at[0]
    fill_planes(2, field0)
    local = grid_sum(field0, field0)

    def rhs():
        with jax.named_scope("rhs"):
            eye = (row[0:16] == lane[0:16]).astype(f32)
            spread(eye, found)
            vec[1] = -vec[1]
            apply(psi_rows, 16, vec.at[1])
            vec[0] = image[...]
            curves = stick_sum(direction, direction, True)
            small_send[3] = jnp.zeros((8, 128), f32)
            small_send[3, 0:1, :] = packed([curves[b] + local[b] for b in range(2)])
            small_send[3, 1:2, :] = packed(stick_sum(direction, direction))
            small_exchange(3)

    to_sticks(3, vloc, field0, rhs)
    sums = small_total(1)
    values0 = sums[0:4]
    coupled0 = coupled_rows(sums)[0:4]
    nonlocal0 = band_dots(values0, coupled0)
    spread(couple[...], values0)
    for c in range(2):
        for b in range(2):
            at, of = slice(96 * c, 96 * c + 96), slice(128 * b, 128 * b + 128)
            vec[1, at, of] = direction[at, of] * (kin[...] + shift[b])
    apply(beta_rows, 128, vec.at[1])
    sums = small_total(3)
    norm0 = unpacked(sums[1:2])
    curve0 = [c + n for c, n in zip(unpacked(sums[0:1]), nonlocal0)]
    alpha0 = [norm0[b] / curve0[b] for b in range(2)]
    arrived(3)
    image[...] += z_forward(3)
    residual = vec.at[1]
    for c in range(2):
        for b in range(2):
            at, of = slice(96 * c, 96 * c + 96), slice(128 * b, 128 * b + 128)
            residual[at, of] = direction[at, of] - alpha0[b] * image[at, of]

    transform_out(4, residual)
    project(beta_rows, 128, residual)
    small_send[2] = jnp.zeros((8, 128), f32)
    for o in range(4):
        small_send[2, o : o + 1, :] = projections(o, 128)
    small_send[2, 4:5, :] = packed(stick_sum(residual, residual))
    small_exchange(2)
    selfs = stick_sum(residual, residual, True)
    crosses = stick_sum(residual, direction, True)
    fill_planes(4, field1)
    self_local = grid_sum(field1, field1)
    cross_local = grid_sum(field1, field0)
    small_send[4] = jnp.zeros((8, 128), f32)
    small_send[4, 0:1, :] = packed([selfs[b] + self_local[b] for b in range(2)])
    small_send[4, 1:2, :] = packed([crosses[b] + cross_local[b] for b in range(2)])
    small_exchange(4)
    with jax.named_scope("products"):
        for p in range(PLANES):
            for b in range(2):
                lanes = slice(128 * (2 * p + b), 128 * (2 * p + b) + 128)
                for n, field in enumerate((field0, field1)):
                    dens[96 * n : 96 * n + 96, lanes] = 4.0 * (
                        psi_field[0:96, lanes] * field[0:96, lanes]
                        + psi_field[96:192, lanes] * field[96:192, lanes]
                    )
    sums = small_total(2)
    values1 = sums[0:4]
    coupled1 = coupled_rows(sums)[0:4]
    self_dots = band_dots(values1, coupled1)
    cross_dots = band_dots(values1, coupled0)
    weight0, weight1 = [], []
    norm1 = unpacked(sums[4:5])
    sums = small_total(4)
    self1, cross1 = (unpacked(sums[n : n + 1]) for n in range(2))
    for b in range(2):
        ratio = norm1[b] / norm0[b]
        self_curve = self1[b] + self_dots[b]
        cross_curve = cross1[b] + cross_dots[b]
        curve = self_curve + ratio * (2.0 * cross_curve + ratio * curve0[b])
        alpha = norm1[b] / curve
        weight0.append(alpha0[b] + alpha * ratio)
        weight1.append(alpha)

    with jax.named_scope("density"):
        for p in range(PLANES):
            total = jnp.zeros((GRID, 128), f32)
            for b in range(2):
                lanes = slice(128 * (2 * p + b), 128 * (2 * p + b) + 128)
                total = total + weight0[b] * dens[0:96, lanes] + weight1[b] * dens[96:192, lanes]
            for i in range(nb):
                part_send[i, 12 * p : 12 * p + 12, :] = total[12 * i : 12 * i + 12, :]

    for k in BANDS_FAR:
        part_copy(k).start()
    part_recv[mb] = part_send[mb]
    first_out[...] = direction[...]
    second_out[...] = residual[...]
    for b in range(2):
        weights_out[b : b + 1, :] = jnp.broadcast_to(weight0[b], (1, 128))
        weights_out[2 + b : 3 + b, :] = jnp.broadcast_to(weight1[b], (1, 128))
    weights_out[4:8, :] = jnp.zeros((4, 128), f32)

    for rnd in range(5):
        if rnd != 2:
            ga_all(rnd).wait_send()
        small_all(rnd).wait_send()
    gather_sent(occupied, psi_sem)
    gather_sent(zall, z_sem)
    proj_all().wait_send()
    with jax.named_scope("part_wait"):
        part_all().wait_recv()
    cells_out[...] = jnp.sum(part_recv[...], axis=0)

    part_all().wait_send()


OUTS = tuple(
    pltpu.VMEM(shape, f32) for shape in ((192, 256), (192, 256), (8, 128), (72, 128))
)


def finish(first, second, weights, cells, response, density):
    for c in range(2):
        for b in range(2):
            at, of = slice(96 * c, 96 * c + 96), slice(128 * b, 128 * b + 128)
            response[c, b] = (
                weights[b : b + 1, :] * first[at, of] + weights[2 + b : 3 + b, :] * second[at, of]
            )
    for y in range(12):
        density[:, 96 * y : 96 * y + 96] = cells[pl.ds(y, PLANES, stride=12), :][:, 0:96]


def per_device(psi, vloc, dv, beta, dij, atom_type, stick_xy, band_shift):
    vmem = pl.BlockSpec(memory_space=pltpu.VMEM)
    dma = pltpu.SemaphoreType.DMA
    every = tables()
    early, late = every[:1], every[1:]
    pieces = pl.pallas_call(
        kernel,
        out_shape=OUTS,
        in_specs=[pl.BlockSpec(memory_space=pl.ANY)] * 19,
        out_specs=(vmem,) * 4,
        scratch_shapes=[
            pltpu.SMEM((2,), f32),
            pltpu.SMEM((2, 4, 4), f32),
            pltpu.SMEM((32,), jnp.int32),
            pltpu.VMEM((2, 2, GRID, 128), bf16),
            pltpu.VMEM((GROUPS, 128), jnp.int32),
            *[pltpu.VMEM(t.shape, t.dtype) for t in early],
            pltpu.VMEM((PLANES, GRID * GRID), f32),
            pltpu.VMEM((PLANES, GRID * GRID), f32),
            *[pltpu.VMEM(t.shape, t.dtype) for t in late],
            pltpu.VMEM((2, 128, GRID, 128), f32),
            pltpu.VMEM((GRID, 768), f32),
            pltpu.VMEM((GRID, 768), f32),
            pltpu.VMEM((768, 128), f32),
            pltpu.VMEM((8, 2, 2, GRID, 128), bf16),
            pltpu.VMEM((512, 2048), bf16),
            pltpu.VMEM((8, 2048), f32),
            pltpu.VMEM((5, GROUPS, ROWS, 128), f32),
            pltpu.VMEM((5, GROUPS, ROWS, 128), f32),
            pltpu.VMEM((5, 8, 128), f32),
            pltpu.VMEM((5, GROUPS, 8, 128), f32),
            pltpu.VMEM((8, 72, 128), f32),
            pltpu.VMEM((8, 72, 128), f32),
            pltpu.VMEM((384, 2048), bf16),
            pltpu.VMEM((192, 512), f32),
            pltpu.VMEM((384, 512), f32),
            pltpu.VMEM((384, 512), bf16),
            pltpu.VMEM((384, 512), bf16),
            pltpu.VMEM((128, 1536), bf16),
            pltpu.VMEM((128, 1536), bf16),
            pltpu.VMEM((192, 1536), f32),
            pltpu.VMEM((192, 1536), f32),
            pltpu.VMEM((192, 1536), f32),
            pltpu.VMEM((384, 512), bf16),
            pltpu.VMEM((2, 384, 512), f32),
            pltpu.VMEM((8, GROUPS, ROWS, 128), f32),
            pltpu.VMEM((256, 2048), bf16),
            pltpu.VMEM((256, 2048), bf16),
            pltpu.VMEM((17, 8, 128), f32),
            pltpu.VMEM((4, 128, 128), f32),
            pltpu.VMEM((4, 128, 128), f32),
            pltpu.VMEM((128, 128), f32),
            pltpu.VMEM((2, 192, 256), f32),
            pltpu.VMEM((192, 256), f32),
            pltpu.VMEM((GRID, 128), f32),
            pltpu.VMEM((8, 2048), f32),
            pltpu.VMEM((192, 1536), f32),
            dma((19,)),
            dma((3,)),
            dma((3,)),
            dma((2,)),
            dma((5,)),
            dma((GROUPS,)),
            dma((4,)),
            dma((5,)),
            dma((5,)),
            dma((2,)),
        ],
        compiler_params=pltpu.CompilerParams(
            collective_id=0, has_side_effects=True, vmem_limit_bytes=60 * 1024 * 1024
        ),
    )(
        band_shift, dij, atom_type, psi, stick_xy.reshape(GROUPS, 128), *early,
        vloc, dv, *late, beta,
    )
    return pl.pallas_call(
        finish,
        out_shape=(
            jax.ShapeDtypeStruct((2, 2, GRID, 128), f32),
            jax.ShapeDtypeStruct((PLANES, 12 * GRID), f32),
        ),
        in_specs=[vmem] * 4,
        out_specs=(vmem, vmem),
    )(*(pltpu.with_memory_space_constraint(p, pltpu.VMEM) for p in pieces))


def solution(mesh):
    return jax.shard_map(
        per_device,
        mesh=mesh,
        in_specs=(
            P(None, "band", None, "ga"),
            P("ga", None),
            P("ga", None),
            P(None, None, None, "ga"),
            P(),
            P(),
            P(),
            P("band"),
        ),
        out_specs=(P(None, "band", None, "ga"), P("ga", "band")),
        check_vma=False,
    )
```
